8 devices in a mesh: pairs: 1 (over z), rows: 8 (over y, x, core).
Axes of the slice: x: 2, y: 2, z: 1, core: 2. Of those that a mesh axis runs over, the one named last changes fastest.
Arguments:
- cost_src: float32 [2048, 2048], P(('pairs', 'rows'))
- cost_tgt: float32 [2048, 2048], P(('pairs', 'rows'))
- plan_init: float32 [2048, 2048], P(('pairs', 'rows'))
- mass_src: float32 [2048], P(('pairs', 'rows'))
- mass_tgt: float32 [2048], P('pairs')
- feat_src: float32 [2048, 256], P(('pairs', 'rows'))
- feat_tgt: float32 [2048, 256], P(('pairs', 'rows'))
- epsilon: float32 [], replicated
Outputs:
- output: float32 [2048, 2048], P(('pairs', 'rows'))
All inputs are finite; a program needn't handle non-finite values.
Results may differ from the reference program's by a relative error of at most 0.001.
Values are sent between devices in bfloat16 or wider.
A program may use at most 1 GiB of HBM per device.

```python
import jax
import jax.numpy as jnp
from jax import lax

N = 2048
M = 2048
D = 256
OUTER_STEPS = 2
SWEEPS = 10
ALPHA = 0.5


def point_costs(key_pts, num_points):
    key_centers, key_labels, key_noise = jax.random.split(key_pts, 3)
    centers = 1.5 * jax.random.normal(key_centers, (8, 3), jnp.float32)
    labels = jax.random.randint(key_labels, (num_points,), 0, 8)
    points = centers[labels] + 0.4 * jax.random.normal(key_noise, (num_points, 3), jnp.float32)
    sq_dist = jnp.zeros((num_points, num_points), jnp.float32)
    for dim_index in range(3):
        column_vals = points[:, dim_index]
        coord_diff = column_vals[:, None] - column_vals[None, :]
        sq_dist = sq_dist + coord_diff * coord_diff
    return sq_dist / jnp.max(sq_dist), labels


def marginal(key_mass, num_points):
    weights = jnp.exp(0.5 * jax.random.normal(key_mass, (num_points,), jnp.float32))
    return weights / jnp.sum(weights)


def setup_inputs(seed: int = 0, part: int = 0) -> dict:
    base_key, shared_key = jax.random.split(jax.random.key(seed))
    sub_keys = jax.random.split(jax.random.fold_in(base_key, part), 7)
    cost_src, labels_src = point_costs(sub_keys[0], N)
    cost_tgt, labels_tgt = point_costs(sub_keys[1], M)
    mass_src = marginal(sub_keys[2], N)
    mass_tgt = marginal(sub_keys[3], M)
    block_logits = 3.0 * jax.random.normal(sub_keys[4], (8, 8), jnp.float32)
    plan_init = mass_src[:, None] * mass_tgt[None, :] * jnp.exp(block_logits[labels_src][:, labels_tgt])
    plan_init = plan_init / jnp.sum(plan_init)
    feat_scale = 0.125 * D ** -0.25
    feat_src = feat_scale * jax.random.normal(sub_keys[5], (N, D), jnp.float32)
    feat_tgt = feat_scale * jax.random.normal(sub_keys[6], (M, D), jnp.float32)
    epsilon = jax.random.uniform(shared_key, (), jnp.float32, 0.04, 0.08)
    return {"cost_src": cost_src, "cost_tgt": cost_tgt, "plan_init": plan_init, "mass_src": mass_src, "mass_tgt": mass_tgt, "feat_src": feat_src, "feat_tgt": feat_tgt, "epsilon": epsilon}


def reference(cost_src, cost_tgt, plan_init, mass_src, mass_tgt, feat_src, feat_tgt, epsilon):
    src_half = cost_src.astype(jnp.bfloat16)
    tgt_half = cost_tgt.astype(jnp.bfloat16)
    cross_term = jnp.dot(feat_src.astype(jnp.bfloat16), feat_tgt.astype(jnp.bfloat16).T, preferred_element_type=jnp.float32)
    feat_cost = (-2.0 * ALPHA) * cross_term

    def outer_step(step_index, transport):
        prod_a = jnp.dot(src_half, transport.astype(jnp.bfloat16), preferred_element_type=jnp.float32)
        prod_b = jnp.dot(prod_a.astype(jnp.bfloat16), tgt_half, preferred_element_type=jnp.float32)
        step_cost = feat_cost - (2.0 * (1.0 - ALPHA)) * prod_b
        kernel = jnp.exp(-(step_cost - jnp.min(step_cost, axis=1, keepdims=True)) / epsilon)

        def sinkhorn_sweep(sweep_index, scales):
            row_scale = mass_src / jnp.sum(kernel * scales[1][None, :], axis=1)
            return row_scale, mass_tgt / jnp.sum(kernel * row_scale[:, None], axis=0)

        start_scales = (jnp.ones_like(mass_src), jnp.ones_like(mass_tgt))
        row_scale, col_scale = lax.fori_loop(0, SWEEPS, sinkhorn_sweep, start_scales)
        return row_scale[:, None] * kernel * col_scale[None, :]

    return lax.fori_loop(0, OUTER_STEPS, outer_step, plan_init)
```

```python
import functools

import jax
import jax.numpy as jnp
from jax import lax
from jax.experimental import pallas as pl
from jax.experimental.pallas import tpu as pltpu
from jax.sharding import PartitionSpec as P

ALPHA = 0.5
OUTER_STEPS = 2
SWEEPS = 10
LANES = 128
SUB = 8


def entry_barrier(me, n):
    barrier = pltpu.get_barrier_semaphore()
    for off in range(1, n):
        pl.semaphore_signal(barrier, inc=1, device_id={"rows": lax.rem(me + off, n)})
    pl.semaphore_wait(barrier, n - 1)


def build_kernel(cost_ref, kern_ref, eps, rows, cols):
    tiles = cols // LANES

    def block(b, carry):
        row = pl.multiple_of(b * SUB, SUB)
        vals = [cost_ref[pl.ds(row, SUB), t * LANES:(t + 1) * LANES] for t in range(tiles)]
        low = functools.reduce(jnp.minimum, vals)
        low = jnp.min(low, axis=1, keepdims=True)
        for t in range(tiles):
            kern_ref[pl.ds(row, SUB), t * LANES:(t + 1) * LANES] = jnp.exp((low - vals[t]) / eps)
        return carry

    lax.fori_loop(0, rows // SUB, block, 0, unroll=4)


def tree_sum(vals):
    while len(vals) > 1:
        vals = [a + b for a, b in zip(vals[::2], vals[1::2])] + vals[len(vals) & ~1:]
    return vals[0]


def sinkhorn(me, n, kern_ref, p_ref, q_ref, u_ref, v_ref, part_ref, gath_ref, send_sem, recv_sem, rows, cols, first):
    tiles = cols // LANES
    blocks = rows // SUB

    def copy(par, peer, slot):
        return pltpu.make_async_remote_copy(
            src_ref=part_ref.at[par], dst_ref=gath_ref.at[par, slot],
            send_sem=send_sem.at[par, peer], recv_sem=recv_sem.at[par, slot], device_id={"rows": peer})

    v_ref[...] = jnp.ones_like(v_ref)

    def sweep(step, carry):
        par = lax.rem(step + first, 2)
        vrow = [jnp.broadcast_to(v_ref[t:t + 1, :], (SUB, LANES)) for t in range(tiles)]
        for b in range(blocks):
            prods = [kern_ref[b * SUB:(b + 1) * SUB, t * LANES:(t + 1) * LANES] * vrow[t] for t in range(tiles)]
            dots = jnp.sum(tree_sum(prods), axis=1, keepdims=True)
            u_ref[b * SUB:(b + 1) * SUB, :] = p_ref[b * SUB:(b + 1) * SUB, :] / dots
        acc = [None] * tiles
        for b in range(blocks):
            scale = u_ref[b * SUB:(b + 1) * SUB, :]
            for t in range(tiles):
                term = kern_ref[b * SUB:(b + 1) * SUB, t * LANES:(t + 1) * LANES] * scale
                acc[t] = term if acc[t] is None else acc[t] + term
        sums = jnp.concatenate([jnp.sum(a, axis=0, keepdims=True) for a in acc], axis=0)
        part_ref[par] = sums
        gath_ref[par, me] = sums
        for off in range(1, n):
            copy(par, lax.rem(me + off, n), me).start()
        for off in range(1, n):
            copy(par, lax.rem(me + off, n), lax.rem(me + off, n)).wait_recv()
        total = gath_ref[par, 0]
        for d in range(1, n):
            total = total + gath_ref[par, d]
        v_ref[...] = q_ref[...] / total
        for off in range(1, n):
            copy(par, lax.rem(me + off, n), me).wait_send()
        return carry

    lax.fori_loop(0, SWEEPS, sweep, 0)


def write_plan(kern_ref, u_ref, v_ref, out_ref, rows, cols):
    tiles = cols // LANES
    vrow = [jnp.broadcast_to(v_ref[t:t + 1, :], (SUB, LANES)) for t in range(tiles)]

    def block(b, carry):
        row = pl.multiple_of(b * SUB, SUB)
        scale = u_ref[pl.ds(row, SUB), :]
        for t in range(tiles):
            out_ref[pl.ds(row, SUB), t * LANES:(t + 1) * LANES] = scale * kern_ref[pl.ds(row, SUB), t * LANES:(t + 1) * LANES] * vrow[t]
        return carry

    lax.fori_loop(0, rows // SUB, block, 0, unroll=4)


def sinkhorn_kernel(n, eps_ref, cost_ref, p_ref, q_ref, out_ref, kern_ref, u_ref, v_ref, part_ref, gath_ref, send_sem, recv_sem):
    me = lax.axis_index("rows")
    rows, cols = cost_ref.shape
    entry_barrier(me, n)
    build_kernel(cost_ref, kern_ref, eps_ref[0], rows, cols)
    sinkhorn(me, n, kern_ref, p_ref, q_ref, u_ref, v_ref, part_ref, gath_ref, send_sem, recv_sem, rows, cols, 0)
    write_plan(kern_ref, u_ref, v_ref, out_ref, rows, cols)


def scaled_plan(n, cid, cost, p_wide, q_tiles, eps):
    rows, cols = cost.shape
    tiles = cols // LANES
    vmem = pl.BlockSpec(memory_space=pltpu.VMEM)
    return pl.pallas_call(
        functools.partial(sinkhorn_kernel, n),
        out_shape=jax.ShapeDtypeStruct((rows, cols), jnp.float32),
        in_specs=[pl.BlockSpec(memory_space=pltpu.SMEM), vmem, vmem, vmem],
        out_specs=vmem,
        scratch_shapes=[
            pltpu.VMEM((rows, cols), jnp.float32),
            pltpu.VMEM((rows, LANES), jnp.float32),
            pltpu.VMEM((tiles, LANES), jnp.float32),
            pltpu.VMEM((2, tiles, LANES), jnp.float32),
            pltpu.VMEM((2, n, tiles, LANES), jnp.float32),
            pltpu.SemaphoreType.DMA((2, n)),
            pltpu.SemaphoreType.DMA((2, n)),
        ],
        compiler_params=pltpu.CompilerParams(collective_id=cid, has_side_effects=True, vmem_limit_bytes=32 << 20),
        name="scaled_plan",
    )(eps, cost, p_wide, q_tiles)


def solution(mesh):
    n = mesh.shape["rows"]

    def local_fgw(cost_src, cost_tgt, plan_init, mass_src, mass_tgt, feat_src, feat_tgt, epsilon):
        src_half = cost_src.astype(jnp.bfloat16)
        tgt_half = cost_tgt.astype(jnp.bfloat16)
        feat_all = lax.all_gather(feat_tgt.astype(jnp.bfloat16), 'rows', tiled=True)
        cross_term = jnp.einsum('id,jd->ij', feat_src.astype(jnp.bfloat16), feat_all, preferred_element_type=jnp.float32)
        feat_cost = (-2.0 * ALPHA) * cross_term
        p_wide = jnp.broadcast_to(mass_src[:, None], (mass_src.shape[0], LANES))
        q_tiles = mass_tgt.reshape(-1, LANES)
        eps = epsilon.reshape(1)
        transport = plan_init
        for step_index in range(OUTER_STEPS):
            transport_all = lax.all_gather(transport.astype(jnp.bfloat16), 'rows', tiled=True)
            tgt_all = lax.all_gather(tgt_half, 'rows', tiled=True)
            prod_a = jnp.dot(src_half, transport_all, preferred_element_type=jnp.float32)
            prod_b = jnp.dot(prod_a.astype(jnp.bfloat16), tgt_all, preferred_element_type=jnp.float32)
            step_cost = feat_cost - (2.0 * (1.0 - ALPHA)) * prod_b
            transport = scaled_plan(n, 0, step_cost, p_wide, q_tiles, eps)
        return transport

    row_spec = P(('pairs', 'rows'), None)
    vec_spec = P(('pairs', 'rows'))
    in_specs = (row_spec, row_spec, row_spec, vec_spec, P('pairs'), row_spec, row_spec, P())
    return jax.shard_map(local_fgw, mesh=mesh, in_specs=in_specs, out_specs=row_spec, check_vma=False)
```

```python
import functools

import jax
import jax.numpy as jnp
from jax import lax
from jax.experimental import pallas as pl
from jax.experimental.pallas import tpu as pltpu
from jax.sharding import PartitionSpec as P

ALPHA = 0.5
OUTER_STEPS = 2
SWEEPS = 10
LANES = 128
SUB = 8
BLK = 256
DEV = 8
AHEAD = 2
LAG = 2


def tree_sum(vals):
    while len(vals) > 1:
        vals = [a + b for a, b in zip(vals[::2], vals[1::2])] + vals[len(vals) & ~1:]
    return vals[0]


def rows_of(owner):
    return pl.ds(pl.multiple_of(owner * BLK, BLK), BLK)


class Place:
    def __init__(self):
        self.me = lax.axis_index("rows")
        core = lax.rem(self.me, 2)
        x = lax.rem(self.me // 2, 2)
        y = self.me // 4
        self.core = core
        self.sib = self.me + 1 - 2 * core
        dx, dy = 2 - 4 * x, 4 - 8 * y
        self.x0, self.x1 = self.me + dx, self.sib + dx
        self.y0, self.y1 = self.me + dy, self.sib + dy
        self.d0, self.d1 = self.me + dx + dy, self.sib + dx + dy


def build_kernel(cost_ref, kern_ref, eps, rows, cols):
    tiles = cols // LANES

    def block(b, carry):
        row = pl.multiple_of(b * SUB, SUB)
        vals = [cost_ref[pl.ds(row, SUB), t * LANES:(t + 1) * LANES] for t in range(tiles)]
        low = functools.reduce(jnp.minimum, vals)
        low = jnp.min(low, axis=1, keepdims=True)
        for t in range(tiles):
            kern_ref[pl.ds(row, SUB), t * LANES:(t + 1) * LANES] = jnp.exp((low - vals[t]) / eps)
        return carry

    lax.fori_loop(0, rows // SUB, block, 0, unroll=4)


def sinkhorn(at, kern_ref, p_ref, q_ref, u_ref, v_ref, part_ref, gath_ref, send_sem, recv_sem, rows, cols):
    tiles = cols // LANES
    blocks = rows // SUB
    me = at.me

    def copy(par, peer, slot):
        return pltpu.make_async_remote_copy(
            src_ref=part_ref.at[par], dst_ref=gath_ref.at[par, slot],
            send_sem=send_sem.at[par, peer], recv_sem=recv_sem.at[par, slot], device_id={"rows": peer})

    v_ref[...] = jnp.ones_like(v_ref)

    def sweep(step, carry):
        par = lax.rem(step, 2)
        vrow = [jnp.broadcast_to(v_ref[t:t + 1, :], (SUB, LANES)) for t in range(tiles)]
        for b in range(blocks):
            prods = [kern_ref[b * SUB:(b + 1) * SUB, t * LANES:(t + 1) * LANES] * vrow[t] for t in range(tiles)]
            dots = jnp.sum(tree_sum(prods), axis=1, keepdims=True)
            u_ref[b * SUB:(b + 1) * SUB, :] = p_ref[b * SUB:(b + 1) * SUB, :] / dots
        acc = [None] * tiles
        for b in range(blocks):
            scale = u_ref[b * SUB:(b + 1) * SUB, :]
            for t in range(tiles):
                term = kern_ref[b * SUB:(b + 1) * SUB, t * LANES:(t + 1) * LANES] * scale
                acc[t] = term if acc[t] is None else acc[t] + term
        sums = jnp.concatenate([jnp.sum(a, axis=0, keepdims=True) for a in acc], axis=0)
        part_ref[par] = sums
        gath_ref[par, me] = sums
        for off in range(1, DEV):
            copy(par, lax.rem(me + off, DEV), me).start()
        for off in range(1, DEV):
            copy(par, lax.rem(me + off, DEV), lax.rem(me + off, DEV)).wait_recv()
        total = gath_ref[par, 0]
        for d in range(1, DEV):
            total = total + gath_ref[par, d]
        v_ref[...] = q_ref[...] / total
        for off in range(1, DEV):
            copy(par, lax.rem(me + off, DEV), me).wait_send()
        return carry

    lax.fori_loop(0, SWEEPS, sweep, 0)


def plan_block(kern_ref, u_ref, v_ref, j):
    cols = pl.multiple_of(j * BLK, BLK)
    parts = []
    for h in range(BLK // LANES):
        vrow = v_ref[pl.ds(j * (BLK // LANES) + h, 1), :]
        parts.append(u_ref[...] * kern_ref[:, pl.ds(cols + h * LANES, LANES)] * vrow)
    return jnp.concatenate(parts, axis=1)


def gather_plan(at, chunks, plan_ref, send_sem, recv_sem, produce, near_end, column):
    def copy(owner, j, dest, kind):
        view = plan_ref.at[j, rows_of(owner), :]
        return pltpu.make_async_remote_copy(
            src_ref=view, dst_ref=view, send_sem=send_sem.at[kind, j],
            recv_sem=recv_sem.at[owner, j], device_id={"rows": dest})

    def send_own(j):
        copy(at.me, j, at.x0, 0).start()
        copy(at.me, j, at.y0, 1).start()
        copy(at.me, j, at.sib, 2).start()

    for j in range(AHEAD):
        produce(j)
        send_own(j)

    def turn(it, carry):
        @pl.when(it + AHEAD < chunks)
        def _():
            produce(it + AHEAD)
            send_own(it + AHEAD)

        @pl.when(it < chunks)
        def _():
            copy(at.x0, it, at.x0, 0).wait_recv()
            copy(at.x0, it, at.sib, 3).start()

            @pl.when(lax.rem(it, 2) == 0)
            def _():
                copy(at.x0, it, at.y0, 6).start()

            copy(at.y0, it, at.y0, 0).wait_recv()
            copy(at.y0, it, at.sib, 4).start()

            @pl.when(lax.rem(it, 2) == 1)
            def _():
                copy(at.y0, it, at.x0, 6).start()

        @pl.when(it == chunks - 1)
        def _():
            near_end()

        @pl.when((it >= LAG) & (it < LAG + chunks))
        def _():
            copy(at.d0, it - LAG, at.d0, 0).wait_recv()
            copy(at.d0, it - LAG, at.sib, 5).start()

        @pl.when(it >= LAG + 1)
        def _():
            j = it - LAG - 1
            for owner in (at.sib, at.x1, at.y1, at.d1):
                copy(owner, j, at.sib, 0).wait_recv()
            column(j)

        return carry

    lax.fori_loop(0, chunks + LAG + 1, turn, 0)

    def drain(j, carry):
        for kind in range(7):
            copy(at.me, j, at.sib, kind).wait_send()
        return carry

    lax.fori_loop(0, chunks, drain, 0)


def fgw_kernel(
    eps_ref, mass_ref, q_ref, src_hbm, tgt_hbm, plan_hbm, fsrc_hbm, ftgt_hbm, out_hbm,
    stage_ref, stage2_ref, feat_ref, plan_ref, tgt_ref, src_ref, fsrc_ref, a_ref, cross_ref, cost_ref, kern_ref,
    p_ref, u_ref, v_ref, part_ref, gath_ref,
    load_sem, plan_send, plan_recv, tgt_send, tgt_recv, sum_send, sum_recv,
):
    at = Place()
    me = at.me
    rows, cols = kern_ref.shape
    nblk = cols // BLK
    eps = eps_ref[0]

    def load_plan(j):
        return pltpu.make_async_copy(plan_hbm.at[:, pl.ds(pl.multiple_of(j * BLK, BLK), BLK)], stage_ref.at[j], load_sem.at[j])

    def load_tgt(j):
        return pltpu.make_async_copy(tgt_hbm.at[:, pl.ds(pl.multiple_of(j * BLK, BLK), BLK)], stage2_ref.at[j], load_sem.at[nblk + j])

    load_feat = pltpu.make_async_copy(ftgt_hbm, feat_ref.at[0], load_sem.at[2 * nblk])
    load_fsrc = pltpu.make_async_copy(fsrc_hbm, feat_ref.at[1], load_sem.at[2 * nblk + 1])
    load_src = pltpu.make_async_copy(src_hbm, cost_ref, load_sem.at[2 * nblk + 2])

    for j in range(nblk):
        load_plan(j).start()
    load_feat.start()
    load_fsrc.start()
    load_src.start()
    for j in range(nblk):
        load_tgt(j).start()

    barrier = pltpu.get_barrier_semaphore()
    for off in range(1, DEV):
        pl.semaphore_signal(barrier, inc=1, device_id={"rows": lax.rem(me + off, DEV)})

    eye = lax.broadcasted_iota(jnp.int32, (LANES, LANES), 0) == lax.broadcasted_iota(jnp.int32, (LANES, LANES), 1)
    for r in range(rows // LANES):
        line = jnp.broadcast_to(mass_ref[r:r + 1, :], (LANES, LANES))
        col = jnp.sum(jnp.where(eye, line, 0.0), axis=1, keepdims=True)
        p_ref[r * LANES:(r + 1) * LANES, :] = jnp.broadcast_to(col, (LANES, LANES))

    pl.semaphore_wait(barrier, DEV - 1)

    def cast_plan(j):
        if isinstance(j, int):
            load_plan(j).wait()
            plan_ref[j, rows_of(me), :] = stage_ref[j].astype(jnp.bfloat16)
            return

        @pl.when(j < nblk)
        def _():
            load_plan(j).wait()
            plan_ref[j, rows_of(me), :] = stage_ref[j].astype(jnp.bfloat16)

        @pl.when(j == nblk)
        def _():
            load_feat.wait()
            plan_ref[nblk, rows_of(me), :] = feat_ref[0].astype(jnp.bfloat16)

        @pl.when(j == AHEAD)
        def _():
            load_fsrc.wait()
            fsrc_ref[...] = feat_ref[1].astype(jnp.bfloat16)
            load_src.wait()
            src_ref[...] = cost_ref[...].astype(jnp.bfloat16)

        @pl.when(j < nblk)
        def _():
            load_tgt(j).wait()
            tgt_ref[j, rows_of(me), :] = stage2_ref[j].astype(jnp.bfloat16)

    def tcopy(owner, col, dest, kind):
        view = tgt_ref.at[col, rows_of(owner), :]
        return pltpu.make_async_remote_copy(
            src_ref=view, dst_ref=view, send_sem=tgt_send.at[kind, col],
            recv_sem=tgt_recv.at[owner, col], device_id={"rows": dest})

    out_x = (at.me, at.sib, at.y0, at.y1, at.d0)
    out_y = (at.sib, at.me, at.x0, at.x1, at.d1)
    in_x = (at.x0, at.x1, at.d0, at.d1, at.y0)
    in_y = (at.y1, at.y0, at.d0, at.d1, at.x1)

    def send_tgt():
        for j in range(AHEAD):
            load_tgt(j).wait()
            tgt_ref[j, rows_of(me), :] = stage2_ref[j].astype(jnp.bfloat16)
        for cx, cy in zip(out_x, out_y):
            tcopy(me, cx, at.x0, 0).start()
            tcopy(me, cy, at.y0, 1).start()

        def to_sib(j, carry):
            tcopy(me, j, at.sib, 2).start()
            return carry

        lax.fori_loop(0, nblk, to_sib, 0)

    def column(j):
        @pl.when(j < nblk)
        def _():
            prod = jnp.dot(src_ref[...], plan_ref[j], preferred_element_type=jnp.float32)
            a_ref[:, pl.ds(pl.multiple_of(j * BLK, BLK), BLK)] = prod.astype(jnp.bfloat16)

    gather_plan(at, nblk + 1, plan_ref, plan_send, plan_recv, cast_plan, send_tgt, column)

    def cross(j, carry):
        prod = lax.dot_general(
            fsrc_ref[...], plan_ref[nblk, rows_of(j), :], (((1,), (1,)), ((), ())), preferred_element_type=jnp.float32)
        cross_ref[:, pl.ds(pl.multiple_of(j * BLK, BLK), BLK)] = (-2.0 * ALPHA) * prod
        return carry

    lax.fori_loop(0, nblk, cross, 0)

    def mirror(owner, col):
        tgt_ref[owner, rows_of(col), :] = tgt_ref[col, rows_of(owner), :].T

    base = me - at.core
    xb, yb, db = at.x0 - at.core, at.y0 - at.core, at.d0 - at.core

    def mirror_own(t, carry):
        mirror(me, lax.rem(base + 2 + t, DEV))
        return carry

    lax.fori_loop(0, DEV - 2, mirror_own, 0)

    for k in range(5):
        tcopy(at.x0, in_x[k], at.x0, 0).wait_recv()
        tcopy(at.x0, in_x[k], at.sib, 3).start()
        if k == 1:
            tcopy(at.x0, at.x1, at.y0, 6).start()
        tcopy(at.y0, in_y[k], at.y0, 0).wait_recv()
        tcopy(at.y0, in_y[k], at.sib, 4).start()
        if k == 1:
            tcopy(at.y0, at.y0, at.x0, 6).start()
    for col in (at.d0, at.d1):
        tcopy(at.d0, col, at.d0, 0).wait_recv()
        tcopy(at.d0, col, at.sib, 5).start()

    def from_sib(j, carry):
        tcopy(at.sib, j, at.sib, 0).wait_recv()
        return carry

    lax.fori_loop(0, nblk, from_sib, 0)
    for col in (at.x1, at.x0, at.d1, at.d0, at.y1):
        tcopy(at.x1, col, at.sib, 0).wait_recv()
    for col in (at.y0, at.y1, at.d1, at.d0, at.x0):
        tcopy(at.y1, col, at.sib, 0).wait_recv()
    for col in (at.d1, at.d0):
        tcopy(at.d1, col, at.sib, 0).wait_recv()

    def mirror_sib(t, carry):
        mirror(at.sib, lax.rem(base + 2 + t, DEV))
        return carry

    lax.fori_loop(0, DEV - 2, mirror_sib, 0)

    def mirror_diag(t, carry):
        first = xb + (yb - xb) * (t // 4) + lax.rem(t // 2, 2)
        mirror(first, db + lax.rem(t, 2))
        return carry

    lax.fori_loop(0, 8, mirror_diag, 0)

    def mirror_xy(t, carry):
        mirror(xb + t, yb + t)
        mirror(yb + t, xb + 1 - t)
        return carry

    lax.fori_loop(0, 2, mirror_xy, 0)

    for cx, cy in zip(out_x, out_y):
        tcopy(me, cx, at.x0, 0).wait_send()
        tcopy(me, cy, at.y0, 1).wait_send()
    for k in range(5):
        tcopy(at.x0, in_x[k], at.sib, 3).wait_send()
        tcopy(at.y0, in_y[k], at.sib, 4).wait_send()
    for col in (at.d0, at.d1):
        tcopy(at.d0, col, at.sib, 5).wait_send()
    tcopy(at.x0, at.x1, at.y0, 6).wait_send()
    tcopy(at.y0, at.y0, at.x0, 6).wait_send()

    def sib_done(j, carry):
        tcopy(me, j, at.sib, 2).wait_send()
        return carry

    lax.fori_loop(0, nblk, sib_done, 0)

    def costs(j, carry):
        prod = jnp.dot(a_ref[...], tgt_ref[j], preferred_element_type=jnp.float32)
        where = pl.ds(pl.multiple_of(j * BLK, BLK), BLK)
        cost_ref[:, where] = cross_ref[:, where] - (2.0 * (1.0 - ALPHA)) * prod
        return carry

    def sweeps():
        lax.fori_loop(0, nblk, costs, 0)
        build_kernel(cost_ref, kern_ref, eps, rows, cols)
        sinkhorn(at, kern_ref, p_ref, q_ref, u_ref, v_ref, part_ref, gath_ref, sum_send, sum_recv, rows, cols)

    sweeps()

    def next_plan(j):
        plan_ref[j, rows_of(me), :] = plan_block(kern_ref, u_ref, v_ref, j).astype(jnp.bfloat16)

    gather_plan(at, nblk, plan_ref, plan_send, plan_recv, next_plan, lambda: None, column)
    sweeps()

    def store(j):
        return pltpu.make_async_copy(stage_ref.at[j], out_hbm.at[:, pl.ds(pl.multiple_of(j * BLK, BLK), BLK)], load_sem.at[j])

    def last_plan(j, carry):
        stage_ref[j] = plan_block(kern_ref, u_ref, v_ref, j)
        store(j).start()
        return carry

    lax.fori_loop(0, nblk, last_plan, 0)
    for j in range(nblk):
        store(j).wait()


def fgw(src, tgt, plan, mass, q, fsrc, ftgt, eps):
    rows, cols = plan.shape
    tiles = cols // LANES
    nblk = cols // BLK
    vmem = pl.BlockSpec(memory_space=pltpu.VMEM)
    hbm = pl.BlockSpec(memory_space=pl.ANY)
    f32, bf16 = jnp.float32, jnp.bfloat16
    return pl.pallas_call(
        fgw_kernel,
        out_shape=jax.ShapeDtypeStruct((rows, cols), f32),
        in_specs=[pl.BlockSpec(memory_space=pltpu.SMEM), vmem, vmem] + [hbm] * 5,
        out_specs=hbm,
        scratch_shapes=[
            pltpu.VMEM((nblk, BLK, BLK), f32),
            pltpu.VMEM((nblk, BLK, BLK), f32),
            pltpu.VMEM((2, BLK, BLK), f32),
            pltpu.VMEM((nblk + 1, DEV * BLK, BLK), bf16),
            pltpu.VMEM((nblk, DEV * BLK, BLK), bf16),
            pltpu.VMEM((rows, cols), bf16),
            pltpu.VMEM((BLK, BLK), bf16),
            pltpu.VMEM((rows, cols), bf16),
            pltpu.VMEM((rows, cols), f32),
            pltpu.VMEM((rows, cols), f32),
            pltpu.VMEM((rows, cols), f32),
            pltpu.VMEM((rows, LANES), f32),
            pltpu.VMEM((rows, LANES), f32),
            pltpu.VMEM((tiles, LANES), f32),
            pltpu.VMEM((2, tiles, LANES), f32),
            pltpu.VMEM((2, DEV, tiles, LANES), f32),
            pltpu.SemaphoreType.DMA((2 * nblk + 3,)),
            pltpu.SemaphoreType.DMA((7, nblk + 1)),
            pltpu.SemaphoreType.DMA((DEV, nblk + 1)),
            pltpu.SemaphoreType.DMA((7, nblk)),
            pltpu.SemaphoreType.DMA((DEV, nblk)),
            pltpu.SemaphoreType.DMA((2, DEV)),
            pltpu.SemaphoreType.DMA((2, DEV)),
        ],
        compiler_params=pltpu.CompilerParams(collective_id=0, has_side_effects=True, vmem_limit_bytes=60 << 20),
        name="fgw",
    )(eps, mass, q, src, tgt, plan, fsrc, ftgt)


def solution(mesh):
    def local_fgw(cost_src, cost_tgt, plan_init, mass_src, mass_tgt, feat_src, feat_tgt, epsilon):
        return fgw(
            cost_src, cost_tgt, plan_init, mass_src.reshape(-1, LANES), mass_tgt.reshape(-1, LANES),
            feat_src, feat_tgt, epsilon.reshape(1))

    row_spec = P(('pairs', 'rows'), None)
    vec_spec = P(('pairs', 'rows'))
    in_specs = (row_spec, row_spec, row_spec, vec_spec, P('pairs'), row_spec, row_spec, P())
    return jax.shard_map(local_fgw, mesh=mesh, in_specs=in_specs, out_specs=row_spec, check_vma=False)
```

```python
import functools

import jax
import jax.numpy as jnp
from jax import lax
from jax.experimental import pallas as pl
from jax.experimental.pallas import tpu as pltpu
from jax.sharding import PartitionSpec as P

ALPHA = 0.5
OUTER_STEPS = 2
SWEEPS = 10
LANES = 128
SUB = 8
BLK = 256
DEV = 8
AHEAD = 2
LAG = 2
EARLY = 7


def tree_sum(vals):
    while len(vals) > 1:
        vals = [a + b for a, b in zip(vals[::2], vals[1::2])] + vals[len(vals) & ~1:]
    return vals[0]


def rows_of(owner):
    return pl.ds(pl.multiple_of(owner * BLK, BLK), BLK)


class Place:
    def __init__(self):
        self.me = lax.axis_index("rows")
        core = lax.rem(self.me, 2)
        x = lax.rem(self.me // 2, 2)
        y = self.me // 4
        self.core = core
        self.sib = self.me + 1 - 2 * core
        dx, dy = 2 - 4 * x, 4 - 8 * y
        self.x0, self.x1 = self.me + dx, self.sib + dx
        self.y0, self.y1 = self.me + dy, self.sib + dy
        self.d0, self.d1 = self.me + dx + dy, self.sib + dx + dy


def build_kernel(cost_ref, kern_ref, eps, start, rows, cols):
    tiles = cols // LANES

    def block(b, carry):
        row = pl.multiple_of(start + b * SUB, SUB)
        vals = [cost_ref[pl.ds(row, SUB), t * LANES:(t + 1) * LANES] for t in range(tiles)]
        low = functools.reduce(jnp.minimum, vals)
        low = jnp.min(low, axis=1, keepdims=True)
        for t in range(tiles):
            kern_ref[0, pl.ds(row, SUB), t * LANES:(t + 1) * LANES] = jnp.exp((low - vals[t]) / eps)
        return carry

    lax.fori_loop(0, rows // SUB, block, 0, unroll=4)


def spread(line, eye):
    wide = jnp.broadcast_to(line, (LANES, LANES))
    col = jnp.sum(jnp.where(eye, wide, 0.0), axis=1, keepdims=True)
    return jnp.broadcast_to(col, (LANES, LANES))


def sinkhorn(at, kern_ref, p_ref, q_ref, u_ref, v_ref, part_ref, gath_ref, send_sem, recv_sem):
    halves, rows, cols = kern_ref.shape
    tiles = cols // LANES
    blocks = [(h, b) for h in range(halves) for b in range(rows // SUB)]
    chip = at.me // 2
    peers = (at.x0, at.y0, at.d0)

    def copy(par, k, slot):
        return pltpu.make_async_remote_copy(
            src_ref=part_ref.at[par], dst_ref=gath_ref.at[par, slot],
            send_sem=send_sem.at[par, k], recv_sem=recv_sem.at[par, slot], device_id={"rows": peers[k]})

    v_ref[...] = jnp.ones_like(v_ref)

    def sweep(step, carry):
        par = lax.rem(step, 2)
        vrow = [jnp.broadcast_to(v_ref[t:t + 1, :], (SUB, LANES)) for t in range(tiles)]
        for h, b in blocks:
            prods = [kern_ref[h, b * SUB:(b + 1) * SUB, t * LANES:(t + 1) * LANES] * vrow[t] for t in range(tiles)]
            dots = jnp.sum(tree_sum(prods), axis=1, keepdims=True)
            at_row = slice(h * rows + b * SUB, h * rows + (b + 1) * SUB)
            u_ref[at_row, :] = p_ref[at_row, :] / dots
        acc = [None] * tiles
        for h, b in blocks:
            scale = u_ref[h * rows + b * SUB:h * rows + (b + 1) * SUB, :]
            for t in range(tiles):
                term = kern_ref[h, b * SUB:(b + 1) * SUB, t * LANES:(t + 1) * LANES] * scale
                acc[t] = term if acc[t] is None else acc[t] + term
        sums = jnp.concatenate([jnp.sum(a, axis=0, keepdims=True) for a in acc], axis=0)
        part_ref[par] = sums
        for k in (2, 0, 1):
            copy(par, k, chip).start()
        gath_ref[par, chip] = sums
        for k in range(3):
            copy(par, k, peers[k] // 2).wait_recv()
        total = gath_ref[par, 0]
        for d in range(1, DEV // 2):
            total = total + gath_ref[par, d]
        v_ref[...] = q_ref[...] / total
        for k in range(3):
            copy(par, k, chip).wait_send()
        return carry

    lax.fori_loop(0, SWEEPS, sweep, 0)


def plan_block(kern, scale, v_ref, j):
    parts = []
    for h in range(BLK // LANES):
        vrow = v_ref[pl.ds(j * (BLK // LANES) + h, 1), :]
        parts.append(scale * kern(h) * vrow)
    return jnp.concatenate(parts, axis=1)


def gather_plan(at, chunks, plan_ref, send_sem, recv_sem, produce, near_end, column, form=None):
    def copy(owner, j, dest, kind):
        view = plan_ref.at[j, rows_of(owner), :]
        return pltpu.make_async_remote_copy(
            src_ref=view, dst_ref=view, send_sem=send_sem.at[kind, j],
            recv_sem=recv_sem.at[owner, j], device_id={"rows": dest})

    def over_links(j):
        return True if form is None else (at.core == 1) | (j >= EARLY)

    def when(cond):
        return (lambda f: f()) if cond is True else pl.when(cond)

    def send_own(j):
        @when(over_links(j))
        def _():
            copy(at.me, j, at.x0, 0).start()
            copy(at.me, j, at.y0, 1).start()

        copy(at.me, j, at.sib, 2).start()

    for j in range(AHEAD):
        produce(j)
        send_own(j)

    def turn(it, carry):
        @pl.when(it + AHEAD < chunks)
        def _():
            produce(it + AHEAD)
            send_own(it + AHEAD)

        @pl.when((it < chunks) & over_links(it))
        def _():
            copy(at.x0, it, at.x0, 0).wait_recv()
            copy(at.x0, it, at.sib, 3).start()

            @pl.when(lax.rem(it, 2) == 0)
            def _():
                copy(at.x0, it, at.y0, 6).start()

            copy(at.y0, it, at.y0, 0).wait_recv()
            copy(at.y0, it, at.sib, 4).start()

            @pl.when(lax.rem(it, 2) == 1)
            def _():
                copy(at.y0, it, at.x0, 6).start()

        if form is not None:
            @pl.when((it < chunks) & (at.core == 0) & (it < EARLY))
            def _():
                for k, owner in enumerate((at.x0, at.y0, at.d0)):
                    plan_ref[it, rows_of(owner), :] = form(k, it).astype(jnp.bfloat16)
                    copy(owner, it, at.sib, 3 + k).start()

        @pl.when(it == chunks - 1)
        def _():
            near_end()

        @pl.when((it >= LAG) & (it < LAG + chunks) & over_links(it - LAG))
        def _():
            copy(at.d0, it - LAG, at.d0, 0).wait_recv()
            copy(at.d0, it - LAG, at.sib, 5).start()

        @pl.when(it >= LAG + 1)
        def _():
            j = it - LAG - 1
            for owner in (at.sib, at.x1, at.y1, at.d1):
                copy(owner, j, at.sib, 0).wait_recv()
            column(j)

        return carry

    lax.fori_loop(0, chunks + LAG + 1, turn, 0)

    def drain(j, carry):
        for kind in (2, 3, 4, 5):
            copy(at.me, j, at.sib, kind).wait_send()

        @when(over_links(j))
        def _():
            for kind in (0, 1, 6):
                copy(at.me, j, at.sib, kind).wait_send()

        return carry

    lax.fori_loop(0, chunks, drain, 0)


def fgw_kernel(
    eps_ref, mass_ref, q_ref, src_hbm, tgt_hbm, plan_hbm, fsrc_hbm, ftgt_hbm, out_hbm,
    stage_ref, stage2_ref, feat_ref, plan_ref, tgt_ref, src_ref, fsrc_ref, a_ref, cross_ref, cost_ref, kern_ref,
    early_ref, p_ref, u_ref, v_ref, other_ref, part_ref, gath_ref, msg_ref, news_ref, mass2_ref,
    load_sem, plan_send, plan_recv, tgt_send, tgt_recv, sum_send, sum_recv, half_send, half_recv,
    early_send, early_recv, msg_send, msg_recv,
):
    at = Place()
    me = at.me
    _, rows, cols = kern_ref.shape
    nblk = cols // BLK
    eps = eps_ref[0]

    def load_plan(j):
        return pltpu.make_async_copy(plan_hbm.at[:, pl.ds(pl.multiple_of(j * BLK, BLK), BLK)], stage_ref.at[j], load_sem.at[j])

    def load_tgt(j):
        return pltpu.make_async_copy(tgt_hbm.at[:, pl.ds(pl.multiple_of(j * BLK, BLK), BLK)], stage2_ref.at[j], load_sem.at[nblk + j])

    load_feat = pltpu.make_async_copy(ftgt_hbm, feat_ref.at[0], load_sem.at[2 * nblk])
    load_fsrc = pltpu.make_async_copy(fsrc_hbm, feat_ref.at[1], load_sem.at[2 * nblk + 1])
    load_src = pltpu.make_async_copy(src_hbm, cost_ref, load_sem.at[2 * nblk + 2])

    for j in range(nblk):
        load_plan(j).start()
    load_feat.start()
    load_fsrc.start()
    load_src.start()
    for j in range(nblk):
        load_tgt(j).start()

    barrier = pltpu.get_barrier_semaphore()
    for off in range(1, DEV):
        pl.semaphore_signal(barrier, inc=1, device_id={"rows": lax.rem(me + off, DEV)})

    pl.semaphore_wait(barrier, DEV - 1)

    swap = pltpu.make_async_remote_copy(
        src_ref=mass_ref, dst_ref=mass2_ref, send_sem=half_send.at[4], recv_sem=half_recv.at[4], device_id={"rows": at.sib})
    swap.start()
    eye = lax.broadcasted_iota(jnp.int32, (LANES, LANES), 0) == lax.broadcasted_iota(jnp.int32, (LANES, LANES), 1)

    def cast_plan(j):
        if isinstance(j, int):
            load_plan(j).wait()
            plan_ref[j, rows_of(me), :] = stage_ref[j].astype(jnp.bfloat16)
            return

        @pl.when(j < nblk)
        def _():
            load_plan(j).wait()
            plan_ref[j, rows_of(me), :] = stage_ref[j].astype(jnp.bfloat16)

        @pl.when(j == nblk)
        def _():
            load_feat.wait()
            plan_ref[nblk, rows_of(me), :] = feat_ref[0].astype(jnp.bfloat16)

        @pl.when(j == AHEAD)
        def _():
            load_fsrc.wait()
            fsrc_ref[...] = feat_ref[1].astype(jnp.bfloat16)
            load_src.wait()
            src_ref[...] = cost_ref[...].astype(jnp.bfloat16)

        @pl.when(j < nblk)
        def _():
            load_tgt(j).wait()
            tgt_ref[j, rows_of(me), :] = stage2_ref[j].astype(jnp.bfloat16)

    def tcopy(owner, col, dest, kind):
        view = tgt_ref.at[col, rows_of(owner), :]
        return pltpu.make_async_remote_copy(
            src_ref=view, dst_ref=view, send_sem=tgt_send.at[kind, col],
            recv_sem=tgt_recv.at[owner, col], device_id={"rows": dest})

    out_x = (at.me, at.sib, at.y0, at.y1, at.d0)
    out_y = (at.sib, at.me, at.x0, at.x1, at.d1)
    in_x = (at.x0, at.x1, at.d0, at.d1, at.y0)
    in_y = (at.y1, at.y0, at.d0, at.d1, at.x1)

    def send_tgt():
        for j in range(AHEAD):
            load_tgt(j).wait()
            tgt_ref[j, rows_of(me), :] = stage2_ref[j].astype(jnp.bfloat16)
        for cx, cy in zip(out_x, out_y):
            tcopy(me, cx, at.x0, 0).start()
            tcopy(me, cy, at.y0, 1).start()

        def to_sib(j, carry):
            tcopy(me, j, at.sib, 2).start()
            return carry

        lax.fori_loop(0, nblk, to_sib, 0)

    def column(j):
        @pl.when(j < nblk)
        def _():
            prod = jnp.dot(src_ref[...], plan_ref[j], preferred_element_type=jnp.float32)
            a_ref[:, pl.ds(pl.multiple_of(j * BLK, BLK), BLK)] = prod.astype(jnp.bfloat16)

    gather_plan(at, nblk + 1, plan_ref, plan_send, plan_recv, cast_plan, send_tgt, column)

    swap.wait()
    for r in range(rows // LANES):
        p_ref[r * LANES:(r + 1) * LANES, :] = spread(mass_ref[r:r + 1, :], eye)
        p_ref[rows + r * LANES:rows + (r + 1) * LANES, :] = spread(mass2_ref[r:r + 1, :], eye)

    def cross(j, carry):
        prod = lax.dot_general(
            fsrc_ref[...], plan_ref[nblk, rows_of(j), :], (((1,), (1,)), ((), ())), preferred_element_type=jnp.float32)
        cross_ref[:, pl.ds(pl.multiple_of(j * BLK, BLK), BLK)] = (-2.0 * ALPHA) * prod
        return carry

    lax.fori_loop(0, nblk, cross, 0)

    def mirror(owner, col):
        tgt_ref[owner, rows_of(col), :] = tgt_ref[col, rows_of(owner), :].T

    base = me - at.core
    xb, yb, db = at.x0 - at.core, at.y0 - at.core, at.d0 - at.core

    def mirror_own(t, carry):
        mirror(me, lax.rem(base + 2 + t, DEV))
        return carry

    lax.fori_loop(0, DEV - 2, mirror_own, 0)

    for k in range(5):
        tcopy(at.x0, in_x[k], at.x0, 0).wait_recv()
        tcopy(at.x0, in_x[k], at.sib, 3).start()
        if k == 1:
            tcopy(at.x0, at.x1, at.y0, 6).start()
        tcopy(at.y0, in_y[k], at.y0, 0).wait_recv()
        tcopy(at.y0, in_y[k], at.sib, 4).start()
        if k == 1:
            tcopy(at.y0, at.y0, at.x0, 6).start()
    for col in (at.d0, at.d1):
        tcopy(at.d0, col, at.d0, 0).wait_recv()
        tcopy(at.d0, col, at.sib, 5).start()

    def from_sib(j, carry):
        tcopy(at.sib, j, at.sib, 0).wait_recv()
        return carry

    lax.fori_loop(0, nblk, from_sib, 0)
    for col in (at.x1, at.x0, at.d1, at.d0, at.y1):
        tcopy(at.x1, col, at.sib, 0).wait_recv()
    for col in (at.y0, at.y1, at.d1, at.d0, at.x0):
        tcopy(at.y1, col, at.sib, 0).wait_recv()
    for col in (at.d1, at.d0):
        tcopy(at.d1, col, at.sib, 0).wait_recv()

    def mirror_sib(t, carry):
        mirror(at.sib, lax.rem(base + 2 + t, DEV))
        return carry

    lax.fori_loop(0, DEV - 2, mirror_sib, 0)

    def mirror_diag(t, carry):
        first = xb + (yb - xb) * (t // 4) + lax.rem(t // 2, 2)
        mirror(first, db + lax.rem(t, 2))
        return carry

    lax.fori_loop(0, 8, mirror_diag, 0)

    def mirror_xy(t, carry):
        mirror(xb + t, yb + t)
        mirror(yb + t, xb + 1 - t)
        return carry

    lax.fori_loop(0, 2, mirror_xy, 0)

    for cx, cy in zip(out_x, out_y):
        tcopy(me, cx, at.x0, 0).wait_send()
        tcopy(me, cy, at.y0, 1).wait_send()
    for k in range(5):
        tcopy(at.x0, in_x[k], at.sib, 3).wait_send()
        tcopy(at.y0, in_y[k], at.sib, 4).wait_send()
    for col in (at.d0, at.d1):
        tcopy(at.d0, col, at.sib, 5).wait_send()
    tcopy(at.x0, at.x1, at.y0, 6).wait_send()
    tcopy(at.y0, at.y0, at.x0, 6).wait_send()

    def sib_done(j, carry):
        tcopy(me, j, at.sib, 2).wait_send()
        return carry

    lax.fori_loop(0, nblk, sib_done, 0)

    def costs(j, carry):
        prod = jnp.dot(a_ref[...], tgt_ref[j], preferred_element_type=jnp.float32)
        where = pl.ds(pl.multiple_of(j * BLK, BLK), BLK)
        cost_ref[:, where] = cross_ref[:, where] - (2.0 * (1.0 - ALPHA)) * prod
        return carry

    def half(i):
        part = pl.ds(i * (rows // 4), rows // 4)
        return pltpu.make_async_remote_copy(
            src_ref=kern_ref.at[0, part], dst_ref=kern_ref.at[1, part], send_sem=half_send.at[i],
            recv_sem=half_recv.at[i], device_id={"rows": at.sib})

    def early(src, j, slot, dest, kind):
        return pltpu.make_async_remote_copy(
            src_ref=src, dst_ref=early_ref.at[slot, j], send_sem=early_send.at[kind, j],
            recv_sem=early_recv.at[slot, j], device_id={"rows": dest})

    def own_part(j):
        return kern_ref.at[0, :, pl.ds(pl.multiple_of(j * BLK, BLK), BLK)]

    def early_round():
        def send(j):
            early(own_part(j), j, 0, at.x0, 0).start()
            early(own_part(j), j, 1, at.y0, 1).start()

        for j in range(AHEAD):
            send(j)

        def turn(j, carry):
            @pl.when(j + AHEAD < EARLY)
            def _():
                send(j + AHEAD)

            early(own_part(j), j, 0, at.x0, 0).wait_recv()

            @pl.when(lax.rem(j, 2) == 0)
            def _():
                early(early_ref.at[0, j], j, 2, at.y0, 2).start()

            early(own_part(j), j, 1, at.y0, 1).wait_recv()

            @pl.when(lax.rem(j, 2) == 1)
            def _():
                early(early_ref.at[1, j], j, 2, at.x0, 2).start()

            return carry

        lax.fori_loop(0, EARLY, turn, 0)

        def done(j, carry):
            early(own_part(j), j, 2, at.x0, 2).wait_recv()
            for kind in range(3):
                early(own_part(j), j, kind, at.x0, kind).wait_send()
            return carry

        lax.fori_loop(0, EARLY, done, 0)

    tiles = cols // LANES
    across = (at.sib, at.x1, at.y1, at.d1)

    def news(k):
        return pltpu.make_async_remote_copy(
            src_ref=msg_ref, dst_ref=news_ref.at[k], send_sem=msg_send.at[k], recv_sem=msg_recv.at[k],
            device_id={"rows": across[k]})

    def sweeps(first):
        reach = len(across) if first else 1
        lax.fori_loop(0, nblk, costs, 0)
        for i in range(4):
            build_kernel(cost_ref, kern_ref, eps, i * (rows // 4), rows // 4, cols)

            @pl.when(at.core == 0)
            def _():
                half(i).start()

        @pl.when(at.core == 1)
        def _():
            for i in range(4):
                half(i).wait_recv()
            sinkhorn(at, kern_ref, p_ref, q_ref, u_ref, v_ref, part_ref, gath_ref, sum_send, sum_recv)
            msg_ref[:tiles] = v_ref[...]
            msg_ref[tiles:] = jnp.zeros_like(msg_ref[tiles:])
            for r in range(rows // LANES):
                scale = u_ref[rows + r * LANES:rows + (r + 1) * LANES, :]
                msg_ref[tiles + r:tiles + r + 1] = jnp.sum(jnp.where(eye, scale, 0.0), axis=0, keepdims=True)
            for k in range(reach):
                news(k).start()
            for k in range(reach):
                news(k).wait_send()

        @pl.when(at.core == 0)
        def _():
            if first:
                early_round()
            for i in range(4):
                half(i).wait_send()
            for k in range(reach):
                news(k).wait_recv()
            v_ref[...] = news_ref[0, :tiles]
            for r in range(rows // LANES):
                u_ref[r * LANES:(r + 1) * LANES, :] = spread(news_ref[0, tiles + r:tiles + r + 1], eye)
                for k in range(1, reach):
                    other_ref[k - 1, r * LANES:(r + 1) * LANES, :] = spread(news_ref[k, tiles + r:tiles + r + 1], eye)

    def own_block(j):
        cols_at = pl.multiple_of(j * BLK, BLK)
        return plan_block(lambda h: kern_ref[0, :, pl.ds(cols_at + h * LANES, LANES)], u_ref[:rows, :], v_ref, j)

    sweeps(True)

    def next_plan(j):
        plan_ref[j, rows_of(me), :] = own_block(j).astype(jnp.bfloat16)

    def form(k, j):
        return plan_block(lambda h: early_ref[k, j, :, h * LANES:(h + 1) * LANES], other_ref[k], v_ref, j)

    gather_plan(at, nblk, plan_ref, plan_send, plan_recv, next_plan, lambda: None, column, form)
    sweeps(False)

    def store(j):
        return pltpu.make_async_copy(stage_ref.at[j], out_hbm.at[:, pl.ds(pl.multiple_of(j * BLK, BLK), BLK)], load_sem.at[j])

    def last_plan(j, carry):
        stage_ref[j] = own_block(j)
        store(j).start()
        return carry

    lax.fori_loop(0, nblk, last_plan, 0)
    for j in range(nblk):
        store(j).wait()


def fgw(src, tgt, plan, mass, q, fsrc, ftgt, eps):
    rows, cols = plan.shape
    tiles = cols // LANES
    nblk = cols // BLK
    vmem = pl.BlockSpec(memory_space=pltpu.VMEM)
    hbm = pl.BlockSpec(memory_space=pl.ANY)
    f32, bf16 = jnp.float32, jnp.bfloat16
    return pl.pallas_call(
        fgw_kernel,
        out_shape=jax.ShapeDtypeStruct((rows, cols), f32),
        in_specs=[pl.BlockSpec(memory_space=pltpu.SMEM), vmem, vmem] + [hbm] * 5,
        out_specs=hbm,
        scratch_shapes=[
            pltpu.VMEM((nblk, BLK, BLK), f32),
            pltpu.VMEM((nblk, BLK, BLK), f32),
            pltpu.VMEM((2, BLK, BLK), f32),
            pltpu.VMEM((nblk + 1, DEV * BLK, BLK), bf16),
            pltpu.VMEM((nblk, DEV * BLK, BLK), bf16),
            pltpu.VMEM((rows, cols), bf16),
            pltpu.VMEM((BLK, BLK), bf16),
            pltpu.VMEM((rows, cols), bf16),
            pltpu.VMEM((rows, cols), f32),
            pltpu.VMEM((rows, cols), f32),
            pltpu.VMEM((2, rows, cols), f32),
            pltpu.VMEM((3, EARLY, BLK, BLK), f32),
            pltpu.VMEM((2 * rows, LANES), f32),
            pltpu.VMEM((2 * rows, LANES), f32),
            pltpu.VMEM((tiles, LANES), f32),
            pltpu.VMEM((3, rows, LANES), f32),
            pltpu.VMEM((2, tiles, LANES), f32),
            pltpu.VMEM((2, DEV // 2, tiles, LANES), f32),
            pltpu.VMEM((tiles + SUB, LANES), f32),
            pltpu.VMEM((4, tiles + SUB, LANES), f32),
            pltpu.VMEM((rows // LANES, LANES), f32),
            pltpu.SemaphoreType.DMA((2 * nblk + 3,)),
            pltpu.SemaphoreType.DMA((7, nblk + 1)),
            pltpu.SemaphoreType.DMA((DEV, nblk + 1)),
            pltpu.SemaphoreType.DMA((7, nblk)),
            pltpu.SemaphoreType.DMA((DEV, nblk)),
            pltpu.SemaphoreType.DMA((2, 3)),
            pltpu.SemaphoreType.DMA((2, DEV // 2)),
            pltpu.SemaphoreType.DMA((5,)),
            pltpu.SemaphoreType.DMA((5,)),
            pltpu.SemaphoreType.DMA((3, EARLY)),
            pltpu.SemaphoreType.DMA((3, EARLY)),
            pltpu.SemaphoreType.DMA((4,)),
            pltpu.SemaphoreType.DMA((4,)),
        ],
        compiler_params=pltpu.CompilerParams(collective_id=0, has_side_effects=True, vmem_limit_bytes=60 << 20),
        name="fgw",
    )(eps, mass, q, src, tgt, plan, fsrc, ftgt)


def solution(mesh):
    def local_fgw(cost_src, cost_tgt, plan_init, mass_src, mass_tgt, feat_src, feat_tgt, epsilon):
        return fgw(
            cost_src, cost_tgt, plan_init, mass_src.reshape(-1, LANES), mass_tgt.reshape(-1, LANES),
            feat_src, feat_tgt, epsilon.reshape(1))

    row_spec = P(('pairs', 'rows'), None)
    vec_spec = P(('pairs', 'rows'))
    in_specs = (row_spec, row_spec, row_spec, vec_spec, P('pairs'), row_spec, row_spec, P())
    return jax.shard_map(local_fgw, mesh=mesh, in_specs=in_specs, out_specs=row_spec, check_vma=False)
```

```python
import functools

import jax
import jax.numpy as jnp
from jax import lax
from jax.experimental import pallas as pl
from jax.experimental.pallas import tpu as pltpu
from jax.sharding import PartitionSpec as P

ALPHA = 0.5
OUTER_STEPS = 2
SWEEPS = 10
LANES = 128
SUB = 8
BLK = 256
DEV = 8
AHEAD = 2
LAG = 2
EARLY = 7


def tree_sum(vals):
    while len(vals) > 1:
        vals = [a + b for a, b in zip(vals[::2], vals[1::2])] + vals[len(vals) & ~1:]
    return vals[0]


def rows_of(owner):
    return pl.ds(pl.multiple_of(owner * BLK, BLK), BLK)


class Place:
    def __init__(self):
        self.me = lax.axis_index("rows")
        core = lax.rem(self.me, 2)
        x = lax.rem(self.me // 2, 2)
        y = self.me // 4
        self.core = core
        self.sib = self.me + 1 - 2 * core
        dx, dy = 2 - 4 * x, 4 - 8 * y
        self.x0, self.x1 = self.me + dx, self.sib + dx
        self.y0, self.y1 = self.me + dy, self.sib + dy
        self.d0, self.d1 = self.me + dx + dy, self.sib + dx + dy


def build_kernel(cost_ref, kern_ref, eps, half, rows, cols):
    tiles = cols // LANES
    inv_eps = 1.0 / jnp.full((SUB, LANES), eps, jnp.float32)

    def block(b, carry):
        row = pl.multiple_of(b * SUB, SUB)
        at_row = pl.ds(half * rows + row, SUB)
        vals = [cost_ref[at_row, t * LANES:(t + 1) * LANES] for t in range(tiles)]
        low = functools.reduce(jnp.minimum, vals)
        low = jnp.min(low, axis=1, keepdims=True)
        for t in range(tiles):
            kern_ref[half, pl.ds(row, SUB), t * LANES:(t + 1) * LANES] = jnp.exp((low - vals[t]) * inv_eps)
        return carry

    lax.fori_loop(0, rows // SUB, block, 0, unroll=4)


def spread(line, eye):
    wide = jnp.broadcast_to(line, (LANES, LANES))
    col = jnp.sum(jnp.where(eye, wide, 0.0), axis=1, keepdims=True)
    return jnp.broadcast_to(col, (LANES, LANES))


def sinkhorn(at, kern_ref, p_ref, q_ref, u_ref, v_ref, part_ref, gath_ref, send_sem, recv_sem):
    halves, rows, cols = kern_ref.shape
    tiles = cols // LANES
    blocks = [(h, b) for h in range(halves) for b in range(rows // SUB)]
    chip = at.me // 2
    peers = (at.x0, at.y0, at.d0)

    def copy(par, k, slot):
        return pltpu.make_async_remote_copy(
            src_ref=part_ref.at[par], dst_ref=gath_ref.at[par, slot],
            send_sem=send_sem.at[par, k], recv_sem=recv_sem.at[par, slot], device_id={"rows": peers[k]})

    v_ref[...] = jnp.ones_like(v_ref)

    def sweep(step, carry):
        par = lax.rem(step, 2)
        vrow = [jnp.broadcast_to(v_ref[t:t + 1, :], (SUB, LANES)) for t in range(tiles)]
        for h, b in blocks:
            prods = [kern_ref[h, b * SUB:(b + 1) * SUB, t * LANES:(t + 1) * LANES] * vrow[t] for t in range(tiles)]
            dots = jnp.sum(tree_sum(prods), axis=1, keepdims=True)
            at_row = slice(h * rows + b * SUB, h * rows + (b + 1) * SUB)
            u_ref[at_row, :] = p_ref[at_row, :] / dots
        acc = [None] * tiles
        for h, b in blocks:
            scale = u_ref[h * rows + b * SUB:h * rows + (b + 1) * SUB, :]
            for t in range(tiles):
                term = kern_ref[h, b * SUB:(b + 1) * SUB, t * LANES:(t + 1) * LANES] * scale
                acc[t] = term if acc[t] is None else acc[t] + term
        sums = jnp.concatenate([jnp.sum(a, axis=0, keepdims=True) for a in acc], axis=0)
        part_ref[par] = sums
        for k in (2, 0, 1):
            copy(par, k, chip).start()
        gath_ref[par, chip] = sums
        for k in range(3):
            copy(par, k, peers[k] // 2).wait_recv()
        total = gath_ref[par, 0]
        for d in range(1, DEV // 2):
            total = total + gath_ref[par, d]
        v_ref[...] = q_ref[...] / total
        for k in range(3):
            copy(par, k, chip).wait_send()
        return carry

    lax.fori_loop(0, SWEEPS, sweep, 0)


def plan_block(kern, scale, v_ref, j):
    parts = []
    for h in range(BLK // LANES):
        vrow = v_ref[pl.ds(j * (BLK // LANES) + h, 1), :]
        parts.append(scale * kern(h) * vrow)
    return jnp.concatenate(parts, axis=1)


def gather_plan(at, chunks, plan_ref, send_sem, recv_sem, produce, near_end, column, form=None):
    def copy(owner, j, dest, kind):
        view = plan_ref.at[j, rows_of(owner), :]
        return pltpu.make_async_remote_copy(
            src_ref=view, dst_ref=view, send_sem=send_sem.at[kind, j],
            recv_sem=recv_sem.at[owner, j], device_id={"rows": dest})

    def over_links(j):
        return True if form is None else (at.core == 1) | (j >= EARLY)

    def when(cond):
        return (lambda f: f()) if cond is True else pl.when(cond)

    def send_own(j):
        @when(over_links(j))
        def _():
            copy(at.me, j, at.x0, 0).start()
            copy(at.me, j, at.y0, 1).start()

        copy(at.me, j, at.sib, 2).start()

    for j in range(AHEAD):
        produce(j)
        send_own(j)

    def turn(it, carry):
        @pl.when(it + AHEAD < chunks)
        def _():
            produce(it + AHEAD)
            send_own(it + AHEAD)

        @pl.when((it < chunks) & over_links(it))
        def _():
            copy(at.x0, it, at.x0, 0).wait_recv()
            copy(at.x0, it, at.sib, 3).start()

            @pl.when(lax.rem(it, 2) == 0)
            def _():
                copy(at.x0, it, at.y0, 6).start()

            copy(at.y0, it, at.y0, 0).wait_recv()
            copy(at.y0, it, at.sib, 4).start()

            @pl.when(lax.rem(it, 2) == 1)
            def _():
                copy(at.y0, it, at.x0, 6).start()

        if form is not None:
            @pl.when((it < chunks) & (at.core == 0) & (it < EARLY))
            def _():
                for k, owner in enumerate((at.x0, at.y0, at.d0)):
                    plan_ref[it, rows_of(owner), :] = form(k, it).astype(jnp.bfloat16)
                    copy(owner, it, at.sib, 3 + k).start()

        @pl.when(it == chunks - 1)
        def _():
            near_end()

        @pl.when((it >= LAG) & (it < LAG + chunks) & over_links(it - LAG))
        def _():
            copy(at.d0, it - LAG, at.d0, 0).wait_recv()
            copy(at.d0, it - LAG, at.sib, 5).start()

        @pl.when(it >= LAG + 1)
        def _():
            j = it - LAG - 1
            for owner in (at.sib, at.x1, at.y1, at.d1):
                copy(owner, j, at.sib, 0).wait_recv()
            column(j)

        return carry

    lax.fori_loop(0, chunks + LAG + 1, turn, 0)

    def drain(j, carry):
        for kind in (2, 3, 4, 5):
            copy(at.me, j, at.sib, kind).wait_send()

        @when(over_links(j))
        def _():
            for kind in (0, 1, 6):
                copy(at.me, j, at.sib, kind).wait_send()

        return carry

    lax.fori_loop(0, chunks, drain, 0)


def fgw_kernel(
    eps_ref, mass_ref, q_ref, src_hbm, tgt_hbm, plan_hbm, fsrc_hbm, ftgt_hbm, out_ref,
    stage_ref, stage2_ref, feat_ref, plan_ref, tgt_ref, src_ref, fsrc_ref, a_ref, cross_ref, cost_ref, kern_ref,
    early_ref, p_ref, u_ref, v_ref, other_ref, part_ref, gath_ref, msg_ref, news_ref, mass2_ref,
    load_sem, plan_send, plan_recv, tgt_send, tgt_recv, sum_send, sum_recv, a_send, a_recv, swap_send, swap_recv,
    early_send, early_recv, msg_send, msg_recv,
):
    at = Place()
    me = at.me
    _, rows, cols = kern_ref.shape
    nblk = cols // BLK
    eps = eps_ref[0]

    def load_plan(j):
        return pltpu.make_async_copy(plan_hbm.at[:, pl.ds(pl.multiple_of(j * BLK, BLK), BLK)], stage_ref.at[j], load_sem.at[j])

    def load_tgt(j):
        return pltpu.make_async_copy(tgt_hbm.at[:, pl.ds(pl.multiple_of(j * BLK, BLK), BLK)], stage2_ref.at[j], load_sem.at[nblk + j])

    load_feat = pltpu.make_async_copy(ftgt_hbm, feat_ref.at[0], load_sem.at[2 * nblk])
    load_fsrc = pltpu.make_async_copy(fsrc_hbm, feat_ref.at[1], load_sem.at[2 * nblk + 1])
    load_src = pltpu.make_async_copy(src_hbm, cost_ref.at[:rows], load_sem.at[2 * nblk + 2])

    for j in range(nblk):
        load_plan(j).start()
    load_feat.start()
    load_fsrc.start()
    load_src.start()
    for j in range(nblk):
        load_tgt(j).start()

    barrier = pltpu.get_barrier_semaphore()
    for off in range(1, DEV):
        pl.semaphore_signal(barrier, inc=1, device_id={"rows": lax.rem(me + off, DEV)})

    pl.semaphore_wait(barrier, DEV - 1)

    swap = pltpu.make_async_remote_copy(
        src_ref=mass_ref, dst_ref=mass2_ref, send_sem=swap_send.at[0], recv_sem=swap_recv.at[0], device_id={"rows": at.sib})
    swap.start()
    swap_feat = pltpu.make_async_remote_copy(
        src_ref=fsrc_ref.at[:BLK], dst_ref=fsrc_ref.at[BLK:], send_sem=swap_send.at[1], recv_sem=swap_recv.at[1],
        device_id={"rows": at.sib})
    eye = lax.broadcasted_iota(jnp.int32, (LANES, LANES), 0) == lax.broadcasted_iota(jnp.int32, (LANES, LANES), 1)

    def cast_plan(j):
        if isinstance(j, int):
            load_plan(j).wait()
            plan_ref[j, rows_of(me), :] = stage_ref[j].astype(jnp.bfloat16)
            return

        @pl.when(j < nblk)
        def _():
            load_plan(j).wait()
            plan_ref[j, rows_of(me), :] = stage_ref[j].astype(jnp.bfloat16)

        @pl.when(j == nblk)
        def _():
            load_feat.wait()
            plan_ref[nblk, rows_of(me), :] = feat_ref[0].astype(jnp.bfloat16)

        @pl.when(j == AHEAD)
        def _():
            load_fsrc.wait()
            fsrc_ref[:BLK] = feat_ref[1].astype(jnp.bfloat16)
            swap_feat.start()
            load_src.wait()
            src_ref[...] = cost_ref[:rows, :].astype(jnp.bfloat16)

        @pl.when(j < nblk)
        def _():
            load_tgt(j).wait()
            tgt_ref[j, rows_of(me), :] = stage2_ref[j].astype(jnp.bfloat16)

    def tcopy(owner, col, dest, kind):
        view = tgt_ref.at[col, rows_of(owner), :]
        return pltpu.make_async_remote_copy(
            src_ref=view, dst_ref=view, send_sem=tgt_send.at[kind, col],
            recv_sem=tgt_recv.at[owner, col], device_id={"rows": dest})

    out_x = (at.me, at.sib, at.y0, at.y1, at.d0)
    out_y = (at.me, at.sib, at.x0, at.x1, at.d1)
    in_x = (at.x0, at.x1, at.d0, at.d1, at.y0)
    in_y = (at.y0, at.y1, at.d0, at.d1, at.x1)

    def send_tgt():
        for j in range(AHEAD):
            load_tgt(j).wait()
            tgt_ref[j, rows_of(me), :] = stage2_ref[j].astype(jnp.bfloat16)
        for cx, cy in zip(out_x, out_y):
            tcopy(me, cx, at.x0, 0).start()
            tcopy(me, cy, at.y0, 1).start()

        def to_sib(j, carry):
            tcopy(me, j, at.sib, 2).start()
            return carry

        lax.fori_loop(0, nblk, to_sib, 0)

    def a_copy(j):
        cols_at = pl.ds(pl.multiple_of(j * BLK, BLK), BLK)
        return pltpu.make_async_remote_copy(
            src_ref=a_ref.at[:rows, cols_at], dst_ref=a_ref.at[rows:, cols_at], send_sem=a_send.at[j],
            recv_sem=a_recv.at[j], device_id={"rows": at.sib})

    def make_column(j):
        prod = jnp.dot(src_ref[...], plan_ref[j], preferred_element_type=jnp.float32)
        a_ref[:rows, pl.ds(pl.multiple_of(j * BLK, BLK), BLK)] = prod.astype(jnp.bfloat16)

        @pl.when(at.core == 0)
        def _():
            a_copy(j).start()

    def first_column(j):
        @pl.when(j < nblk)
        def _():
            make_column(j)

    gather_plan(at, nblk + 1, plan_ref, plan_send, plan_recv, cast_plan, send_tgt, first_column)

    def on_reach(f):
        @pl.when(at.core == 1)
        def _():
            f(2 * rows)

        @pl.when(at.core == 0)
        def _():
            f(rows)

    swap.wait()
    swap_feat.wait()
    for r in range(rows // LANES):
        p_ref[r * LANES:(r + 1) * LANES, :] = spread(mass_ref[r:r + 1, :], eye)
        p_ref[rows + r * LANES:rows + (r + 1) * LANES, :] = spread(mass2_ref[r:r + 1, :], eye)

    def crosses(reach):
        def cross(j, carry):
            prod = lax.dot_general(
                fsrc_ref[:reach, :], plan_ref[nblk, rows_of(j), :], (((1,), (1,)), ((), ())),
                preferred_element_type=jnp.float32)
            where = pl.ds(pl.multiple_of(j * BLK, BLK), BLK)
            cross_ref[:reach, where] = (-2.0 * ALPHA) * prod
            cost_ref[:reach, where] = (-2.0 * ALPHA) * prod
            return carry

        lax.fori_loop(0, nblk, cross, 0)

    on_reach(crosses)

    @pl.when(at.core == 1)
    def _():
        def arrived(j, carry):
            a_copy(j).wait_recv()
            return carry

        lax.fori_loop(0, nblk, arrived, 0)

    def term(reach, i, col):
        lhs = a_ref[:reach, pl.ds(pl.multiple_of(i * BLK, BLK), BLK)]
        prod = jnp.dot(lhs, tgt_ref[col, rows_of(i), :], preferred_element_type=jnp.float32)
        return (2.0 * (1.0 - ALPHA)) * prod

    def add(i, col):
        def go(reach):
            where = pl.ds(pl.multiple_of(col * BLK, BLK), BLK)
            cost_ref[:reach, where] = cost_ref[:reach, where] - term(reach, i, col)

        on_reach(go)

    def mirror(owner, col):
        tgt_ref[owner, rows_of(col), :] = tgt_ref[col, rows_of(owner), :].T

    def use(owner, col, paired):
        add(owner, col)

        @pl.when(paired)
        def _():
            mirror(owner, col)
            add(col, owner)

    base = me - at.core

    def use_row(owner):
        def body(t, carry):
            use(owner, lax.rem(base + t, DEV), t >= 2)
            return carry

        lax.fori_loop(0, DEV, body, 0)

    use_row(me)

    def stream(k, s, other):
        core = lax.rem(at.core + other, 2)
        xb, yb, db = at.x0 - at.core, at.y0 - at.core, at.d0 - at.core
        near = xb + s * (yb - xb)
        far = yb + s * (xb - yb)
        which = k // 2
        chip = jnp.where(which == 0, near, jnp.where(which == 1, db, far))
        flip = jnp.where(which == 2, s, 0)
        return near + core, chip + lax.rem(core + k + flip, 2)

    def arrivals(k, carry):
        for s, fwd in ((0, 3), (1, 4)):
            owner, col = stream(k, s, 0)
            tcopy(owner, col, at.sib, 0).wait_recv()
            tcopy(owner, col, at.sib, fwd).start()
            if s == 0:
                @pl.when(k == 1)
                def _():
                    tcopy(at.x0, at.x1, at.y0, 6).start()
            else:
                @pl.when(k == 0)
                def _():
                    tcopy(at.y0, at.y0, at.x0, 6).start()

        @pl.when(k == 0)
        def _():
            def from_sib(j, c):
                tcopy(at.sib, j, at.sib, 0).wait_recv()
                return c

            lax.fori_loop(0, nblk, from_sib, 0)
            use_row(at.sib)

        def near(s, c):
            use(*stream(k, s, 0), k >= 2)
            return c

        lax.fori_loop(0, 2, near, 0)

        def near_other(s, c):
            owner, col = stream(k, s, 1)
            tcopy(owner, col, at.sib, 0).wait_recv()
            use(owner, col, k >= 2)
            return c

        lax.fori_loop(0, 2, near_other, 0)
        return carry

    lax.fori_loop(0, 5, arrivals, 0)
    for col in (at.d0, at.d1):
        tcopy(at.d0, col, at.d0, 0).wait_recv()
        tcopy(at.d0, col, at.sib, 5).start()

    def diag(t, carry):
        owner = at.d0 + (t // 2) * (at.d1 - at.d0)
        col = at.d0 + lax.rem(t, 2) * (at.d1 - at.d0)

        @pl.when(t >= 2)
        def _():
            tcopy(owner, col, at.sib, 0).wait_recv()

        add(owner, col)
        return carry

    lax.fori_loop(0, 4, diag, 0)

    for cx, cy in zip(out_x, out_y):
        tcopy(me, cx, at.x0, 0).wait_send()
        tcopy(me, cy, at.y0, 1).wait_send()
    for k in range(5):
        tcopy(at.x0, in_x[k], at.sib, 3).wait_send()
        tcopy(at.y0, in_y[k], at.sib, 4).wait_send()
    for col in (at.d0, at.d1):
        tcopy(at.d0, col, at.sib, 5).wait_send()
    tcopy(at.x0, at.x1, at.y0, 6).wait_send()
    tcopy(at.y0, at.y0, at.x0, 6).wait_send()

    def sib_done(j, carry):
        tcopy(me, j, at.sib, 2).wait_send()
        return carry

    lax.fori_loop(0, nblk, sib_done, 0)

    def a_done():
        @pl.when(at.core == 0)
        def _():
            def body(j, carry):
                a_copy(j).wait_send()
                return carry

            lax.fori_loop(0, nblk, body, 0)

    a_done()

    def early(src, j, slot, dest, kind):
        return pltpu.make_async_remote_copy(
            src_ref=src, dst_ref=early_ref.at[slot, j], send_sem=early_send.at[kind, j],
            recv_sem=early_recv.at[slot, j], device_id={"rows": dest})

    def own_part(j):
        return kern_ref.at[0, :, pl.ds(pl.multiple_of(j * BLK, BLK), BLK)]

    def early_round():
        def send(j):
            early(own_part(j), j, 0, at.x0, 0).start()
            early(own_part(j), j, 1, at.y0, 1).start()

        for j in range(AHEAD):
            send(j)

        def turn(j, carry):
            @pl.when(j + AHEAD < EARLY)
            def _():
                send(j + AHEAD)

            early(own_part(j), j, 0, at.x0, 0).wait_recv()

            @pl.when(lax.rem(j, 2) == 0)
            def _():
                early(early_ref.at[0, j], j, 2, at.y0, 2).start()

            early(own_part(j), j, 1, at.y0, 1).wait_recv()

            @pl.when(lax.rem(j, 2) == 1)
            def _():
                early(early_ref.at[1, j], j, 2, at.x0, 2).start()

            return carry

        lax.fori_loop(0, EARLY, turn, 0)

        def done(j, carry):
            early(own_part(j), j, 2, at.x0, 2).wait_recv()
            for kind in range(3):
                early(own_part(j), j, kind, at.x0, kind).wait_send()
            return carry

        lax.fori_loop(0, EARLY, done, 0)

    tiles = cols // LANES
    across = (at.sib, at.x1, at.y1, at.d1)

    def news(k):
        return pltpu.make_async_remote_copy(
            src_ref=msg_ref, dst_ref=news_ref.at[k], send_sem=msg_send.at[k], recv_sem=msg_recv.at[k],
            device_id={"rows": across[k]})

    def sweeps(first):
        reach = len(across) if first else 1
        build_kernel(cost_ref, kern_ref, eps, 0, rows, cols)

        @pl.when(at.core == 1)
        def _():
            build_kernel(cost_ref, kern_ref, eps, 1, rows, cols)
            sinkhorn(at, kern_ref, p_ref, q_ref, u_ref, v_ref, part_ref, gath_ref, sum_send, sum_recv)
            msg_ref[:tiles] = v_ref[...]
            msg_ref[tiles:] = jnp.zeros_like(msg_ref[tiles:])
            for r in range(rows // LANES):
                scale = u_ref[rows + r * LANES:rows + (r + 1) * LANES, :]
                msg_ref[tiles + r:tiles + r + 1] = jnp.sum(jnp.where(eye, scale, 0.0), axis=0, keepdims=True)
            for k in range(reach):
                news(k).start()
            for k in range(reach):
                news(k).wait_send()

        @pl.when(at.core == 0)
        def _():
            if first:
                early_round()
            for k in range(reach):
                news(k).wait_recv()
            v_ref[...] = news_ref[0, :tiles]
            for r in range(rows // LANES):
                u_ref[r * LANES:(r + 1) * LANES, :] = spread(news_ref[0, tiles + r:tiles + r + 1], eye)
                for k in range(1, reach):
                    other_ref[k - 1, r * LANES:(r + 1) * LANES, :] = spread(news_ref[k, tiles + r:tiles + r + 1], eye)

    def own_block(j):
        cols_at = pl.multiple_of(j * BLK, BLK)
        return plan_block(lambda h: kern_ref[0, :, pl.ds(cols_at + h * LANES, LANES)], u_ref[:rows, :], v_ref, j)

    sweeps(True)

    def next_plan(j):
        plan_ref[j, rows_of(me), :] = own_block(j).astype(jnp.bfloat16)

    def form(k, j):
        return plan_block(lambda h: early_ref[k, j, :, h * LANES:(h + 1) * LANES], other_ref[k], v_ref, j)

    def add_column(j):
        @pl.when(at.core == 1)
        def _():
            a_copy(j).wait_recv()

        def go(reach):
            def body(col, carry):
                where = pl.ds(pl.multiple_of(col * BLK, BLK), BLK)

                @pl.when(j == 0)
                def _():
                    cost_ref[:reach, where] = cross_ref[:reach, where] - term(reach, j, col)

                @pl.when(j > 0)
                def _():
                    cost_ref[:reach, where] = cost_ref[:reach, where] - term(reach, j, col)

                return carry

            lax.fori_loop(0, nblk, body, 0)

        on_reach(go)

    def second_column(j):
        make_column(j)

        @pl.when(j > 0)
        def _():
            add_column(j - 1)

    gather_plan(at, nblk, plan_ref, plan_send, plan_recv, next_plan, lambda: None, second_column, form)
    add_column(nblk - 1)
    a_done()
    sweeps(False)

    for j in range(nblk):
        out_ref[:, j * BLK:(j + 1) * BLK] = own_block(j)


def fgw(src, tgt, plan, mass, q, fsrc, ftgt, eps):
    rows, cols = plan.shape
    tiles = cols // LANES
    nblk = cols // BLK
    vmem = pl.BlockSpec(memory_space=pltpu.VMEM)
    hbm = pl.BlockSpec(memory_space=pltpu.HBM)
    f32, bf16 = jnp.float32, jnp.bfloat16
    return pl.pallas_call(
        fgw_kernel,
        out_shape=jax.ShapeDtypeStruct((rows, cols), f32),
        in_specs=[pl.BlockSpec(memory_space=pltpu.SMEM), vmem, vmem] + [hbm] * 5,
        out_specs=vmem,
        scratch_shapes=[
            pltpu.VMEM((nblk, BLK, BLK), f32),
            pltpu.VMEM((nblk, BLK, BLK), f32),
            pltpu.VMEM((2, BLK, BLK), f32),
            pltpu.VMEM((nblk + 1, DEV * BLK, BLK), bf16),
            pltpu.VMEM((nblk, DEV * BLK, BLK), bf16),
            pltpu.VMEM((rows, cols), bf16),
            pltpu.VMEM((2 * BLK, BLK), bf16),
            pltpu.VMEM((2 * rows, cols), bf16),
            pltpu.VMEM((2 * rows, cols), f32),
            pltpu.VMEM((2 * rows, cols), f32),
            pltpu.VMEM((2, rows, cols), f32),
            pltpu.VMEM((3, EARLY, BLK, BLK), f32),
            pltpu.VMEM((2 * rows, LANES), f32),
            pltpu.VMEM((2 * rows, LANES), f32),
            pltpu.VMEM((tiles, LANES), f32),
            pltpu.VMEM((3, rows, LANES), f32),
            pltpu.VMEM((2, tiles, LANES), f32),
            pltpu.VMEM((2, DEV // 2, tiles, LANES), f32),
            pltpu.VMEM((tiles + SUB, LANES), f32),
            pltpu.VMEM((4, tiles + SUB, LANES), f32),
            pltpu.VMEM((rows // LANES, LANES), f32),
            pltpu.SemaphoreType.DMA((2 * nblk + 3,)),
            pltpu.SemaphoreType.DMA((7, nblk + 1)),
            pltpu.SemaphoreType.DMA((DEV, nblk + 1)),
            pltpu.SemaphoreType.DMA((7, nblk)),
            pltpu.SemaphoreType.DMA((DEV, nblk)),
            pltpu.SemaphoreType.DMA((2, 3)),
            pltpu.SemaphoreType.DMA((2, DEV // 2)),
            pltpu.SemaphoreType.DMA((nblk,)),
            pltpu.SemaphoreType.DMA((nblk,)),
            pltpu.SemaphoreType.DMA((2,)),
            pltpu.SemaphoreType.DMA((2,)),
            pltpu.SemaphoreType.DMA((3, EARLY)),
            pltpu.SemaphoreType.DMA((3, EARLY)),
            pltpu.SemaphoreType.DMA((4,)),
            pltpu.SemaphoreType.DMA((4,)),
        ],
        compiler_params=pltpu.CompilerParams(collective_id=0, has_side_effects=True, vmem_limit_bytes=50 << 20),
        name="fgw",
    )(eps, mass, q, src, tgt, plan, fsrc, ftgt)


def solution(mesh):
    def local_fgw(cost_src, cost_tgt, plan_init, mass_src, mass_tgt, feat_src, feat_tgt, epsilon):
        return fgw(
            cost_src, cost_tgt, plan_init, mass_src.reshape(-1, LANES), mass_tgt.reshape(-1, LANES),
            feat_src, feat_tgt, epsilon.reshape(1))

    row_spec = P(('pairs', 'rows'), None)
    vec_spec = P(('pairs', 'rows'))
    in_specs = (row_spec, row_spec, row_spec, vec_spec, P('pairs'), row_spec, row_spec, P())
    return jax.shard_map(local_fgw, mesh=mesh, in_specs=in_specs, out_specs=row_spec, check_vma=False)
```

```python
import functools

import jax
import jax.numpy as jnp
from jax import lax
from jax.experimental import pallas as pl
from jax.experimental.pallas import tpu as pltpu
from jax.sharding import PartitionSpec as P

ALPHA = 0.5
OUTER_STEPS = 2
SWEEPS = 10
LANES = 128
SUB = 8
BLK = 256
DEV = 8
AHEAD = 2
LAG = 2
EARLY = 7


def tree_sum(vals):
    while len(vals) > 1:
        vals = [a + b for a, b in zip(vals[::2], vals[1::2])] + vals[len(vals) & ~1:]
    return vals[0]


def rows_of(owner):
    return pl.ds(pl.multiple_of(owner * BLK, BLK), BLK)


class Place:
    def __init__(self):
        self.me = lax.axis_index("rows")
        core = lax.rem(self.me, 2)
        x = lax.rem(self.me // 2, 2)
        y = self.me // 4
        self.core = core
        self.sib = self.me + 1 - 2 * core
        dx, dy = 2 - 4 * x, 4 - 8 * y
        self.x0, self.x1 = self.me + dx, self.sib + dx
        self.y0, self.y1 = self.me + dy, self.sib + dy
        self.d0, self.d1 = self.me + dx + dy, self.sib + dx + dy


def build_kernel(cost_ref, kern_ref, eps, half, rows, cols):
    tiles = cols // LANES
    inv_eps = 1.0 / jnp.full((SUB, LANES), eps, jnp.float32)

    def block(b, carry):
        row = pl.multiple_of(b * SUB, SUB)
        at_row = pl.ds(half * rows + row, SUB)
        vals = [cost_ref[at_row, t * LANES:(t + 1) * LANES] for t in range(tiles)]
        low = functools.reduce(jnp.minimum, vals)
        low = jnp.min(low, axis=1, keepdims=True)
        for t in range(tiles):
            kern_ref[half, pl.ds(row, SUB), t * LANES:(t + 1) * LANES] = jnp.exp((low - vals[t]) * inv_eps)
        return carry

    lax.fori_loop(0, rows // SUB, block, 0, unroll=8)


def spread(line, eye):
    wide = jnp.broadcast_to(line, (LANES, LANES))
    col = jnp.sum(jnp.where(eye, wide, 0.0), axis=1, keepdims=True)
    return jnp.broadcast_to(col, (LANES, LANES))


def sinkhorn(at, kern_ref, p_ref, q_ref, u_ref, v_ref, part_ref, gath_ref, send_sem, recv_sem):
    halves, rows, cols = kern_ref.shape
    tiles = cols // LANES
    blocks = [(h, b) for h in range(halves) for b in range(rows // SUB)]
    chip = at.me // 2
    peers = (at.x0, at.y0, at.d0)

    def copy(par, k, slot):
        return pltpu.make_async_remote_copy(
            src_ref=part_ref.at[par], dst_ref=gath_ref.at[par, slot],
            send_sem=send_sem.at[par, k], recv_sem=recv_sem.at[par, slot], device_id={"rows": peers[k]})

    v_ref[...] = jnp.ones_like(v_ref)

    def sweep(step, carry):
        par = lax.rem(step, 2)
        vrow = [jnp.broadcast_to(v_ref[t:t + 1, :], (SUB, LANES)) for t in range(tiles)]
        for h, b in blocks:
            prods = [kern_ref[h, b * SUB:(b + 1) * SUB, t * LANES:(t + 1) * LANES] * vrow[t] for t in range(tiles)]
            dots = jnp.sum(tree_sum(prods), axis=1, keepdims=True)
            at_row = slice(h * rows + b * SUB, h * rows + (b + 1) * SUB)
            u_ref[at_row, :] = p_ref[at_row, :] / dots
        acc = [None] * tiles
        for h, b in blocks:
            scale = u_ref[h * rows + b * SUB:h * rows + (b + 1) * SUB, :]
            for t in range(tiles):
                term = kern_ref[h, b * SUB:(b + 1) * SUB, t * LANES:(t + 1) * LANES] * scale
                acc[t] = term if acc[t] is None else acc[t] + term
        sums = jnp.concatenate([jnp.sum(a, axis=0, keepdims=True) for a in acc], axis=0)
        part_ref[par] = sums
        for k in (2, 0, 1):
            copy(par, k, chip).start()
        gath_ref[par, chip] = sums
        for k in range(3):
            copy(par, k, peers[k] // 2).wait_recv()
        total = gath_ref[par, 0]
        for d in range(1, DEV // 2):
            total = total + gath_ref[par, d]
        v_ref[...] = q_ref[...] / total
        for k in range(3):
            copy(par, k, chip).wait_send()
        return carry

    lax.fori_loop(0, SWEEPS, sweep, 0)


def plan_block(kern, scale, v_ref, j):
    parts = []
    for h in range(BLK // LANES):
        vrow = v_ref[pl.ds(j * (BLK // LANES) + h, 1), :]
        parts.append(scale * kern(h) * vrow)
    return jnp.concatenate(parts, axis=1)


def gather_plan(at, chunks, plan_ref, send_sem, recv_sem, produce, column, form=None):
    def copy(owner, j, dest, kind):
        view = plan_ref.at[j, rows_of(owner), :]
        return pltpu.make_async_remote_copy(
            src_ref=view, dst_ref=view, send_sem=send_sem.at[kind, j],
            recv_sem=recv_sem.at[owner, j], device_id={"rows": dest})

    def over_links(j):
        return True if form is None else (at.core == 1) | (j >= EARLY)

    def when(cond):
        return (lambda f: f()) if cond is True else pl.when(cond)

    def send_own(j):
        @when(over_links(j))
        def _():
            copy(at.me, j, at.x0, 0).start()
            copy(at.me, j, at.y0, 1).start()

        copy(at.me, j, at.sib, 2).start()

    def begin():
        for j in range(AHEAD):
            produce(j)
            send_own(j)

    def turn(it, carry):
        @pl.when(it + AHEAD < chunks)
        def _():
            produce(it + AHEAD)
            send_own(it + AHEAD)

        @pl.when((it < chunks) & over_links(it))
        def _():
            copy(at.x0, it, at.x0, 0).wait_recv()
            copy(at.x0, it, at.sib, 3).start()

            @pl.when(lax.rem(it, 2) == 0)
            def _():
                copy(at.x0, it, at.y0, 6).start()

            copy(at.y0, it, at.y0, 0).wait_recv()
            copy(at.y0, it, at.sib, 4).start()

            @pl.when(lax.rem(it, 2) == 1)
            def _():
                copy(at.y0, it, at.x0, 6).start()

        if form is not None:
            @pl.when((it < chunks) & (at.core == 0) & (it < EARLY))
            def _():
                for k, owner in enumerate((at.x0, at.y0, at.d0)):
                    plan_ref[it, rows_of(owner), :] = form(k, it).astype(jnp.bfloat16)
                    copy(owner, it, at.sib, 3 + k).start()

        @pl.when((it >= LAG) & (it < LAG + chunks) & over_links(it - LAG))
        def _():
            copy(at.d0, it - LAG, at.d0, 0).wait_recv()
            copy(at.d0, it - LAG, at.sib, 5).start()

        @pl.when(it >= LAG + 1)
        def _():
            j = it - LAG - 1
            for owner in (at.sib, at.x1, at.y1, at.d1):
                copy(owner, j, at.sib, 0).wait_recv()
            column(j)

        return carry

    def drain(j, carry):
        for kind in (2, 3, 4, 5):
            copy(at.me, j, at.sib, kind).wait_send()

        @when(over_links(j))
        def _():
            for kind in (0, 1, 6):
                copy(at.me, j, at.sib, kind).wait_send()

        return carry

    def go_on():
        lax.fori_loop(0, chunks + LAG + 1, turn, 0)
        lax.fori_loop(0, chunks, drain, 0)

    return begin, go_on


def fgw_kernel(
    eps_ref, mass_hbm, q_hbm, src_hbm, tgt_hbm, plan_hbm, fsrc_hbm, ftgt_hbm, out_ref,
    stage_ref, stage2_ref, feat_ref, plan_ref, tgt_ref, src_ref, fsrc_ref, ftgt_ref, a_ref, cross_ref, cost_ref, kern_ref,
    early_ref, p_ref, q_ref, u_ref, v_ref, other_ref, part_ref, gath_ref, msg_ref, news_ref, mass_ref, mass2_ref,
    load_sem, plan_send, plan_recv, tgt_send, tgt_recv, feat_send, feat_recv, sum_send, sum_recv, a_send, a_recv,
    swap_send, swap_recv, early_send, early_recv, msg_send, msg_recv,
):
    at = Place()
    me = at.me
    _, rows, cols = kern_ref.shape
    nblk = cols // BLK
    eps = eps_ref[0]

    def load_plan(j):
        return pltpu.make_async_copy(plan_hbm.at[:, pl.ds(pl.multiple_of(j * BLK, BLK), BLK)], stage_ref.at[j], load_sem.at[j])

    def load_tgt(j):
        return pltpu.make_async_copy(tgt_hbm.at[:, pl.ds(pl.multiple_of(j * BLK, BLK), BLK)], stage2_ref.at[j], load_sem.at[nblk + j])

    load_feat = pltpu.make_async_copy(ftgt_hbm, feat_ref.at[0], load_sem.at[2 * nblk])
    load_fsrc = pltpu.make_async_copy(fsrc_hbm, feat_ref.at[1], load_sem.at[2 * nblk + 1])
    load_src = pltpu.make_async_copy(src_hbm, cost_ref.at[:rows], load_sem.at[2 * nblk + 2])
    load_mass = pltpu.make_async_copy(mass_hbm, mass_ref, load_sem.at[2 * nblk + 3])
    load_q = pltpu.make_async_copy(q_hbm, q_ref, load_sem.at[2 * nblk + 4])

    barrier = pltpu.get_barrier_semaphore()
    for off in range(1, DEV):
        pl.semaphore_signal(barrier, inc=1, device_id={"rows": lax.rem(me + off, DEV)})

    order = (me, at.sib, at.y0, at.x0, at.y1, at.x1, at.d0, at.d1)
    for j in order:
        load_tgt(j).start()
    load_feat.start()
    load_mass.start()
    load_q.start()
    load_fsrc.start()
    for j in range(nblk):
        load_plan(j).start()
    load_src.start()

    def cast_tgt(j):
        load_tgt(j).wait()
        tgt_ref[j, rows_of(me), :] = stage2_ref[j].astype(jnp.bfloat16)

    cast_tgt(me)
    cast_tgt(at.sib)
    pl.semaphore_wait(barrier, DEV - 1)

    def tcopy(owner, col, dest, kind):
        view = tgt_ref.at[col, rows_of(owner), :]
        return pltpu.make_async_remote_copy(
            src_ref=view, dst_ref=view, send_sem=tgt_send.at[kind, col],
            recv_sem=tgt_recv.at[owner, col], device_id={"rows": dest})

    def fcopy(owner, dest, kind):
        view = ftgt_ref.at[rows_of(owner), :]
        return pltpu.make_async_remote_copy(
            src_ref=view, dst_ref=view, send_sem=feat_send.at[kind], recv_sem=feat_recv.at[owner], device_id={"rows": dest})

    out_x = (at.me, at.sib, at.y0, at.y1, at.d0)
    out_y = (at.me, at.sib, at.x0, at.x1, at.d1)
    in_x = (at.x0, at.x1, at.d0, at.d1, at.y0)
    in_y = (at.y0, at.y1, at.d0, at.d1, at.x1)

    for k in range(2):
        tcopy(me, out_x[k], at.x0, 0).start()
        tcopy(me, out_y[k], at.y0, 1).start()
        tcopy(me, out_x[k], at.sib, 2).start()
    load_feat.wait()
    ftgt_ref[rows_of(me), :] = feat_ref[0].astype(jnp.bfloat16)
    fcopy(me, at.x0, 0).start()
    fcopy(me, at.y0, 1).start()
    fcopy(me, at.sib, 2).start()
    for j in order[2:]:
        cast_tgt(j)
        tcopy(me, j, at.sib, 2).start()
    for k in range(2, 5):
        tcopy(me, out_x[k], at.x0, 0).start()
        tcopy(me, out_y[k], at.y0, 1).start()

    load_mass.wait()
    load_q.wait()
    swap = pltpu.make_async_remote_copy(
        src_ref=mass_ref, dst_ref=mass2_ref, send_sem=swap_send.at[0], recv_sem=swap_recv.at[0], device_id={"rows": at.sib})
    swap.start()
    load_fsrc.wait()
    fsrc_ref[:BLK] = feat_ref[1].astype(jnp.bfloat16)
    swap_feat = pltpu.make_async_remote_copy(
        src_ref=fsrc_ref.at[:BLK], dst_ref=fsrc_ref.at[BLK:], send_sem=swap_send.at[1], recv_sem=swap_recv.at[1],
        device_id={"rows": at.sib})
    swap_feat.start()
    load_src.wait()
    src_ref[...] = cost_ref[:rows, :].astype(jnp.bfloat16)
    eye = lax.broadcasted_iota(jnp.int32, (LANES, LANES), 0) == lax.broadcasted_iota(jnp.int32, (LANES, LANES), 1)
    swap.wait()
    for r in range(rows // LANES):
        p_ref[r * LANES:(r + 1) * LANES, :] = spread(mass_ref[r:r + 1, :], eye)
        p_ref[rows + r * LANES:rows + (r + 1) * LANES, :] = spread(mass2_ref[r:r + 1, :], eye)

    def on_reach(f):
        @pl.when(at.core == 1)
        def _():
            f(2 * rows)

        @pl.when(at.core == 0)
        def _():
            f(rows)

    def a_copy(j):
        cols_at = pl.ds(pl.multiple_of(j * BLK, BLK), BLK)
        return pltpu.make_async_remote_copy(
            src_ref=a_ref.at[:rows, cols_at], dst_ref=a_ref.at[rows:, cols_at], send_sem=a_send.at[j],
            recv_sem=a_recv.at[j], device_id={"rows": at.sib})

    def add_column(j):
        @pl.when(at.core == 1)
        def _():
            a_copy(j).wait_recv()

        def add(reach, base_ref):
            lhs = a_ref[:reach, pl.ds(pl.multiple_of(j * BLK, BLK), BLK)]
            for col in range(nblk):
                where = slice(col * BLK, (col + 1) * BLK)
                prod = jnp.dot(lhs, tgt_ref[col, rows_of(j), :], preferred_element_type=jnp.float32)
                cost_ref[:reach, where] = base_ref[:reach, where] - (2.0 * (1.0 - ALPHA)) * prod

        def go(reach):
            @pl.when(j == 0)
            def _():
                add(reach, cross_ref)

            @pl.when(j > 0)
            def _():
                add(reach, cost_ref)

        on_reach(go)

    def column(j):
        prod = jnp.dot(src_ref[...], plan_ref[j], preferred_element_type=jnp.float32)
        a_ref[:rows, pl.ds(pl.multiple_of(j * BLK, BLK), BLK)] = prod.astype(jnp.bfloat16)

        @pl.when(at.core == 0)
        def _():
            a_copy(j).start()

        @pl.when(j > 0)
        def _():
            add_column(j - 1)

    def cast_plan(j):
        load_plan(j).wait()
        plan_ref[j, rows_of(me), :] = stage_ref[j].astype(jnp.bfloat16)

    begin, go_on = gather_plan(at, nblk, plan_ref, plan_send, plan_recv, cast_plan, column)

    def mirror(owner, col):
        tgt_ref[owner, rows_of(col), :] = tgt_ref[col, rows_of(owner), :].T

    base = me - at.core

    def mirror_row(owner):
        def body(t, carry):
            mirror(owner, lax.rem(base + 2 + t, DEV))
            return carry

        lax.fori_loop(0, DEV - 2, body, 0)

    def stream(k, s, other):
        core = lax.rem(at.core + other, 2)
        xb, yb, db = at.x0 - at.core, at.y0 - at.core, at.d0 - at.core
        near = xb + s * (yb - xb)
        far = yb + s * (xb - yb)
        which = k // 2
        chip = jnp.where(which == 0, near, jnp.where(which == 1, db, far))
        flip = jnp.where(which == 2, s, 0)
        return near + core, chip + lax.rem(core + k + flip, 2)

    def arrivals(k, carry):
        for s, fwd in ((0, 3), (1, 4)):
            owner, col = stream(k, s, 0)
            tcopy(owner, col, at.sib, 0).wait_recv()
            tcopy(owner, col, at.sib, fwd).start()
            if s == 0:
                @pl.when(k == 1)
                def _():
                    tcopy(at.x0, at.x1, at.y0, 6).start()
            else:
                @pl.when(k == 0)
                def _():
                    tcopy(at.y0, at.y0, at.x0, 6).start()

        @pl.when(k == 1)
        def _():
            fcopy(at.x0, at.sib, 0).wait_recv()
            fcopy(at.x0, at.sib, 3).start()
            fcopy(at.y0, at.sib, 0).wait_recv()
            fcopy(at.y0, at.sib, 4).start()

            @pl.when(at.core == 0)
            def _():
                fcopy(at.x0, at.y0, 6).start()

            @pl.when(at.core == 1)
            def _():
                fcopy(at.y0, at.x0, 6).start()

            mirror_row(me)

        @pl.when(k == 2)
        def _():
            begin()

            def from_sib(j, c):
                tcopy(at.sib, j, at.sib, 0).wait_recv()
                return c

            lax.fori_loop(0, nblk, from_sib, 0)
            mirror_row(at.sib)

        @pl.when(k >= 2)
        def _():
            def near(s, c):
                mirror(*stream(k, s, 0))
                return c

            lax.fori_loop(0, 2, near, 0)

        def near_other(s, c):
            owner, col = stream(k, s, 1)
            tcopy(owner, col, at.sib, 0).wait_recv()

            @pl.when(k >= 2)
            def _():
                mirror(owner, col)

            return c

        lax.fori_loop(0, 2, near_other, 0)
        return carry

    lax.fori_loop(0, 5, arrivals, 0)
    for col in (at.d0, at.d1):
        tcopy(at.d0, col, at.d0, 0).wait_recv()
        tcopy(at.d0, col, at.sib, 5).start()
    fcopy(at.d0, at.sib, 0).wait_recv()
    fcopy(at.d0, at.sib, 5).start()
    for owner in (at.sib, at.x1, at.y1, at.d1):
        fcopy(owner, at.sib, 0).wait_recv()
    swap_feat.wait()

    def crosses(reach):
        def cross(j, carry):
            prod = lax.dot_general(
                fsrc_ref[:reach, :], ftgt_ref[rows_of(j), :], (((1,), (1,)), ((), ())),
                preferred_element_type=jnp.float32)
            cross_ref[:reach, pl.ds(pl.multiple_of(j * BLK, BLK), BLK)] = (-2.0 * ALPHA) * prod
            return carry

        lax.fori_loop(0, nblk, cross, 0)

    on_reach(crosses)
    for col in (at.d1, at.d0):
        tcopy(at.d1, col, at.sib, 0).wait_recv()

    go_on()
    add_column(nblk - 1)

    for kind in range(7):
        fcopy(me, at.sib, kind).wait_send()
    for cx, cy in zip(out_x, out_y):
        tcopy(me, cx, at.x0, 0).wait_send()
        tcopy(me, cy, at.y0, 1).wait_send()
    for k in range(5):
        tcopy(at.x0, in_x[k], at.sib, 3).wait_send()
        tcopy(at.y0, in_y[k], at.sib, 4).wait_send()
    for col in (at.d0, at.d1):
        tcopy(at.d0, col, at.sib, 5).wait_send()
    tcopy(at.x0, at.x1, at.y0, 6).wait_send()
    tcopy(at.y0, at.y0, at.x0, 6).wait_send()

    def sib_done(j, carry):
        tcopy(me, j, at.sib, 2).wait_send()
        return carry

    lax.fori_loop(0, nblk, sib_done, 0)

    def a_done():
        @pl.when(at.core == 0)
        def _():
            def body(j, carry):
                a_copy(j).wait_send()
                return carry

            lax.fori_loop(0, nblk, body, 0)

    a_done()

    def early(src, j, slot, dest, kind):
        return pltpu.make_async_remote_copy(
            src_ref=src, dst_ref=early_ref.at[slot, j], send_sem=early_send.at[kind, j],
            recv_sem=early_recv.at[slot, j], device_id={"rows": dest})

    def own_part(j):
        return kern_ref.at[0, :, pl.ds(pl.multiple_of(j * BLK, BLK), BLK)]

    def early_round():
        def send(j):
            early(own_part(j), j, 0, at.x0, 0).start()
            early(own_part(j), j, 1, at.y0, 1).start()

        for j in range(AHEAD):
            send(j)

        def turn(j, carry):
            @pl.when(j + AHEAD < EARLY)
            def _():
                send(j + AHEAD)

            early(own_part(j), j, 0, at.x0, 0).wait_recv()

            @pl.when(lax.rem(j, 2) == 0)
            def _():
                early(early_ref.at[0, j], j, 2, at.y0, 2).start()

            early(own_part(j), j, 1, at.y0, 1).wait_recv()

            @pl.when(lax.rem(j, 2) == 1)
            def _():
                early(early_ref.at[1, j], j, 2, at.x0, 2).start()

            return carry

        lax.fori_loop(0, EARLY, turn, 0)

        def done(j, carry):
            early(own_part(j), j, 2, at.x0, 2).wait_recv()
            for kind in range(3):
                early(own_part(j), j, kind, at.x0, kind).wait_send()
            return carry

        lax.fori_loop(0, EARLY, done, 0)

    tiles = cols // LANES
    across = (at.sib, at.x1, at.y1, at.d1)

    def news(k):
        return pltpu.make_async_remote_copy(
            src_ref=msg_ref, dst_ref=news_ref.at[k], send_sem=msg_send.at[k], recv_sem=msg_recv.at[k],
            device_id={"rows": across[k]})

    def sweeps(first):
        reach = len(across) if first else 1
        build_kernel(cost_ref, kern_ref, eps, 0, rows, cols)

        @pl.when(at.core == 1)
        def _():
            build_kernel(cost_ref, kern_ref, eps, 1, rows, cols)
            sinkhorn(at, kern_ref, p_ref, q_ref, u_ref, v_ref, part_ref, gath_ref, sum_send, sum_recv)
            msg_ref[:tiles] = v_ref[...]
            msg_ref[tiles:] = jnp.zeros_like(msg_ref[tiles:])
            for r in range(rows // LANES):
                scale = u_ref[rows + r * LANES:rows + (r + 1) * LANES, :]
                msg_ref[tiles + r:tiles + r + 1] = jnp.sum(jnp.where(eye, scale, 0.0), axis=0, keepdims=True)
            for k in range(reach):
                news(k).start()
            for k in range(reach):
                news(k).wait_send()

        @pl.when(at.core == 0)
        def _():
            if first:
                early_round()
            for k in range(reach):
                news(k).wait_recv()
            v_ref[...] = news_ref[0, :tiles]
            for r in range(rows // LANES):
                u_ref[r * LANES:(r + 1) * LANES, :] = spread(news_ref[0, tiles + r:tiles + r + 1], eye)
                for k in range(1, reach):
                    other_ref[k - 1, r * LANES:(r + 1) * LANES, :] = spread(news_ref[k, tiles + r:tiles + r + 1], eye)

    def own_block(j):
        cols_at = pl.multiple_of(j * BLK, BLK)
        return plan_block(lambda h: kern_ref[0, :, pl.ds(cols_at + h * LANES, LANES)], u_ref[:rows, :], v_ref, j)

    sweeps(True)

    def next_plan(j):
        plan_ref[j, rows_of(me), :] = own_block(j).astype(jnp.bfloat16)

    def form(k, j):
        return plan_block(lambda h: early_ref[k, j, :, h * LANES:(h + 1) * LANES], other_ref[k], v_ref, j)

    begin, go_on = gather_plan(at, nblk, plan_ref, plan_send, plan_recv, next_plan, column, form)
    begin()
    go_on()
    add_column(nblk - 1)
    a_done()
    sweeps(False)

    for j in range(nblk):
        out_ref[:, j * BLK:(j + 1) * BLK] = own_block(j)


def fgw(src, tgt, plan, mass, q, fsrc, ftgt, eps):
    rows, cols = plan.shape
    tiles = cols // LANES
    nblk = cols // BLK
    vmem = pl.BlockSpec(memory_space=pltpu.VMEM)
    hbm = pl.BlockSpec(memory_space=pltpu.HBM)
    f32, bf16 = jnp.float32, jnp.bfloat16
    return pl.pallas_call(
        fgw_kernel,
        out_shape=jax.ShapeDtypeStruct((rows, cols), f32),
        in_specs=[pl.BlockSpec(memory_space=pltpu.SMEM)] + [hbm] * 7,
        out_specs=vmem,
        scratch_shapes=[
            pltpu.VMEM((nblk, BLK, BLK), f32),
            pltpu.VMEM((nblk, BLK, BLK), f32),
            pltpu.VMEM((2, BLK, BLK), f32),
            pltpu.VMEM((nblk, DEV * BLK, BLK), bf16),
            pltpu.VMEM((nblk, DEV * BLK, BLK), bf16),
            pltpu.VMEM((rows, cols), bf16),
            pltpu.VMEM((2 * BLK, BLK), bf16),
            pltpu.VMEM((DEV * BLK, BLK), bf16),
            pltpu.VMEM((2 * rows, cols), bf16),
            pltpu.VMEM((2 * rows, cols), f32),
            pltpu.VMEM((2 * rows, cols), f32),
            pltpu.VMEM((2, rows, cols), f32),
            pltpu.VMEM((3, EARLY, BLK, BLK), f32),
            pltpu.VMEM((2 * rows, LANES), f32),
            pltpu.VMEM((tiles, LANES), f32),
            pltpu.VMEM((2 * rows, LANES), f32),
            pltpu.VMEM((tiles, LANES), f32),
            pltpu.VMEM((3, rows, LANES), f32),
            pltpu.VMEM((2, tiles, LANES), f32),
            pltpu.VMEM((2, DEV // 2, tiles, LANES), f32),
            pltpu.VMEM((tiles + SUB, LANES), f32),
            pltpu.VMEM((4, tiles + SUB, LANES), f32),
            pltpu.VMEM((rows // LANES, LANES), f32),
            pltpu.VMEM((rows // LANES, LANES), f32),
            pltpu.SemaphoreType.DMA((2 * nblk + 5,)),
            pltpu.SemaphoreType.DMA((7, nblk)),
            pltpu.SemaphoreType.DMA((DEV, nblk)),
            pltpu.SemaphoreType.DMA((7, nblk)),
            pltpu.SemaphoreType.DMA((DEV, nblk)),
            pltpu.SemaphoreType.DMA((7,)),
            pltpu.SemaphoreType.DMA((DEV,)),
            pltpu.SemaphoreType.DMA((2, 3)),
            pltpu.SemaphoreType.DMA((2, DEV // 2)),
            pltpu.SemaphoreType.DMA((nblk,)),
            pltpu.SemaphoreType.DMA((nblk,)),
            pltpu.SemaphoreType.DMA((2,)),
            pltpu.SemaphoreType.DMA((2,)),
            pltpu.SemaphoreType.DMA((3, EARLY)),
            pltpu.SemaphoreType.DMA((3, EARLY)),
            pltpu.SemaphoreType.DMA((4,)),
            pltpu.SemaphoreType.DMA((4,)),
        ],
        compiler_params=pltpu.CompilerParams(collective_id=0, has_side_effects=True, vmem_limit_bytes=50 << 20),
        name="fgw",
    )(eps, *[pltpu.with_memory_space_constraint(x, pltpu.HBM) for x in (mass, q, src, tgt, plan, fsrc, ftgt)])


def solution(mesh):
    def local_fgw(cost_src, cost_tgt, plan_init, mass_src, mass_tgt, feat_src, feat_tgt, epsilon):
        return fgw(
            cost_src, cost_tgt, plan_init, mass_src.reshape(-1, LANES), mass_tgt.reshape(-1, LANES),
            feat_src, feat_tgt, epsilon.reshape(1))

    row_spec = P(('pairs', 'rows'), None)
    vec_spec = P(('pairs', 'rows'))
    in_specs = (row_spec, row_spec, row_spec, vec_spec, P('pairs'), row_spec, row_spec, P())
    return jax.shard_map(local_fgw, mesh=mesh, in_specs=in_specs, out_specs=row_spec, check_vma=False)
```

```python
import functools

import jax
import jax.numpy as jnp
from jax import lax
from jax.experimental import pallas as pl
from jax.experimental.pallas import tpu as pltpu
from jax.sharding import PartitionSpec as P

ALPHA = 0.5
OUTER_STEPS = 2
SWEEPS = 10
LANES = 128
SUB = 8
BLK = 256
DEV = 8
AHEAD = 2
LAG = 2
EARLY = 7
PIECES = 2


def tree_sum(vals):
    while len(vals) > 1:
        vals = [a + b for a, b in zip(vals[::2], vals[1::2])] + vals[len(vals) & ~1:]
    return vals[0]


def rows_of(owner):
    return pl.ds(pl.multiple_of(owner * BLK, BLK), BLK)


class Place:
    def __init__(self):
        self.me = lax.axis_index("rows")
        core = lax.rem(self.me, 2)
        x = lax.rem(self.me // 2, 2)
        y = self.me // 4
        self.core = core
        self.sib = self.me + 1 - 2 * core
        dx, dy = 2 - 4 * x, 4 - 8 * y
        self.x0, self.x1 = self.me + dx, self.sib + dx
        self.y0, self.y1 = self.me + dy, self.sib + dy
        self.d0, self.d1 = self.me + dx + dy, self.sib + dx + dy


def build_kernel(cost_ref, kern_ref, eps, half, rows, cols):
    tiles = cols // LANES
    inv_eps = 1.0 / jnp.full((SUB, LANES), eps, jnp.float32)

    def block(b, carry):
        row = pl.multiple_of(b * SUB, SUB)
        at_row = pl.ds(half * rows + row, SUB)
        vals = [cost_ref[at_row, t * LANES:(t + 1) * LANES] for t in range(tiles)]
        low = functools.reduce(jnp.minimum, vals)
        low = jnp.min(low, axis=1, keepdims=True)
        for t in range(tiles):
            kern_ref[half, pl.ds(row, SUB), t * LANES:(t + 1) * LANES] = jnp.exp((low - vals[t]) * inv_eps)
        return carry

    lax.fori_loop(0, rows // SUB, block, 0, unroll=8)


def spread(line, eye):
    wide = jnp.broadcast_to(line, (LANES, LANES))
    col = jnp.sum(jnp.where(eye, wide, 0.0), axis=1, keepdims=True)
    return jnp.broadcast_to(col, (LANES, LANES))


def sinkhorn(at, kern_ref, p_ref, q_ref, u_ref, v_ref, dots_ref, part_ref, gath_ref, send_sem, recv_sem):
    halves, rows, cols = kern_ref.shape
    tiles = cols // LANES
    span = tiles // PIECES
    blocks = [(h, b) for h in range(halves) for b in range(rows // SUB)]
    chip = at.me // 2
    peers = (at.x0, at.y0, at.d0)

    def copy(par, g, k, slot):
        return pltpu.make_async_remote_copy(
            src_ref=part_ref.at[par, g], dst_ref=gath_ref.at[par, g, slot],
            send_sem=send_sem.at[par, g, k], recv_sem=recv_sem.at[par, g, slot], device_id={"rows": peers[k]})

    def tile(h, b, t):
        return kern_ref[h, b * SUB:(b + 1) * SUB, t * LANES:(t + 1) * LANES]

    def at_row(h, b):
        return slice(h * rows + b * SUB, h * rows + (b + 1) * SUB)

    def dots_of(g):
        vrow = [jnp.broadcast_to(v_ref[t:t + 1, :], (SUB, LANES)) for t in range(g * span, (g + 1) * span)]
        for h, b in blocks:
            dots = tree_sum([tile(h, b, g * span + t) * vrow[t] for t in range(span)])
            if g > 0:
                dots = dots + dots_ref[at_row(h, b), :]
            if g < PIECES - 1:
                dots_ref[at_row(h, b), :] = dots
            else:
                u_ref[at_row(h, b), :] = p_ref[at_row(h, b), :] / jnp.sum(dots, axis=1, keepdims=True)

    def sums_of(par, g):
        acc = [None] * span
        for h, b in blocks:
            scale = u_ref[at_row(h, b), :]
            for t in range(span):
                term = tile(h, b, g * span + t) * scale
                acc[t] = term if acc[t] is None else acc[t] + term
        sums = jnp.concatenate([jnp.sum(a, axis=0, keepdims=True) for a in acc], axis=0)
        part_ref[par, g] = sums
        for k in (2, 0, 1):
            copy(par, g, k, chip).start()
        gath_ref[par, g, chip] = sums

    def scales_of(par, g):
        for k in range(3):
            copy(par, g, k, peers[k] // 2).wait_recv()
        total = gath_ref[par, g, 0]
        for d in range(1, DEV // 2):
            total = total + gath_ref[par, g, d]
        v_ref[g * span:(g + 1) * span, :] = q_ref[g * span:(g + 1) * span, :] / total

    def sent(par):
        for g in range(PIECES):
            for k in range(3):
                copy(par, g, k, chip).wait_send()

    v_ref[...] = jnp.ones_like(v_ref)

    def sweep(step, carry):
        par = lax.rem(step, 2)
        for g in range(PIECES):
            @pl.when(step > 0)
            def _():
                scales_of(1 - par, g)

            dots_of(g)

        @pl.when(step > 0)
        def _():
            sent(1 - par)

        for g in range(PIECES):
            sums_of(par, g)
        return carry

    lax.fori_loop(0, SWEEPS, sweep, 0)
    for g in range(PIECES):
        scales_of((SWEEPS - 1) % 2, g)
    sent((SWEEPS - 1) % 2)


def plan_block(kern, scale, v_ref, j):
    parts = []
    for h in range(BLK // LANES):
        vrow = v_ref[pl.ds(j * (BLK // LANES) + h, 1), :]
        parts.append(scale * kern(h) * vrow)
    return jnp.concatenate(parts, axis=1)


def gather_plan(at, chunks, plan_ref, send_sem, recv_sem, produce, column, form=None):
    def copy(owner, j, dest, kind):
        view = plan_ref.at[j, rows_of(owner), :]
        return pltpu.make_async_remote_copy(
            src_ref=view, dst_ref=view, send_sem=send_sem.at[kind, j],
            recv_sem=recv_sem.at[owner, j], device_id={"rows": dest})

    def over_links(j):
        return True if form is None else (at.core == 1) | (j >= EARLY)

    def when(cond):
        return (lambda f: f()) if cond is True else pl.when(cond)

    def send_own(j):
        @when(over_links(j))
        def _():
            copy(at.me, j, at.x0, 0).start()
            copy(at.me, j, at.y0, 1).start()

        copy(at.me, j, at.sib, 2).start()

    def begin():
        for j in range(AHEAD):
            produce(j)
            send_own(j)

    def turn(it, carry):
        @pl.when(it + AHEAD < chunks)
        def _():
            produce(it + AHEAD)
            send_own(it + AHEAD)

        @pl.when((it < chunks) & over_links(it))
        def _():
            copy(at.x0, it, at.x0, 0).wait_recv()
            copy(at.x0, it, at.sib, 3).start()

            @pl.when(lax.rem(it, 2) == 0)
            def _():
                copy(at.x0, it, at.y0, 6).start()

            copy(at.y0, it, at.y0, 0).wait_recv()
            copy(at.y0, it, at.sib, 4).start()

            @pl.when(lax.rem(it, 2) == 1)
            def _():
                copy(at.y0, it, at.x0, 6).start()

        if form is not None:
            @pl.when((it < chunks) & (at.core == 0) & (it < EARLY))
            def _():
                for k, owner in enumerate((at.x0, at.y0, at.d0)):
                    plan_ref[it, rows_of(owner), :] = form(k, it).astype(jnp.bfloat16)
                    copy(owner, it, at.sib, 3 + k).start()

        @pl.when((it >= LAG) & (it < LAG + chunks) & over_links(it - LAG))
        def _():
            copy(at.d0, it - LAG, at.d0, 0).wait_recv()
            copy(at.d0, it - LAG, at.sib, 5).start()

        @pl.when(it >= LAG + 1)
        def _():
            j = it - LAG - 1
            for owner in (at.sib, at.x1, at.y1, at.d1):
                copy(owner, j, at.sib, 0).wait_recv()
            column(j)

        return carry

    def drain(j, carry):
        for kind in (2, 3, 4, 5):
            copy(at.me, j, at.sib, kind).wait_send()

        @when(over_links(j))
        def _():
            for kind in (0, 1, 6):
                copy(at.me, j, at.sib, kind).wait_send()

        return carry

    def go_on():
        lax.fori_loop(0, chunks + LAG + 1, turn, 0)
        lax.fori_loop(0, chunks, drain, 0)

    return begin, go_on


def fgw_kernel(
    eps_ref, mass_hbm, q_hbm, src_hbm, tgt_hbm, plan_hbm, fsrc_hbm, ftgt_hbm, out_ref,
    stage_ref, stage2_ref, feat_ref, plan_ref, tgt_ref, src_ref, fsrc_ref, ftgt_ref, a_ref, cross_ref, cost_ref, kern_ref,
    early_ref, p_ref, q_ref, u_ref, v_ref, dots_ref, other_ref, part_ref, gath_ref, msg_ref, news_ref, mass_ref, mass2_ref,
    load_sem, plan_send, plan_recv, tgt_send, tgt_recv, feat_send, feat_recv, sum_send, sum_recv, a_send, a_recv,
    swap_send, swap_recv, early_send, early_recv, msg_send, msg_recv,
):
    at = Place()
    me = at.me
    _, rows, cols = kern_ref.shape
    nblk = cols // BLK
    eps = eps_ref[0]

    def load_plan(j):
        return pltpu.make_async_copy(plan_hbm.at[:, pl.ds(pl.multiple_of(j * BLK, BLK), BLK)], stage_ref.at[j], load_sem.at[j])

    def load_tgt(j):
        return pltpu.make_async_copy(tgt_hbm.at[:, pl.ds(pl.multiple_of(j * BLK, BLK), BLK)], stage2_ref.at[j], load_sem.at[nblk + j])

    load_feat = pltpu.make_async_copy(ftgt_hbm, feat_ref.at[0], load_sem.at[2 * nblk])
    load_fsrc = pltpu.make_async_copy(fsrc_hbm, feat_ref.at[1], load_sem.at[2 * nblk + 1])
    load_src = pltpu.make_async_copy(src_hbm, cost_ref.at[:rows], load_sem.at[2 * nblk + 2])
    load_mass = pltpu.make_async_copy(mass_hbm, mass_ref, load_sem.at[2 * nblk + 3])
    load_q = pltpu.make_async_copy(q_hbm, q_ref, load_sem.at[2 * nblk + 4])

    barrier = pltpu.get_barrier_semaphore()
    for off in range(1, DEV):
        pl.semaphore_signal(barrier, inc=1, device_id={"rows": lax.rem(me + off, DEV)})

    order = (me, at.sib, at.y0, at.x0, at.y1, at.x1, at.d0, at.d1)
    for j in order:
        load_tgt(j).start()
    load_feat.start()
    load_mass.start()
    load_q.start()
    load_fsrc.start()
    for j in range(nblk):
        load_plan(j).start()
    load_src.start()

    def cast_tgt(j):
        load_tgt(j).wait()
        tgt_ref[j, rows_of(me), :] = stage2_ref[j].astype(jnp.bfloat16)

    cast_tgt(me)
    cast_tgt(at.sib)
    pl.semaphore_wait(barrier, DEV - 1)

    def tcopy(owner, col, dest, kind):
        view = tgt_ref.at[col, rows_of(owner), :]
        return pltpu.make_async_remote_copy(
            src_ref=view, dst_ref=view, send_sem=tgt_send.at[kind, col],
            recv_sem=tgt_recv.at[owner, col], device_id={"rows": dest})

    def fcopy(owner, dest, kind):
        view = ftgt_ref.at[rows_of(owner), :]
        return pltpu.make_async_remote_copy(
            src_ref=view, dst_ref=view, send_sem=feat_send.at[kind], recv_sem=feat_recv.at[owner], device_id={"rows": dest})

    out_x = (at.me, at.sib, at.y0, at.y1, at.d0)
    out_y = (at.me, at.sib, at.x0, at.x1, at.d1)
    in_x = (at.x0, at.x1, at.d0, at.d1, at.y0)
    in_y = (at.y0, at.y1, at.d0, at.d1, at.x1)

    for k in range(2):
        tcopy(me, out_x[k], at.x0, 0).start()
        tcopy(me, out_y[k], at.y0, 1).start()
        tcopy(me, out_x[k], at.sib, 2).start()
    load_feat.wait()
    ftgt_ref[rows_of(me), :] = feat_ref[0].astype(jnp.bfloat16)
    fcopy(me, at.x0, 0).start()
    fcopy(me, at.y0, 1).start()
    fcopy(me, at.sib, 2).start()
    for j in order[2:]:
        cast_tgt(j)
        tcopy(me, j, at.sib, 2).start()
    for k in range(2, 5):
        tcopy(me, out_x[k], at.x0, 0).start()
        tcopy(me, out_y[k], at.y0, 1).start()

    load_mass.wait()
    load_q.wait()
    swap = pltpu.make_async_remote_copy(
        src_ref=mass_ref, dst_ref=mass2_ref, send_sem=swap_send.at[0], recv_sem=swap_recv.at[0], device_id={"rows": at.sib})
    swap.start()
    load_fsrc.wait()
    fsrc_ref[:BLK] = feat_ref[1].astype(jnp.bfloat16)
    swap_feat = pltpu.make_async_remote_copy(
        src_ref=fsrc_ref.at[:BLK], dst_ref=fsrc_ref.at[BLK:], send_sem=swap_send.at[1], recv_sem=swap_recv.at[1],
        device_id={"rows": at.sib})
    swap_feat.start()
    load_src.wait()
    src_ref[...] = cost_ref[:rows, :].astype(jnp.bfloat16)
    eye = lax.broadcasted_iota(jnp.int32, (LANES, LANES), 0) == lax.broadcasted_iota(jnp.int32, (LANES, LANES), 1)
    swap.wait()
    for r in range(rows // LANES):
        p_ref[r * LANES:(r + 1) * LANES, :] = spread(mass_ref[r:r + 1, :], eye)
        p_ref[rows + r * LANES:rows + (r + 1) * LANES, :] = spread(mass2_ref[r:r + 1, :], eye)

    def on_reach(f):
        @pl.when(at.core == 1)
        def _():
            f(2 * rows)

        @pl.when(at.core == 0)
        def _():
            f(rows)

    def a_copy(j):
        cols_at = pl.ds(pl.multiple_of(j * BLK, BLK), BLK)
        return pltpu.make_async_remote_copy(
            src_ref=a_ref.at[:rows, cols_at], dst_ref=a_ref.at[rows:, cols_at], send_sem=a_send.at[j],
            recv_sem=a_recv.at[j], device_id={"rows": at.sib})

    def add_column(j):
        @pl.when(at.core == 1)
        def _():
            a_copy(j).wait_recv()

        def add(reach, base_ref):
            lhs = a_ref[:reach, pl.ds(pl.multiple_of(j * BLK, BLK), BLK)]
            for col in range(nblk):
                where = slice(col * BLK, (col + 1) * BLK)
                prod = jnp.dot(lhs, tgt_ref[col, rows_of(j), :], preferred_element_type=jnp.float32)
                cost_ref[:reach, where] = base_ref[:reach, where] - (2.0 * (1.0 - ALPHA)) * prod

        def go(reach):
            @pl.when(j == 0)
            def _():
                add(reach, cross_ref)

            @pl.when(j > 0)
            def _():
                add(reach, cost_ref)

        on_reach(go)

    def column(j):
        prod = jnp.dot(src_ref[...], plan_ref[j], preferred_element_type=jnp.float32)
        a_ref[:rows, pl.ds(pl.multiple_of(j * BLK, BLK), BLK)] = prod.astype(jnp.bfloat16)

        @pl.when(at.core == 0)
        def _():
            a_copy(j).start()

        @pl.when(j > 0)
        def _():
            add_column(j - 1)

    def cast_plan(j):
        load_plan(j).wait()
        plan_ref[j, rows_of(me), :] = stage_ref[j].astype(jnp.bfloat16)

    begin, go_on = gather_plan(at, nblk, plan_ref, plan_send, plan_recv, cast_plan, column)

    def mirror(owner, col):
        tgt_ref[owner, rows_of(col), :] = tgt_ref[col, rows_of(owner), :].T

    base = me - at.core

    def mirror_row(owner):
        def body(t, carry):
            mirror(owner, lax.rem(base + 2 + t, DEV))
            return carry

        lax.fori_loop(0, DEV - 2, body, 0)

    def stream(k, s, other):
        core = lax.rem(at.core + other, 2)
        xb, yb, db = at.x0 - at.core, at.y0 - at.core, at.d0 - at.core
        near = xb + s * (yb - xb)
        far = yb + s * (xb - yb)
        which = k // 2
        chip = jnp.where(which == 0, near, jnp.where(which == 1, db, far))
        flip = jnp.where(which == 2, s, 0)
        return near + core, chip + lax.rem(core + k + flip, 2)

    def arrivals(k, carry):
        for s, fwd in ((0, 3), (1, 4)):
            owner, col = stream(k, s, 0)
            tcopy(owner, col, at.sib, 0).wait_recv()
            tcopy(owner, col, at.sib, fwd).start()
            if s == 0:
                @pl.when(k == 1)
                def _():
                    tcopy(at.x0, at.x1, at.y0, 6).start()
            else:
                @pl.when(k == 0)
                def _():
                    tcopy(at.y0, at.y0, at.x0, 6).start()

        @pl.when(k == 1)
        def _():
            fcopy(at.x0, at.sib, 0).wait_recv()
            fcopy(at.x0, at.sib, 3).start()
            fcopy(at.y0, at.sib, 0).wait_recv()
            fcopy(at.y0, at.sib, 4).start()

            @pl.when(at.core == 0)
            def _():
                fcopy(at.x0, at.y0, 6).start()

            @pl.when(at.core == 1)
            def _():
                fcopy(at.y0, at.x0, 6).start()

            mirror_row(me)

        @pl.when(k == 2)
        def _():
            begin()

            def from_sib(j, c):
                tcopy(at.sib, j, at.sib, 0).wait_recv()
                return c

            lax.fori_loop(0, nblk, from_sib, 0)
            mirror_row(at.sib)

        @pl.when(k >= 2)
        def _():
            def near(s, c):
                mirror(*stream(k, s, 0))
                return c

            lax.fori_loop(0, 2, near, 0)

        def near_other(s, c):
            owner, col = stream(k, s, 1)
            tcopy(owner, col, at.sib, 0).wait_recv()

            @pl.when(k >= 2)
            def _():
                mirror(owner, col)

            return c

        lax.fori_loop(0, 2, near_other, 0)
        return carry

    lax.fori_loop(0, 5, arrivals, 0)
    for col in (at.d0, at.d1):
        tcopy(at.d0, col, at.d0, 0).wait_recv()
        tcopy(at.d0, col, at.sib, 5).start()
    fcopy(at.d0, at.sib, 0).wait_recv()
    fcopy(at.d0, at.sib, 5).start()
    for owner in (at.sib, at.x1, at.y1, at.d1):
        fcopy(owner, at.sib, 0).wait_recv()
    swap_feat.wait()

    def crosses(reach):
        def cross(j, carry):
            prod = lax.dot_general(
                fsrc_ref[:reach, :], ftgt_ref[rows_of(j), :], (((1,), (1,)), ((), ())),
                preferred_element_type=jnp.float32)
            cross_ref[:reach, pl.ds(pl.multiple_of(j * BLK, BLK), BLK)] = (-2.0 * ALPHA) * prod
            return carry

        lax.fori_loop(0, nblk, cross, 0)

    on_reach(crosses)
    for col in (at.d1, at.d0):
        tcopy(at.d1, col, at.sib, 0).wait_recv()

    go_on()
    add_column(nblk - 1)

    for kind in range(7):
        fcopy(me, at.sib, kind).wait_send()
    for cx, cy in zip(out_x, out_y):
        tcopy(me, cx, at.x0, 0).wait_send()
        tcopy(me, cy, at.y0, 1).wait_send()
    for k in range(5):
        tcopy(at.x0, in_x[k], at.sib, 3).wait_send()
        tcopy(at.y0, in_y[k], at.sib, 4).wait_send()
    for col in (at.d0, at.d1):
        tcopy(at.d0, col, at.sib, 5).wait_send()
    tcopy(at.x0, at.x1, at.y0, 6).wait_send()
    tcopy(at.y0, at.y0, at.x0, 6).wait_send()

    def sib_done(j, carry):
        tcopy(me, j, at.sib, 2).wait_send()
        return carry

    lax.fori_loop(0, nblk, sib_done, 0)

    def a_done():
        @pl.when(at.core == 0)
        def _():
            def body(j, carry):
                a_copy(j).wait_send()
                return carry

            lax.fori_loop(0, nblk, body, 0)

    a_done()

    def early(src, j, slot, dest, kind):
        return pltpu.make_async_remote_copy(
            src_ref=src, dst_ref=early_ref.at[slot, j], send_sem=early_send.at[kind, j],
            recv_sem=early_recv.at[slot, j], device_id={"rows": dest})

    def early_half(i, dest):
        part = pl.ds(i * (BLK // 2), BLK // 2)
        return pltpu.make_async_remote_copy(
            src_ref=early_ref.at[i, EARLY - 1, part], dst_ref=early_ref.at[2, EARLY - 1, part],
            send_sem=early_send.at[2, EARLY - 1 + i], recv_sem=early_recv.at[2, EARLY - 1 + i], device_id={"rows": dest})

    def own_part(j):
        return kern_ref.at[0, :, pl.ds(pl.multiple_of(j * BLK, BLK), BLK)]

    def early_round():
        def send(j):
            early(own_part(j), j, 0, at.x0, 0).start()
            early(own_part(j), j, 1, at.y0, 1).start()

        for j in range(AHEAD):
            send(j)

        def turn(j, carry):
            @pl.when(j + AHEAD < EARLY)
            def _():
                send(j + AHEAD)

            early(own_part(j), j, 0, at.x0, 0).wait_recv()

            @pl.when((lax.rem(j, 2) == 0) & (j < EARLY - 1))
            def _():
                early(early_ref.at[0, j], j, 2, at.y0, 2).start()

            @pl.when(j == EARLY - 1)
            def _():
                early_half(0, at.y0).start()

            early(own_part(j), j, 1, at.y0, 1).wait_recv()

            @pl.when((lax.rem(j, 2) == 1) & (j < EARLY - 1))
            def _():
                early(early_ref.at[1, j], j, 2, at.x0, 2).start()

            @pl.when(j == EARLY - 1)
            def _():
                early_half(1, at.x0).start()

            return carry

        lax.fori_loop(0, EARLY, turn, 0)

        def done(j, carry):
            for kind in range(2):
                early(own_part(j), j, kind, at.x0, kind).wait_send()

            @pl.when(j < EARLY - 1)
            def _():
                early(own_part(j), j, 2, at.x0, 2).wait_recv()
                early(own_part(j), j, 2, at.x0, 2).wait_send()

            return carry

        lax.fori_loop(0, EARLY, done, 0)
        for i in range(2):
            early_half(i, at.x0).wait_recv()
            early_half(i, at.x0).wait_send()

    tiles = cols // LANES
    across = (at.sib, at.x1, at.y1, at.d1)

    def news(k):
        return pltpu.make_async_remote_copy(
            src_ref=msg_ref, dst_ref=news_ref.at[k], send_sem=msg_send.at[k], recv_sem=msg_recv.at[k],
            device_id={"rows": across[k]})

    def sweeps(first):
        reach = len(across) if first else 1
        build_kernel(cost_ref, kern_ref, eps, 0, rows, cols)

        @pl.when(at.core == 1)
        def _():
            build_kernel(cost_ref, kern_ref, eps, 1, rows, cols)
            sinkhorn(at, kern_ref, p_ref, q_ref, u_ref, v_ref, dots_ref, part_ref, gath_ref, sum_send, sum_recv)
            msg_ref[:tiles] = v_ref[...]
            msg_ref[tiles:] = jnp.zeros_like(msg_ref[tiles:])
            for r in range(rows // LANES):
                scale = u_ref[rows + r * LANES:rows + (r + 1) * LANES, :]
                msg_ref[tiles + r:tiles + r + 1] = jnp.sum(jnp.where(eye, scale, 0.0), axis=0, keepdims=True)
            for k in range(reach):
                news(k).start()
            for k in range(reach):
                news(k).wait_send()

        @pl.when(at.core == 0)
        def _():
            if first:
                early_round()
            for k in range(reach):
                news(k).wait_recv()
            v_ref[...] = news_ref[0, :tiles]
            for r in range(rows // LANES):
                u_ref[r * LANES:(r + 1) * LANES, :] = spread(news_ref[0, tiles + r:tiles + r + 1], eye)
                for k in range(1, reach):
                    other_ref[k - 1, r * LANES:(r + 1) * LANES, :] = spread(news_ref[k, tiles + r:tiles + r + 1], eye)

    def own_block(j):
        cols_at = pl.multiple_of(j * BLK, BLK)
        return plan_block(lambda h: kern_ref[0, :, pl.ds(cols_at + h * LANES, LANES)], u_ref[:rows, :], v_ref, j)

    sweeps(True)

    def next_plan(j):
        plan_ref[j, rows_of(me), :] = own_block(j).astype(jnp.bfloat16)

    def form(k, j):
        return plan_block(lambda h: early_ref[k, j, :, h * LANES:(h + 1) * LANES], other_ref[k], v_ref, j)

    begin, go_on = gather_plan(at, nblk, plan_ref, plan_send, plan_recv, next_plan, column, form)
    begin()
    go_on()
    add_column(nblk - 1)
    a_done()
    sweeps(False)

    for j in range(nblk):
        out_ref[:, j * BLK:(j + 1) * BLK] = own_block(j)


def fgw(src, tgt, plan, mass, q, fsrc, ftgt, eps):
    rows, cols = plan.shape
    tiles = cols // LANES
    nblk = cols // BLK
    vmem = pl.BlockSpec(memory_space=pltpu.VMEM)
    hbm = pl.BlockSpec(memory_space=pltpu.HBM)
    f32, bf16 = jnp.float32, jnp.bfloat16
    return pl.pallas_call(
        fgw_kernel,
        out_shape=jax.ShapeDtypeStruct((rows, cols), f32),
        in_specs=[pl.BlockSpec(memory_space=pltpu.SMEM)] + [hbm] * 7,
        out_specs=vmem,
        scratch_shapes=[
            pltpu.VMEM((nblk, BLK, BLK), f32),
            pltpu.VMEM((nblk, BLK, BLK), f32),
            pltpu.VMEM((2, BLK, BLK), f32),
            pltpu.VMEM((nblk, DEV * BLK, BLK), bf16),
            pltpu.VMEM((nblk, DEV * BLK, BLK), bf16),
            pltpu.VMEM((rows, cols), bf16),
            pltpu.VMEM((2 * BLK, BLK), bf16),
            pltpu.VMEM((DEV * BLK, BLK), bf16),
            pltpu.VMEM((2 * rows, cols), bf16),
            pltpu.VMEM((2 * rows, cols), f32),
            pltpu.VMEM((2 * rows, cols), f32),
            pltpu.VMEM((2, rows, cols), f32),
            pltpu.VMEM((3, EARLY, BLK, BLK), f32),
            pltpu.VMEM((2 * rows, LANES), f32),
            pltpu.VMEM((tiles, LANES), f32),
            pltpu.VMEM((2 * rows, LANES), f32),
            pltpu.VMEM((tiles, LANES), f32),
            pltpu.VMEM((2 * rows, LANES), f32),
            pltpu.VMEM((3, rows, LANES), f32),
            pltpu.VMEM((2, PIECES, tiles // PIECES, LANES), f32),
            pltpu.VMEM((2, PIECES, DEV // 2, tiles // PIECES, LANES), f32),
            pltpu.VMEM((tiles + SUB, LANES), f32),
            pltpu.VMEM((4, tiles + SUB, LANES), f32),
            pltpu.VMEM((rows // LANES, LANES), f32),
            pltpu.VMEM((rows // LANES, LANES), f32),
            pltpu.SemaphoreType.DMA((2 * nblk + 5,)),
            pltpu.SemaphoreType.DMA((7, nblk)),
            pltpu.SemaphoreType.DMA((DEV, nblk)),
            pltpu.SemaphoreType.DMA((7, nblk)),
            pltpu.SemaphoreType.DMA((DEV, nblk)),
            pltpu.SemaphoreType.DMA((7,)),
            pltpu.SemaphoreType.DMA((DEV,)),
            pltpu.SemaphoreType.DMA((2, PIECES, 3)),
            pltpu.SemaphoreType.DMA((2, PIECES, DEV // 2)),
            pltpu.SemaphoreType.DMA((nblk,)),
            pltpu.SemaphoreType.DMA((nblk,)),
            pltpu.SemaphoreType.DMA((2,)),
            pltpu.SemaphoreType.DMA((2,)),
            pltpu.SemaphoreType.DMA((3, EARLY + 1)),
            pltpu.SemaphoreType.DMA((3, EARLY + 1)),
            pltpu.SemaphoreType.DMA((4,)),
            pltpu.SemaphoreType.DMA((4,)),
        ],
        compiler_params=pltpu.CompilerParams(collective_id=0, has_side_effects=True, vmem_limit_bytes=50 << 20),
        name="fgw",
    )(eps, *[pltpu.with_memory_space_constraint(x, pltpu.HBM) for x in (mass, q, src, tgt, plan, fsrc, ftgt)])


def solution(mesh):
    def local_fgw(cost_src, cost_tgt, plan_init, mass_src, mass_tgt, feat_src, feat_tgt, epsilon):
        return fgw(
            cost_src, cost_tgt, plan_init, mass_src.reshape(-1, LANES), mass_tgt.reshape(-1, LANES),
            feat_src, feat_tgt, epsilon.reshape(1))

    row_spec = P(('pairs', 'rows'), None)
    vec_spec = P(('pairs', 'rows'))
    in_specs = (row_spec, row_spec, row_spec, vec_spec, P('pairs'), row_spec, row_spec, P())
    return jax.shard_map(local_fgw, mesh=mesh, in_specs=in_specs, out_specs=row_spec, check_vma=False)
```

```python
import functools

import jax
import jax.numpy as jnp
from jax import lax
from jax.experimental import pallas as pl
from jax.experimental.pallas import tpu as pltpu
from jax.sharding import PartitionSpec as P

ALPHA = 0.5
OUTER_STEPS = 2
SWEEPS = 10
LANES = 128
SUB = 8
BLK = 256
DEV = 8
AHEAD = 2
LAG = 2
EARLY = 7
PIECES = 2


def tree_sum(vals):
    while len(vals) > 1:
        vals = [a + b for a, b in zip(vals[::2], vals[1::2])] + vals[len(vals) & ~1:]
    return vals[0]


def rows_of(owner):
    return pl.ds(pl.multiple_of(owner * BLK, BLK), BLK)


class Place:
    def __init__(self):
        self.me = lax.axis_index("rows")
        core = lax.rem(self.me, 2)
        x = lax.rem(self.me // 2, 2)
        y = self.me // 4
        self.core = core
        self.sib = self.me + 1 - 2 * core
        dx, dy = 2 - 4 * x, 4 - 8 * y
        self.x0, self.x1 = self.me + dx, self.sib + dx
        self.y0, self.y1 = self.me + dy, self.sib + dy
        self.d0, self.d1 = self.me + dx + dy, self.sib + dx + dy


def build_kernel(cost_ref, kern_ref, eps, half, rows, cols):
    tiles = cols // LANES
    inv_eps = 1.0 / jnp.full((SUB, LANES), eps, jnp.float32)

    def block(b, carry):
        row = pl.multiple_of(b * SUB, SUB)
        at_row = pl.ds(half * rows + row, SUB)
        vals = [cost_ref[at_row, t * LANES:(t + 1) * LANES] for t in range(tiles)]
        low = functools.reduce(jnp.minimum, vals)
        low = jnp.min(low, axis=1, keepdims=True)
        for t in range(tiles):
            kern_ref[half, pl.ds(row, SUB), t * LANES:(t + 1) * LANES] = jnp.exp((low - vals[t]) * inv_eps)
        return carry

    lax.fori_loop(0, rows // SUB, block, 0, unroll=8)


def spread(line, eye):
    wide = jnp.broadcast_to(line, (LANES, LANES))
    col = jnp.sum(jnp.where(eye, wide, 0.0), axis=1, keepdims=True)
    return jnp.broadcast_to(col, (LANES, LANES))


def sinkhorn(at, kern_ref, p_ref, q_ref, u_ref, v_ref, dots_ref, part_ref, gath_ref, send_sem, recv_sem):
    halves, rows, cols = kern_ref.shape
    tiles = cols // LANES
    span = tiles // PIECES
    blocks = [(h, b) for h in range(halves) for b in range(rows // SUB)]
    chip = at.me // 2
    peers = (at.x0, at.y0, at.d0)

    def copy(par, g, k, slot):
        return pltpu.make_async_remote_copy(
            src_ref=part_ref.at[par, g], dst_ref=gath_ref.at[par, g, slot],
            send_sem=send_sem.at[par, g, k], recv_sem=recv_sem.at[par, g, slot], device_id={"rows": peers[k]})

    def tile(h, b, t):
        return kern_ref[h, b * SUB:(b + 1) * SUB, t * LANES:(t + 1) * LANES]

    def at_row(h, b):
        return slice(h * rows + b * SUB, h * rows + (b + 1) * SUB)

    def dots_of(g):
        vrow = [jnp.broadcast_to(v_ref[t:t + 1, :], (SUB, LANES)) for t in range(g * span, (g + 1) * span)]
        for h, b in blocks:
            dots = tree_sum([tile(h, b, g * span + t) * vrow[t] for t in range(span)])
            if g > 0:
                dots = dots + dots_ref[at_row(h, b), :]
            if g < PIECES - 1:
                dots_ref[at_row(h, b), :] = dots
            else:
                u_ref[at_row(h, b), :] = p_ref[at_row(h, b), :] / jnp.sum(dots, axis=1, keepdims=True)

    def sums_of(par, g):
        acc = [None] * span
        for h, b in blocks:
            scale = u_ref[at_row(h, b), :]
            for t in range(span):
                term = tile(h, b, g * span + t) * scale
                acc[t] = term if acc[t] is None else acc[t] + term
        sums = jnp.concatenate([jnp.sum(a, axis=0, keepdims=True) for a in acc], axis=0)
        part_ref[par, g] = sums
        for k in (2, 0, 1):
            copy(par, g, k, chip).start()
        gath_ref[par, g, chip] = sums

    def scales_of(par, g):
        for k in range(3):
            copy(par, g, k, peers[k] // 2).wait_recv()
        total = gath_ref[par, g, 0]
        for d in range(1, DEV // 2):
            total = total + gath_ref[par, g, d]
        v_ref[g * span:(g + 1) * span, :] = q_ref[g * span:(g + 1) * span, :] / total

    def sent(par):
        for g in range(PIECES):
            for k in range(3):
                copy(par, g, k, chip).wait_send()

    v_ref[...] = jnp.ones_like(v_ref)

    def sweep(step, carry):
        par = lax.rem(step, 2)
        for g in range(PIECES):
            @pl.when(step > 0)
            def _():
                scales_of(1 - par, g)

            dots_of(g)

        @pl.when(step > 0)
        def _():
            sent(1 - par)

        for g in range(PIECES):
            sums_of(par, g)
        return carry

    lax.fori_loop(0, SWEEPS, sweep, 0)
    for g in range(PIECES):
        scales_of((SWEEPS - 1) % 2, g)
    sent((SWEEPS - 1) % 2)


def plan_block(kern, scale, v_ref, j):
    parts = []
    for h in range(BLK // LANES):
        vrow = v_ref[pl.ds(j * (BLK // LANES) + h, 1), :]
        parts.append(scale * kern(h) * vrow)
    return jnp.concatenate(parts, axis=1)


def gather_plan(at, chunks, plan_ref, send_sem, recv_sem, produce, column, form=None):
    def copy(owner, j, dest, kind):
        view = plan_ref.at[j, rows_of(owner), :]
        return pltpu.make_async_remote_copy(
            src_ref=view, dst_ref=view, send_sem=send_sem.at[kind, j],
            recv_sem=recv_sem.at[owner, j], device_id={"rows": dest})

    def over_links(j):
        return True if form is None else (at.core == 1) | (j >= EARLY)

    def when(cond):
        return (lambda f: f()) if cond is True else pl.when(cond)

    def send_own(j):
        @when(over_links(j))
        def _():
            copy(at.me, j, at.x0, 0).start()
            copy(at.me, j, at.y0, 1).start()

        copy(at.me, j, at.sib, 2).start()

    def begin():
        for j in range(AHEAD):
            produce(j)
            send_own(j)

    def turn(it, carry):
        @pl.when(it + AHEAD < chunks)
        def _():
            produce(it + AHEAD)
            send_own(it + AHEAD)

        @pl.when((it < chunks) & over_links(it))
        def _():
            copy(at.x0, it, at.x0, 0).wait_recv()
            copy(at.x0, it, at.sib, 3).start()

            @pl.when(lax.rem(it, 2) == 0)
            def _():
                copy(at.x0, it, at.y0, 6).start()

            copy(at.y0, it, at.y0, 0).wait_recv()
            copy(at.y0, it, at.sib, 4).start()

            @pl.when(lax.rem(it, 2) == 1)
            def _():
                copy(at.y0, it, at.x0, 6).start()

        if form is not None:
            @pl.when((it < chunks) & (at.core == 0) & (it < EARLY))
            def _():
                for k, owner in enumerate((at.x0, at.y0, at.d0)):
                    plan_ref[it, rows_of(owner), :] = form(k, it).astype(jnp.bfloat16)
                    copy(owner, it, at.sib, 3 + k).start()

        @pl.when((it >= LAG) & (it < LAG + chunks) & over_links(it - LAG))
        def _():
            copy(at.d0, it - LAG, at.d0, 0).wait_recv()
            copy(at.d0, it - LAG, at.sib, 5).start()

        @pl.when(it >= LAG + 1)
        def _():
            j = it - LAG - 1
            for owner in (at.sib, at.x1, at.y1, at.d1):
                copy(owner, j, at.sib, 0).wait_recv()
            column(j)

        return carry

    def drain(j, carry):
        for kind in (2, 3, 4, 5):
            copy(at.me, j, at.sib, kind).wait_send()

        @when(over_links(j))
        def _():
            for kind in (0, 1, 6):
                copy(at.me, j, at.sib, kind).wait_send()

        return carry

    def go_on():
        lax.fori_loop(0, chunks + LAG + 1, turn, 0)
        lax.fori_loop(0, chunks, drain, 0)

    return begin, go_on


def fgw_kernel(
    eps_ref, mass_hbm, q_hbm, src_hbm, tgt_hbm, plan_hbm, fsrc_hbm, ftgt_hbm, out_ref,
    stage_ref, stage2_ref, feat_ref, plan_ref, tgt_ref, src_ref, fsrc_ref, ftgt_ref, a_ref, cross_ref, cost_ref, kern_ref,
    early_ref, p_ref, q_ref, u_ref, v_ref, dots_ref, other_ref, part_ref, gath_ref, msg_ref, news_ref, mass_ref, mass2_ref,
    load_sem, plan_send, plan_recv, tgt_send, tgt_recv, feat_send, feat_recv, sum_send, sum_recv, a_send, a_recv,
    swap_send, swap_recv, early_send, early_recv, msg_send, msg_recv,
):
    at = Place()
    me = at.me
    _, rows, cols = kern_ref.shape
    nblk = cols // BLK
    eps = eps_ref[0]

    def load_plan(j):
        return pltpu.make_async_copy(plan_hbm.at[:, pl.ds(pl.multiple_of(j * BLK, BLK), BLK)], stage_ref.at[j], load_sem.at[j])

    def load_tgt(j):
        return pltpu.make_async_copy(tgt_hbm.at[:, pl.ds(pl.multiple_of(j * BLK, BLK), BLK)], stage2_ref.at[j], load_sem.at[nblk + j])

    load_feat = pltpu.make_async_copy(ftgt_hbm, feat_ref.at[0], load_sem.at[2 * nblk])
    load_fsrc = pltpu.make_async_copy(fsrc_hbm, feat_ref.at[1], load_sem.at[2 * nblk + 1])
    load_src = pltpu.make_async_copy(src_hbm, cost_ref.at[:rows], load_sem.at[2 * nblk + 2])
    load_mass = pltpu.make_async_copy(mass_hbm, mass_ref, load_sem.at[2 * nblk + 3])
    load_q = pltpu.make_async_copy(q_hbm, q_ref, load_sem.at[2 * nblk + 4])

    barrier = pltpu.get_barrier_semaphore()
    for off in range(1, DEV):
        pl.semaphore_signal(barrier, inc=1, device_id={"rows": lax.rem(me + off, DEV)})

    order = (me, at.sib, at.y0, at.x0, at.y1, at.x1, at.d0, at.d1)
    for j in order:
        load_tgt(j).start()
    load_feat.start()
    load_mass.start()
    load_q.start()
    load_fsrc.start()
    for j in range(nblk):
        load_plan(j).start()
    load_src.start()

    def cast_tgt(j):
        load_tgt(j).wait()
        tgt_ref[j, rows_of(me), :] = stage2_ref[j].astype(jnp.bfloat16)

    cast_tgt(me)
    cast_tgt(at.sib)
    pl.semaphore_wait(barrier, DEV - 1)

    def tcopy(owner, col, dest, kind):
        view = tgt_ref.at[col, rows_of(owner), :]
        return pltpu.make_async_remote_copy(
            src_ref=view, dst_ref=view, send_sem=tgt_send.at[kind, col],
            recv_sem=tgt_recv.at[owner, col], device_id={"rows": dest})

    def fcopy(owner, dest, kind):
        view = ftgt_ref.at[rows_of(owner), :]
        return pltpu.make_async_remote_copy(
            src_ref=view, dst_ref=view, send_sem=feat_send.at[kind], recv_sem=feat_recv.at[owner], device_id={"rows": dest})

    out_x = (at.me, at.sib, at.y0, at.y1, at.d0)
    out_y = (at.me, at.sib, at.x0, at.x1, at.d1)
    in_x = (at.x0, at.x1, at.d0, at.d1, at.y0)
    in_y = (at.y0, at.y1, at.d0, at.d1, at.x1)

    def pair_send(wait):
        for core, dest in ((0, at.x0), (1, at.y0)):
            @pl.when(at.core == core)
            def _():
                copy = tcopy(me, at.sib, dest, core)
                copy.wait_send() if wait else copy.start()

    tcopy(me, me, at.x0, 0).start()
    tcopy(me, me, at.y0, 1).start()
    pair_send(False)
    for col in (me, at.sib):
        tcopy(me, col, at.sib, 2).start()
    load_feat.wait()
    ftgt_ref[rows_of(me), :] = feat_ref[0].astype(jnp.bfloat16)
    fcopy(me, at.x0, 0).start()
    fcopy(me, at.y0, 1).start()
    fcopy(me, at.sib, 2).start()
    for j in order[2:]:
        cast_tgt(j)
        tcopy(me, j, at.sib, 2).start()
    for k in range(2, 5):
        tcopy(me, out_x[k], at.x0, 0).start()
        tcopy(me, out_y[k], at.y0, 1).start()

    load_mass.wait()
    load_q.wait()
    swap = pltpu.make_async_remote_copy(
        src_ref=mass_ref, dst_ref=mass2_ref, send_sem=swap_send.at[0], recv_sem=swap_recv.at[0], device_id={"rows": at.sib})
    swap.start()
    load_fsrc.wait()
    fsrc_ref[:BLK] = feat_ref[1].astype(jnp.bfloat16)
    swap_feat = pltpu.make_async_remote_copy(
        src_ref=fsrc_ref.at[:BLK], dst_ref=fsrc_ref.at[BLK:], send_sem=swap_send.at[1], recv_sem=swap_recv.at[1],
        device_id={"rows": at.sib})
    swap_feat.start()
    load_src.wait()
    src_ref[...] = cost_ref[:rows, :].astype(jnp.bfloat16)
    eye = lax.broadcasted_iota(jnp.int32, (LANES, LANES), 0) == lax.broadcasted_iota(jnp.int32, (LANES, LANES), 1)
    swap.wait()
    for r in range(rows // LANES):
        p_ref[r * LANES:(r + 1) * LANES, :] = spread(mass_ref[r:r + 1, :], eye)
        p_ref[rows + r * LANES:rows + (r + 1) * LANES, :] = spread(mass2_ref[r:r + 1, :], eye)

    def on_reach(f):
        @pl.when(at.core == 1)
        def _():
            f(2 * rows)

        @pl.when(at.core == 0)
        def _():
            f(rows)

    def a_copy(j):
        cols_at = pl.ds(pl.multiple_of(j * BLK, BLK), BLK)
        return pltpu.make_async_remote_copy(
            src_ref=a_ref.at[:rows, cols_at], dst_ref=a_ref.at[rows:, cols_at], send_sem=a_send.at[j],
            recv_sem=a_recv.at[j], device_id={"rows": at.sib})

    def add_column(j):
        @pl.when(at.core == 1)
        def _():
            a_copy(j).wait_recv()

        def add(reach, base_ref):
            lhs = a_ref[:reach, pl.ds(pl.multiple_of(j * BLK, BLK), BLK)]
            for col in range(nblk):
                where = slice(col * BLK, (col + 1) * BLK)
                prod = jnp.dot(lhs, tgt_ref[col, rows_of(j), :], preferred_element_type=jnp.float32)
                cost_ref[:reach, where] = base_ref[:reach, where] - (2.0 * (1.0 - ALPHA)) * prod

        def go(reach):
            @pl.when(j == 0)
            def _():
                add(reach, cross_ref)

            @pl.when(j > 0)
            def _():
                add(reach, cost_ref)

        on_reach(go)

    def column(j):
        prod = jnp.dot(src_ref[...], plan_ref[j], preferred_element_type=jnp.float32)
        a_ref[:rows, pl.ds(pl.multiple_of(j * BLK, BLK), BLK)] = prod.astype(jnp.bfloat16)

        @pl.when(at.core == 0)
        def _():
            a_copy(j).start()

        @pl.when(j > 0)
        def _():
            add_column(j - 1)

    def cast_plan(j):
        load_plan(j).wait()
        plan_ref[j, rows_of(me), :] = stage_ref[j].astype(jnp.bfloat16)

    begin, go_on = gather_plan(at, nblk, plan_ref, plan_send, plan_recv, cast_plan, column)

    def mirror(owner, col):
        tgt_ref[owner, rows_of(col), :] = tgt_ref[col, rows_of(owner), :].T

    base = me - at.core

    def mirror_row(owner):
        def body(t, carry):
            mirror(owner, lax.rem(base + 2 + t, DEV))
            return carry

        lax.fori_loop(0, DEV - 2, body, 0)

    def stream(k, s, other):
        core = lax.rem(at.core + other, 2)
        xb, yb, db = at.x0 - at.core, at.y0 - at.core, at.d0 - at.core
        near = xb + s * (yb - xb)
        far = yb + s * (xb - yb)
        which = k // 2
        chip = jnp.where(which == 0, near, jnp.where(which == 1, db, far))
        flip = jnp.where(which == 2, s, 0)
        return near + core, chip + lax.rem(core + k + flip, 2)

    def arrivals(k, carry):
        for s, fwd in ((0, 3), (1, 4)):
            @pl.when((k != 1) | (at.core == s))
            def _():
                owner, col = stream(k, s, 0)
                tcopy(owner, col, at.sib, 0).wait_recv()
                tcopy(owner, col, at.sib, fwd).start()

        @pl.when(k == 0)
        def _():
            tcopy(at.y0, at.y0, at.x0, 6).start()

        @pl.when((k == 1) & (at.core == 0))
        def _():
            tcopy(at.x0, at.x1, at.y0, 6).start()

        @pl.when(k == 1)
        def _():
            fcopy(at.x0, at.sib, 0).wait_recv()
            fcopy(at.x0, at.sib, 3).start()
            fcopy(at.y0, at.sib, 0).wait_recv()
            fcopy(at.y0, at.sib, 4).start()

            @pl.when(at.core == 0)
            def _():
                fcopy(at.x0, at.y0, 6).start()

            @pl.when(at.core == 1)
            def _():
                fcopy(at.y0, at.x0, 6).start()

            mirror_row(me)

        @pl.when(k == 2)
        def _():
            begin()

            def from_sib(j, c):
                tcopy(at.sib, j, at.sib, 0).wait_recv()
                return c

            lax.fori_loop(0, nblk, from_sib, 0)
            mirror_row(at.sib)

        def near(t, c):
            other = t // 2
            owner, col = stream(k, lax.rem(t, 2), other)

            @pl.when((k != 1) | (lax.rem(at.core + other, 2) == lax.rem(t, 2)))
            def _():
                @pl.when(t >= 2)
                def _():
                    tcopy(owner, col, at.sib, 0).wait_recv()

                @pl.when(k >= 1)
                def _():
                    mirror(owner, col)

            return c

        lax.fori_loop(0, 4, near, 0)
        return carry

    lax.fori_loop(0, 5, arrivals, 0)
    tcopy(at.d0, at.d0, at.d0, 0).wait_recv()
    tcopy(at.d0, at.d0, at.sib, 5).start()

    @pl.when(at.core == 0)
    def _():
        tcopy(at.d0, at.d1, at.d0, 0).wait_recv()
        tcopy(at.d0, at.d1, at.sib, 5).start()

    fcopy(at.d0, at.sib, 0).wait_recv()
    fcopy(at.d0, at.sib, 5).start()
    for owner in (at.sib, at.x1, at.y1, at.d1):
        fcopy(owner, at.sib, 0).wait_recv()
    swap_feat.wait()

    def crosses(reach):
        def cross(j, carry):
            prod = lax.dot_general(
                fsrc_ref[:reach, :], ftgt_ref[rows_of(j), :], (((1,), (1,)), ((), ())),
                preferred_element_type=jnp.float32)
            cross_ref[:reach, pl.ds(pl.multiple_of(j * BLK, BLK), BLK)] = (-2.0 * ALPHA) * prod
            return carry

        lax.fori_loop(0, nblk, cross, 0)

    on_reach(crosses)
    tcopy(at.d1, at.d1, at.sib, 0).wait_recv()

    @pl.when(at.core == 1)
    def _():
        tcopy(at.d1, at.d0, at.sib, 0).wait_recv()

    mirror(at.d0 - at.core, at.d0 - at.core + 1)

    go_on()
    add_column(nblk - 1)

    for kind in range(7):
        fcopy(me, at.sib, kind).wait_send()
    pair_send(True)
    for k in (0, 2, 3, 4):
        tcopy(me, out_x[k], at.x0, 0).wait_send()
        tcopy(me, out_y[k], at.y0, 1).wait_send()
        tcopy(at.x0, in_x[k], at.sib, 3).wait_send()
        tcopy(at.y0, in_y[k], at.sib, 4).wait_send()
    tcopy(at.d0, at.d0, at.sib, 5).wait_send()
    tcopy(at.y0, at.y0, at.x0, 6).wait_send()

    @pl.when(at.core == 0)
    def _():
        tcopy(at.x0, at.x1, at.sib, 3).wait_send()
        tcopy(at.d0, at.d1, at.sib, 5).wait_send()
        tcopy(at.x0, at.x1, at.y0, 6).wait_send()

    @pl.when(at.core == 1)
    def _():
        tcopy(at.y0, at.y1, at.sib, 4).wait_send()

    def sib_done(j, carry):
        tcopy(me, j, at.sib, 2).wait_send()
        return carry

    lax.fori_loop(0, nblk, sib_done, 0)

    def a_done():
        @pl.when(at.core == 0)
        def _():
            def body(j, carry):
                a_copy(j).wait_send()
                return carry

            lax.fori_loop(0, nblk, body, 0)

    a_done()

    def early(src, j, slot, dest, kind):
        return pltpu.make_async_remote_copy(
            src_ref=src, dst_ref=early_ref.at[slot, j], send_sem=early_send.at[kind, j],
            recv_sem=early_recv.at[slot, j], device_id={"rows": dest})

    def early_half(i, dest):
        part = pl.ds(i * (BLK // 2), BLK // 2)
        return pltpu.make_async_remote_copy(
            src_ref=early_ref.at[i, EARLY - 1, part], dst_ref=early_ref.at[2, EARLY - 1, part],
            send_sem=early_send.at[2, EARLY - 1 + i], recv_sem=early_recv.at[2, EARLY - 1 + i], device_id={"rows": dest})

    def own_part(j):
        return kern_ref.at[0, :, pl.ds(pl.multiple_of(j * BLK, BLK), BLK)]

    def early_round():
        def send(j):
            early(own_part(j), j, 0, at.x0, 0).start()
            early(own_part(j), j, 1, at.y0, 1).start()

        for j in range(AHEAD):
            send(j)

        def turn(j, carry):
            @pl.when(j + AHEAD < EARLY)
            def _():
                send(j + AHEAD)

            early(own_part(j), j, 0, at.x0, 0).wait_recv()

            @pl.when((lax.rem(j, 2) == 0) & (j < EARLY - 1))
            def _():
                early(early_ref.at[0, j], j, 2, at.y0, 2).start()

            @pl.when(j == EARLY - 1)
            def _():
                early_half(0, at.y0).start()

            early(own_part(j), j, 1, at.y0, 1).wait_recv()

            @pl.when((lax.rem(j, 2) == 1) & (j < EARLY - 1))
            def _():
                early(early_ref.at[1, j], j, 2, at.x0, 2).start()

            @pl.when(j == EARLY - 1)
            def _():
                early_half(1, at.x0).start()

            return carry

        lax.fori_loop(0, EARLY, turn, 0)

        def done(j, carry):
            for kind in range(2):
                early(own_part(j), j, kind, at.x0, kind).wait_send()

            @pl.when(j < EARLY - 1)
            def _():
                early(own_part(j), j, 2, at.x0, 2).wait_recv()
                early(own_part(j), j, 2, at.x0, 2).wait_send()

            return carry

        lax.fori_loop(0, EARLY, done, 0)
        for i in range(2):
            early_half(i, at.x0).wait_recv()
            early_half(i, at.x0).wait_send()

    tiles = cols // LANES
    across = (at.sib, at.x1, at.y1, at.d1)

    def news(k):
        return pltpu.make_async_remote_copy(
            src_ref=msg_ref, dst_ref=news_ref.at[k], send_sem=msg_send.at[k], recv_sem=msg_recv.at[k],
            device_id={"rows": across[k]})

    def sweeps(first):
        reach = len(across) if first else 1
        build_kernel(cost_ref, kern_ref, eps, 0, rows, cols)

        @pl.when(at.core == 1)
        def _():
            build_kernel(cost_ref, kern_ref, eps, 1, rows, cols)
            sinkhorn(at, kern_ref, p_ref, q_ref, u_ref, v_ref, dots_ref, part_ref, gath_ref, sum_send, sum_recv)
            msg_ref[:tiles] = v_ref[...]
            msg_ref[tiles:] = jnp.zeros_like(msg_ref[tiles:])
            for r in range(rows // LANES):
                scale = u_ref[rows + r * LANES:rows + (r + 1) * LANES, :]
                msg_ref[tiles + r:tiles + r + 1] = jnp.sum(jnp.where(eye, scale, 0.0), axis=0, keepdims=True)
            for k in range(reach):
                news(k).start()
            for k in range(reach):
                news(k).wait_send()

        @pl.when(at.core == 0)
        def _():
            if first:
                early_round()
            for k in range(reach):
                news(k).wait_recv()
            v_ref[...] = news_ref[0, :tiles]
            for r in range(rows // LANES):
                u_ref[r * LANES:(r + 1) * LANES, :] = spread(news_ref[0, tiles + r:tiles + r + 1], eye)
                for k in range(1, reach):
                    other_ref[k - 1, r * LANES:(r + 1) * LANES, :] = spread(news_ref[k, tiles + r:tiles + r + 1], eye)

    def own_block(j):
        cols_at = pl.multiple_of(j * BLK, BLK)
        return plan_block(lambda h: kern_ref[0, :, pl.ds(cols_at + h * LANES, LANES)], u_ref[:rows, :], v_ref, j)

    sweeps(True)

    def next_plan(j):
        plan_ref[j, rows_of(me), :] = own_block(j).astype(jnp.bfloat16)

    def form(k, j):
        return plan_block(lambda h: early_ref[k, j, :, h * LANES:(h + 1) * LANES], other_ref[k], v_ref, j)

    begin, go_on = gather_plan(at, nblk, plan_ref, plan_send, plan_recv, next_plan, column, form)
    begin()
    go_on()
    add_column(nblk - 1)
    a_done()
    sweeps(False)

    for j in range(nblk):
        out_ref[:, j * BLK:(j + 1) * BLK] = own_block(j)


def fgw(src, tgt, plan, mass, q, fsrc, ftgt, eps):
    rows, cols = plan.shape
    tiles = cols // LANES
    nblk = cols // BLK
    vmem = pl.BlockSpec(memory_space=pltpu.VMEM)
    hbm = pl.BlockSpec(memory_space=pltpu.HBM)
    f32, bf16 = jnp.float32, jnp.bfloat16
    return pl.pallas_call(
        fgw_kernel,
        out_shape=jax.ShapeDtypeStruct((rows, cols), f32),
        in_specs=[pl.BlockSpec(memory_space=pltpu.SMEM)] + [hbm] * 7,
        out_specs=vmem,
        scratch_shapes=[
            pltpu.VMEM((nblk, BLK, BLK), f32),
            pltpu.VMEM((nblk, BLK, BLK), f32),
            pltpu.VMEM((2, BLK, BLK), f32),
            pltpu.VMEM((nblk, DEV * BLK, BLK), bf16),
            pltpu.VMEM((nblk, DEV * BLK, BLK), bf16),
            pltpu.VMEM((rows, cols), bf16),
            pltpu.VMEM((2 * BLK, BLK), bf16),
            pltpu.VMEM((DEV * BLK, BLK), bf16),
            pltpu.VMEM((2 * rows, cols), bf16),
            pltpu.VMEM((2 * rows, cols), f32),
            pltpu.VMEM((2 * rows, cols), f32),
            pltpu.VMEM((2, rows, cols), f32),
            pltpu.VMEM((3, EARLY, BLK, BLK), f32),
            pltpu.VMEM((2 * rows, LANES), f32),
            pltpu.VMEM((tiles, LANES), f32),
            pltpu.VMEM((2 * rows, LANES), f32),
            pltpu.VMEM((tiles, LANES), f32),
            pltpu.VMEM((2 * rows, LANES), f32),
            pltpu.VMEM((3, rows, LANES), f32),
            pltpu.VMEM((2, PIECES, tiles // PIECES, LANES), f32),
            pltpu.VMEM((2, PIECES, DEV // 2, tiles // PIECES, LANES), f32),
            pltpu.VMEM((tiles + SUB, LANES), f32),
            pltpu.VMEM((4, tiles + SUB, LANES), f32),
            pltpu.VMEM((rows // LANES, LANES), f32),
            pltpu.VMEM((rows // LANES, LANES), f32),
            pltpu.SemaphoreType.DMA((2 * nblk + 5,)),
            pltpu.SemaphoreType.DMA((7, nblk)),
            pltpu.SemaphoreType.DMA((DEV, nblk)),
            pltpu.SemaphoreType.DMA((7, nblk)),
            pltpu.SemaphoreType.DMA((DEV, nblk)),
            pltpu.SemaphoreType.DMA((7,)),
            pltpu.SemaphoreType.DMA((DEV,)),
            pltpu.SemaphoreType.DMA((2, PIECES, 3)),
            pltpu.SemaphoreType.DMA((2, PIECES, DEV // 2)),
            pltpu.SemaphoreType.DMA((nblk,)),
            pltpu.SemaphoreType.DMA((nblk,)),
            pltpu.SemaphoreType.DMA((2,)),
            pltpu.SemaphoreType.DMA((2,)),
            pltpu.SemaphoreType.DMA((3, EARLY + 1)),
            pltpu.SemaphoreType.DMA((3, EARLY + 1)),
            pltpu.SemaphoreType.DMA((4,)),
            pltpu.SemaphoreType.DMA((4,)),
        ],
        compiler_params=pltpu.CompilerParams(collective_id=0, has_side_effects=True, vmem_limit_bytes=50 << 20),
        name="fgw",
    )(eps, *[pltpu.with_memory_space_constraint(x, pltpu.HBM) for x in (mass, q, src, tgt, plan, fsrc, ftgt)])


def solution(mesh):
    def local_fgw(cost_src, cost_tgt, plan_init, mass_src, mass_tgt, feat_src, feat_tgt, epsilon):
        return fgw(
            cost_src, cost_tgt, plan_init, mass_src.reshape(-1, LANES), mass_tgt.reshape(-1, LANES),
            feat_src, feat_tgt, epsilon.reshape(1))

    row_spec = P(('pairs', 'rows'), None)
    vec_spec = P(('pairs', 'rows'))
    in_specs = (row_spec, row_spec, row_spec, vec_spec, P('pairs'), row_spec, row_spec, P())
    return jax.shard_map(local_fgw, mesh=mesh, in_specs=in_specs, out_specs=row_spec, check_vma=False)
```

```python
import functools

import jax
import jax.numpy as jnp
from jax import lax
from jax.experimental import pallas as pl
from jax.experimental.pallas import tpu as pltpu
from jax.sharding import PartitionSpec as P

ALPHA = 0.5
OUTER_STEPS = 2
SWEEPS = 10
LANES = 128
SUB = 8
BLK = 256
DEV = 8
AHEAD = 2
LAG = 2
EARLY = 7
PIECES = 2


def tree_sum(vals):
    while len(vals) > 1:
        vals = [a + b for a, b in zip(vals[::2], vals[1::2])] + vals[len(vals) & ~1:]
    return vals[0]


def rows_of(owner):
    return pl.ds(pl.multiple_of(owner * BLK, BLK), BLK)


class Place:
    def __init__(self):
        self.me = lax.axis_index("rows")
        core = lax.rem(self.me, 2)
        x = lax.rem(self.me // 2, 2)
        y = self.me // 4
        self.core = core
        self.sib = self.me + 1 - 2 * core
        dx, dy = 2 - 4 * x, 4 - 8 * y
        self.x0, self.x1 = self.me + dx, self.sib + dx
        self.y0, self.y1 = self.me + dy, self.sib + dy
        self.d0, self.d1 = self.me + dx + dy, self.sib + dx + dy


def build_kernel(cost_ref, kern_ref, eps, half, rows, cols):
    tiles = cols // LANES
    inv_eps = 1.0 / jnp.full((SUB, LANES), eps, jnp.float32)

    def block(b, carry):
        row = pl.multiple_of(b * SUB, SUB)
        at_row = pl.ds(half * rows + row, SUB)
        vals = [cost_ref[at_row, t * LANES:(t + 1) * LANES] for t in range(tiles)]
        low = functools.reduce(jnp.minimum, vals)
        low = jnp.min(low, axis=1, keepdims=True)
        for t in range(tiles):
            kern_ref[half, pl.ds(row, SUB), t * LANES:(t + 1) * LANES] = jnp.exp((low - vals[t]) * inv_eps)
        return carry

    lax.fori_loop(0, rows // SUB, block, 0, unroll=8)


def spread(line, eye):
    wide = jnp.broadcast_to(line, (LANES, LANES))
    col = jnp.sum(jnp.where(eye, wide, 0.0), axis=1, keepdims=True)
    return jnp.broadcast_to(col, (LANES, LANES))


def sinkhorn(at, kern_ref, p_ref, q_ref, u_ref, v_ref, dots_ref, part_ref, gath_ref, send_sem, recv_sem):
    halves, rows, cols = kern_ref.shape
    tiles = cols // LANES
    span = tiles // PIECES
    blocks = [(h, b) for h in range(halves) for b in range(rows // SUB)]
    chip = at.me // 2
    peers = (at.x0, at.y0, at.d0)

    def copy(par, g, k, slot):
        return pltpu.make_async_remote_copy(
            src_ref=part_ref.at[par, g], dst_ref=gath_ref.at[par, g, slot],
            send_sem=send_sem.at[par, g, k], recv_sem=recv_sem.at[par, g, slot], device_id={"rows": peers[k]})

    def tile(h, b, t):
        return kern_ref[h, b * SUB:(b + 1) * SUB, t * LANES:(t + 1) * LANES]

    def at_row(h, b):
        return slice(h * rows + b * SUB, h * rows + (b + 1) * SUB)

    def dots_of(g):
        vrow = [jnp.broadcast_to(v_ref[t:t + 1, :], (SUB, LANES)) for t in range(g * span, (g + 1) * span)]
        for h, b in blocks:
            dots = tree_sum([tile(h, b, g * span + t) * vrow[t] for t in range(span)])
            if g > 0:
                dots = dots + dots_ref[at_row(h, b), :]
            if g < PIECES - 1:
                dots_ref[at_row(h, b), :] = dots
            else:
                u_ref[at_row(h, b), :] = p_ref[at_row(h, b), :] / jnp.sum(dots, axis=1, keepdims=True)

    def sums_of(par, g):
        acc = [None] * span
        for h, b in blocks:
            scale = u_ref[at_row(h, b), :]
            for t in range(span):
                term = tile(h, b, g * span + t) * scale
                acc[t] = term if acc[t] is None else acc[t] + term
        sums = jnp.concatenate([jnp.sum(a, axis=0, keepdims=True) for a in acc], axis=0)
        part_ref[par, g] = sums
        for k in (2, 0, 1):
            copy(par, g, k, chip).start()
        gath_ref[par, g, chip] = sums

    def scales_of(par, g):
        for k in range(3):
            copy(par, g, k, peers[k] // 2).wait_recv()
        total = gath_ref[par, g, 0]
        for d in range(1, DEV // 2):
            total = total + gath_ref[par, g, d]
        v_ref[g * span:(g + 1) * span, :] = q_ref[g * span:(g + 1) * span, :] / total

    def sent(par):
        for g in range(PIECES):
            for k in range(3):
                copy(par, g, k, chip).wait_send()

    v_ref[...] = jnp.ones_like(v_ref)

    def sweep(step, carry):
        par = lax.rem(step, 2)
        for g in range(PIECES):
            @pl.when(step > 0)
            def _():
                scales_of(1 - par, g)

            dots_of(g)

        @pl.when(step > 0)
        def _():
            sent(1 - par)

        for g in range(PIECES):
            sums_of(par, g)
        return carry

    lax.fori_loop(0, SWEEPS, sweep, 0)
    for g in range(PIECES):
        scales_of((SWEEPS - 1) % 2, g)
    sent((SWEEPS - 1) % 2)


def plan_block(kern, scale, v_ref, j):
    parts = []
    for h in range(BLK // LANES):
        vrow = v_ref[pl.ds(j * (BLK // LANES) + h, 1), :]
        parts.append(scale * kern(h) * vrow)
    return jnp.concatenate(parts, axis=1)


def gather_plan(at, chunks, plan_ref, send_sem, recv_sem, produce, column, form=None):
    def copy(owner, j, dest, kind):
        view = plan_ref.at[j, rows_of(owner), :]
        return pltpu.make_async_remote_copy(
            src_ref=view, dst_ref=view, send_sem=send_sem.at[kind, j],
            recv_sem=recv_sem.at[owner, j], device_id={"rows": dest})

    def over_links(j):
        return True if form is None else (at.core == 1) | (j >= EARLY)

    def when(cond):
        return (lambda f: f()) if cond is True else pl.when(cond)

    def send_own(j):
        @when(over_links(j))
        def _():
            copy(at.me, j, at.x0, 0).start()
            copy(at.me, j, at.y0, 1).start()

        copy(at.me, j, at.sib, 2).start()

    def begin():
        for j in range(AHEAD):
            produce(j)
            send_own(j)

    def turn(it, carry):
        @pl.when(it + AHEAD < chunks)
        def _():
            produce(it + AHEAD)
            send_own(it + AHEAD)

        @pl.when((it < chunks) & over_links(it))
        def _():
            copy(at.x0, it, at.x0, 0).wait_recv()
            copy(at.x0, it, at.sib, 3).start()

            @pl.when(lax.rem(it, 2) == 0)
            def _():
                copy(at.x0, it, at.y0, 6).start()

            copy(at.y0, it, at.y0, 0).wait_recv()
            copy(at.y0, it, at.sib, 4).start()

            @pl.when(lax.rem(it, 2) == 1)
            def _():
                copy(at.y0, it, at.x0, 6).start()

        if form is not None:
            @pl.when((it < chunks) & (at.core == 0) & (it < EARLY))
            def _():
                for k, owner in enumerate((at.x0, at.y0, at.d0)):
                    plan_ref[it, rows_of(owner), :] = form(k, it).astype(jnp.bfloat16)
                    copy(owner, it, at.sib, 3 + k).start()

        @pl.when((it >= LAG) & (it < LAG + chunks) & over_links(it - LAG))
        def _():
            copy(at.d0, it - LAG, at.d0, 0).wait_recv()
            copy(at.d0, it - LAG, at.sib, 5).start()

        @pl.when(it >= LAG + 1)
        def _():
            j = it - LAG - 1
            for owner in (at.sib, at.x1, at.y1, at.d1):
                copy(owner, j, at.sib, 0).wait_recv()
            column(j)

        return carry

    def drain(j, carry):
        for kind in (2, 3, 4, 5):
            copy(at.me, j, at.sib, kind).wait_send()

        @when(over_links(j))
        def _():
            for kind in (0, 1, 6):
                copy(at.me, j, at.sib, kind).wait_send()

        return carry

    def go_on():
        lax.fori_loop(0, chunks + LAG + 1, turn, 0)
        lax.fori_loop(0, chunks, drain, 0)

    return begin, go_on


def fgw_kernel(
    eps_ref, mass_hbm, q_hbm, src_hbm, tgt_hbm, plan_hbm, fsrc_hbm, ftgt_hbm, out_ref,
    stage_ref, stage2_ref, feat_ref, plan_ref, tgt_ref, src_ref, fsrc_ref, ftgt_ref, a_ref, cross_ref, cost_ref, kern_ref,
    early_ref, p_ref, q_ref, u_ref, v_ref, dots_ref, other_ref, part_ref, gath_ref, msg_ref, news_ref, mass_ref, mass2_ref,
    load_sem, plan_send, plan_recv, tgt_send, tgt_recv, feat_send, feat_recv, sum_send, sum_recv,
    swap_send, swap_recv, early_send, early_recv, msg_send, msg_recv,
):
    at = Place()
    me = at.me
    _, rows, cols = kern_ref.shape
    nblk = cols // BLK
    eps = eps_ref[0]

    def load_plan(j):
        return pltpu.make_async_copy(plan_hbm.at[:, pl.ds(pl.multiple_of(j * BLK, BLK), BLK)], stage_ref.at[j], load_sem.at[j])

    def load_tgt(j):
        return pltpu.make_async_copy(tgt_hbm.at[:, pl.ds(pl.multiple_of(j * BLK, BLK), BLK)], stage2_ref.at[j], load_sem.at[nblk + j])

    load_feat = pltpu.make_async_copy(ftgt_hbm, feat_ref.at[0], load_sem.at[2 * nblk])
    load_fsrc = pltpu.make_async_copy(fsrc_hbm, feat_ref.at[1], load_sem.at[2 * nblk + 1])
    load_src = pltpu.make_async_copy(src_hbm, cost_ref.at[:rows], load_sem.at[2 * nblk + 2])
    load_mass = pltpu.make_async_copy(mass_hbm, mass_ref, load_sem.at[2 * nblk + 3])
    load_q = pltpu.make_async_copy(q_hbm, q_ref, load_sem.at[2 * nblk + 4])

    barrier = pltpu.get_barrier_semaphore()
    for off in range(1, DEV):
        pl.semaphore_signal(barrier, inc=1, device_id={"rows": lax.rem(me + off, DEV)})

    order = (me, at.sib, at.y0, at.x0, at.y1, at.x1, at.d0, at.d1)
    for j in order:
        load_tgt(j).start()
    load_feat.start()
    load_mass.start()
    load_q.start()
    load_fsrc.start()
    for j in range(nblk):
        load_plan(j).start()
    load_src.start()

    def cast_tgt(j):
        load_tgt(j).wait()
        tgt_ref[j, rows_of(me), :] = stage2_ref[j].astype(jnp.bfloat16)

    cast_tgt(me)
    cast_tgt(at.sib)
    pl.semaphore_wait(barrier, DEV - 1)

    def tcopy(owner, col, dest, kind):
        view = tgt_ref.at[col, rows_of(owner), :]
        return pltpu.make_async_remote_copy(
            src_ref=view, dst_ref=view, send_sem=tgt_send.at[kind, col],
            recv_sem=tgt_recv.at[owner, col], device_id={"rows": dest})

    def fcopy(owner, dest, kind):
        view = ftgt_ref.at[rows_of(owner), :]
        return pltpu.make_async_remote_copy(
            src_ref=view, dst_ref=view, send_sem=feat_send.at[kind], recv_sem=feat_recv.at[owner], device_id={"rows": dest})

    out_x = (at.me, at.sib, at.y0, at.y1, at.d0)
    out_y = (at.me, at.sib, at.x0, at.x1, at.d1)
    in_x = (at.x0, at.x1, at.d0, at.d1, at.y0)
    in_y = (at.y0, at.y1, at.d0, at.d1, at.x1)

    def pair_send(wait):
        for core, dest in ((0, at.x0), (1, at.y0)):
            @pl.when(at.core == core)
            def _():
                copy = tcopy(me, at.sib, dest, core)
                copy.wait_send() if wait else copy.start()

    tcopy(me, me, at.x0, 0).start()
    tcopy(me, me, at.y0, 1).start()
    pair_send(False)
    for col in (me, at.sib):
        tcopy(me, col, at.sib, 2).start()
    load_feat.wait()
    ftgt_ref[rows_of(me), :] = feat_ref[0].astype(jnp.bfloat16)
    fcopy(me, at.x0, 0).start()
    fcopy(me, at.y0, 1).start()
    fcopy(me, at.sib, 2).start()
    for j in order[2:]:
        cast_tgt(j)
        tcopy(me, j, at.sib, 2).start()
    for k in range(2, 5):
        tcopy(me, out_x[k], at.x0, 0).start()
        tcopy(me, out_y[k], at.y0, 1).start()

    load_mass.wait()
    load_q.wait()
    swap = pltpu.make_async_remote_copy(
        src_ref=mass_ref, dst_ref=mass2_ref, send_sem=swap_send.at[0], recv_sem=swap_recv.at[0], device_id={"rows": at.sib})
    swap.start()
    load_fsrc.wait()
    fsrc_ref[:BLK] = feat_ref[1].astype(jnp.bfloat16)
    swap_feat = pltpu.make_async_remote_copy(
        src_ref=fsrc_ref.at[:BLK], dst_ref=fsrc_ref.at[BLK:], send_sem=swap_send.at[1], recv_sem=swap_recv.at[1],
        device_id={"rows": at.sib})
    swap_feat.start()
    load_src.wait()
    src_ref[:rows] = cost_ref[:rows, :].astype(jnp.bfloat16)
    swap_src = pltpu.make_async_remote_copy(
        src_ref=src_ref.at[:rows], dst_ref=src_ref.at[rows:], send_sem=swap_send.at[2], recv_sem=swap_recv.at[2],
        device_id={"rows": at.sib})
    swap_src.start()
    eye = lax.broadcasted_iota(jnp.int32, (LANES, LANES), 0) == lax.broadcasted_iota(jnp.int32, (LANES, LANES), 1)
    swap.wait()
    for r in range(rows // LANES):
        p_ref[r * LANES:(r + 1) * LANES, :] = spread(mass_ref[r:r + 1, :], eye)
        p_ref[rows + r * LANES:rows + (r + 1) * LANES, :] = spread(mass2_ref[r:r + 1, :], eye)

    def on_reach(f):
        @pl.when(at.core == 1)
        def _():
            f(2 * rows)

        @pl.when(at.core == 0)
        def _():
            f(rows)

    def add_column(j):
        def add(reach, base_ref):
            lhs = a_ref[:reach, pl.ds(pl.multiple_of(j * BLK, BLK), BLK)]
            for col in range(nblk):
                where = slice(col * BLK, (col + 1) * BLK)
                prod = jnp.dot(lhs, tgt_ref[col, rows_of(j), :], preferred_element_type=jnp.float32)
                cost_ref[:reach, where] = base_ref[:reach, where] - (2.0 * (1.0 - ALPHA)) * prod

        def go(reach):
            @pl.when(j == 0)
            def _():
                add(reach, cross_ref)

            @pl.when(j > 0)
            def _():
                add(reach, cost_ref)

        on_reach(go)

    def column(j):
        def go(reach):
            prod = jnp.dot(src_ref[:reach, :], plan_ref[j], preferred_element_type=jnp.float32)
            a_ref[:reach, pl.ds(pl.multiple_of(j * BLK, BLK), BLK)] = prod.astype(jnp.bfloat16)

        on_reach(go)
        add_column(j)

    def cast_plan(j):
        load_plan(j).wait()
        plan_ref[j, rows_of(me), :] = stage_ref[j].astype(jnp.bfloat16)

    begin, go_on = gather_plan(at, nblk, plan_ref, plan_send, plan_recv, cast_plan, column)

    def mirror(owner, col):
        tgt_ref[owner, rows_of(col), :] = tgt_ref[col, rows_of(owner), :].T

    base = me - at.core

    def mirror_row(owner):
        def body(t, carry):
            mirror(owner, lax.rem(base + 2 + t, DEV))
            return carry

        lax.fori_loop(0, DEV - 2, body, 0)

    def stream(k, s, other):
        core = lax.rem(at.core + other, 2)
        xb, yb, db = at.x0 - at.core, at.y0 - at.core, at.d0 - at.core
        near = xb + s * (yb - xb)
        far = yb + s * (xb - yb)
        which = k // 2
        chip = jnp.where(which == 0, near, jnp.where(which == 1, db, far))
        flip = jnp.where(which == 2, s, 0)
        return near + core, chip + lax.rem(core + k + flip, 2)

    def arrivals(k, carry):
        for s, fwd in ((0, 3), (1, 4)):
            @pl.when((k != 1) | (at.core == s))
            def _():
                owner, col = stream(k, s, 0)
                tcopy(owner, col, at.sib, 0).wait_recv()
                tcopy(owner, col, at.sib, fwd).start()

        @pl.when(k == 0)
        def _():
            tcopy(at.y0, at.y0, at.x0, 6).start()

        @pl.when((k == 1) & (at.core == 0))
        def _():
            tcopy(at.x0, at.x1, at.y0, 6).start()

        @pl.when(k == 1)
        def _():
            fcopy(at.x0, at.sib, 0).wait_recv()
            fcopy(at.x0, at.sib, 3).start()
            fcopy(at.y0, at.sib, 0).wait_recv()
            fcopy(at.y0, at.sib, 4).start()

            @pl.when(at.core == 0)
            def _():
                fcopy(at.x0, at.y0, 6).start()

            @pl.when(at.core == 1)
            def _():
                fcopy(at.y0, at.x0, 6).start()

            mirror_row(me)

        @pl.when(k == 2)
        def _():
            begin()

            def from_sib(j, c):
                tcopy(at.sib, j, at.sib, 0).wait_recv()
                return c

            lax.fori_loop(0, nblk, from_sib, 0)
            mirror_row(at.sib)

        def near(t, c):
            other = t // 2
            owner, col = stream(k, lax.rem(t, 2), other)

            @pl.when((k != 1) | (lax.rem(at.core + other, 2) == lax.rem(t, 2)))
            def _():
                @pl.when(t >= 2)
                def _():
                    tcopy(owner, col, at.sib, 0).wait_recv()

                @pl.when(k >= 1)
                def _():
                    mirror(owner, col)

            return c

        lax.fori_loop(0, 4, near, 0)
        return carry

    lax.fori_loop(0, 5, arrivals, 0)
    tcopy(at.d0, at.d0, at.d0, 0).wait_recv()
    tcopy(at.d0, at.d0, at.sib, 5).start()

    @pl.when(at.core == 0)
    def _():
        tcopy(at.d0, at.d1, at.d0, 0).wait_recv()
        tcopy(at.d0, at.d1, at.sib, 5).start()

    fcopy(at.d0, at.sib, 0).wait_recv()
    fcopy(at.d0, at.sib, 5).start()
    for owner in (at.sib, at.x1, at.y1, at.d1):
        fcopy(owner, at.sib, 0).wait_recv()
    swap_feat.wait()
    swap_src.wait()

    def crosses(reach):
        def cross(j, carry):
            prod = lax.dot_general(
                fsrc_ref[:reach, :], ftgt_ref[rows_of(j), :], (((1,), (1,)), ((), ())),
                preferred_element_type=jnp.float32)
            cross_ref[:reach, pl.ds(pl.multiple_of(j * BLK, BLK), BLK)] = (-2.0 * ALPHA) * prod
            return carry

        lax.fori_loop(0, nblk, cross, 0)

    on_reach(crosses)
    tcopy(at.d1, at.d1, at.sib, 0).wait_recv()

    @pl.when(at.core == 1)
    def _():
        tcopy(at.d1, at.d0, at.sib, 0).wait_recv()

    mirror(at.d0 - at.core, at.d0 - at.core + 1)

    go_on()

    for kind in range(7):
        fcopy(me, at.sib, kind).wait_send()
    pair_send(True)
    for k in (0, 2, 3, 4):
        tcopy(me, out_x[k], at.x0, 0).wait_send()
        tcopy(me, out_y[k], at.y0, 1).wait_send()
        tcopy(at.x0, in_x[k], at.sib, 3).wait_send()
        tcopy(at.y0, in_y[k], at.sib, 4).wait_send()
    tcopy(at.d0, at.d0, at.sib, 5).wait_send()
    tcopy(at.y0, at.y0, at.x0, 6).wait_send()

    @pl.when(at.core == 0)
    def _():
        tcopy(at.x0, at.x1, at.sib, 3).wait_send()
        tcopy(at.d0, at.d1, at.sib, 5).wait_send()
        tcopy(at.x0, at.x1, at.y0, 6).wait_send()

    @pl.when(at.core == 1)
    def _():
        tcopy(at.y0, at.y1, at.sib, 4).wait_send()

    def sib_done(j, carry):
        tcopy(me, j, at.sib, 2).wait_send()
        return carry

    lax.fori_loop(0, nblk, sib_done, 0)

    def early(src, j, slot, dest, kind):
        return pltpu.make_async_remote_copy(
            src_ref=src, dst_ref=early_ref.at[slot, j], send_sem=early_send.at[kind, j],
            recv_sem=early_recv.at[slot, j], device_id={"rows": dest})

    def early_half(i, dest):
        part = pl.ds(i * (BLK // 2), BLK // 2)
        return pltpu.make_async_remote_copy(
            src_ref=early_ref.at[i, EARLY - 1, part], dst_ref=early_ref.at[2, EARLY - 1, part],
            send_sem=early_send.at[2, EARLY - 1 + i], recv_sem=early_recv.at[2, EARLY - 1 + i], device_id={"rows": dest})

    def own_part(j):
        return kern_ref.at[0, :, pl.ds(pl.multiple_of(j * BLK, BLK), BLK)]

    def early_round():
        def send(j):
            early(own_part(j), j, 0, at.x0, 0).start()
            early(own_part(j), j, 1, at.y0, 1).start()

        for j in range(AHEAD):
            send(j)

        def turn(j, carry):
            @pl.when(j + AHEAD < EARLY)
            def _():
                send(j + AHEAD)

            early(own_part(j), j, 0, at.x0, 0).wait_recv()

            @pl.when((lax.rem(j, 2) == 0) & (j < EARLY - 1))
            def _():
                early(early_ref.at[0, j], j, 2, at.y0, 2).start()

            @pl.when(j == EARLY - 1)
            def _():
                early_half(0, at.y0).start()

            early(own_part(j), j, 1, at.y0, 1).wait_recv()

            @pl.when((lax.rem(j, 2) == 1) & (j < EARLY - 1))
            def _():
                early(early_ref.at[1, j], j, 2, at.x0, 2).start()

            @pl.when(j == EARLY - 1)
            def _():
                early_half(1, at.x0).start()

            return carry

        lax.fori_loop(0, EARLY, turn, 0)

        def done(j, carry):
            for kind in range(2):
                early(own_part(j), j, kind, at.x0, kind).wait_send()

            @pl.when(j < EARLY - 1)
            def _():
                early(own_part(j), j, 2, at.x0, 2).wait_recv()
                early(own_part(j), j, 2, at.x0, 2).wait_send()

            return carry

        lax.fori_loop(0, EARLY, done, 0)
        for i in range(2):
            early_half(i, at.x0).wait_recv()
            early_half(i, at.x0).wait_send()

    tiles = cols // LANES
    across = (at.sib, at.x1, at.y1, at.d1)

    def news(k):
        return pltpu.make_async_remote_copy(
            src_ref=msg_ref, dst_ref=news_ref.at[k], send_sem=msg_send.at[k], recv_sem=msg_recv.at[k],
            device_id={"rows": across[k]})

    def sweeps(first):
        reach = len(across) if first else 1
        build_kernel(cost_ref, kern_ref, eps, 0, rows, cols)

        @pl.when(at.core == 1)
        def _():
            build_kernel(cost_ref, kern_ref, eps, 1, rows, cols)
            sinkhorn(at, kern_ref, p_ref, q_ref, u_ref, v_ref, dots_ref, part_ref, gath_ref, sum_send, sum_recv)
            msg_ref[:tiles] = v_ref[...]
            msg_ref[tiles:] = jnp.zeros_like(msg_ref[tiles:])
            for r in range(rows // LANES):
                scale = u_ref[rows + r * LANES:rows + (r + 1) * LANES, :]
                msg_ref[tiles + r:tiles + r + 1] = jnp.sum(jnp.where(eye, scale, 0.0), axis=0, keepdims=True)
            for k in range(reach):
                news(k).start()

        @pl.when(at.core == 0)
        def _():
            if first:
                early_round()
            for k in range(reach):
                news(k).wait_recv()
            v_ref[...] = news_ref[0, :tiles]
            for r in range(rows // LANES):
                u_ref[r * LANES:(r + 1) * LANES, :] = spread(news_ref[0, tiles + r:tiles + r + 1], eye)
                for k in range(1, reach):
                    other_ref[k - 1, r * LANES:(r + 1) * LANES, :] = spread(news_ref[k, tiles + r:tiles + r + 1], eye)

    def news_done(reach):
        @pl.when(at.core == 1)
        def _():
            for k in range(reach):
                news(k).wait_send()

    def own_block(j):
        cols_at = pl.multiple_of(j * BLK, BLK)
        return plan_block(lambda h: kern_ref[0, :, pl.ds(cols_at + h * LANES, LANES)], u_ref[:rows, :], v_ref, j)

    sweeps(True)

    def next_plan(j):
        plan_ref[j, rows_of(me), :] = own_block(j).astype(jnp.bfloat16)

    def form(k, j):
        return plan_block(lambda h: early_ref[k, j, :, h * LANES:(h + 1) * LANES], other_ref[k], v_ref, j)

    begin, go_on = gather_plan(at, nblk, plan_ref, plan_send, plan_recv, next_plan, column, form)
    begin()
    go_on()
    news_done(len(across))
    sweeps(False)

    for j in range(nblk):
        out_ref[:, j * BLK:(j + 1) * BLK] = own_block(j)
    news_done(1)


def fgw(src, tgt, plan, mass, q, fsrc, ftgt, eps):
    rows, cols = plan.shape
    tiles = cols // LANES
    nblk = cols // BLK
    vmem = pl.BlockSpec(memory_space=pltpu.VMEM)
    hbm = pl.BlockSpec(memory_space=pltpu.HBM)
    f32, bf16 = jnp.float32, jnp.bfloat16
    return pl.pallas_call(
        fgw_kernel,
        out_shape=jax.ShapeDtypeStruct((rows, cols), f32),
        in_specs=[pl.BlockSpec(memory_space=pltpu.SMEM)] + [hbm] * 7,
        out_specs=vmem,
        scratch_shapes=[
            pltpu.VMEM((nblk, BLK, BLK), f32),
            pltpu.VMEM((nblk, BLK, BLK), f32),
            pltpu.VMEM((2, BLK, BLK), f32),
            pltpu.VMEM((nblk, DEV * BLK, BLK), bf16),
            pltpu.VMEM((nblk, DEV * BLK, BLK), bf16),
            pltpu.VMEM((2 * rows, cols), bf16),
            pltpu.VMEM((2 * BLK, BLK), bf16),
            pltpu.VMEM((DEV * BLK, BLK), bf16),
            pltpu.VMEM((2 * rows, cols), bf16),
            pltpu.VMEM((2 * rows, cols), f32),
            pltpu.VMEM((2 * rows, cols), f32),
            pltpu.VMEM((2, rows, cols), f32),
            pltpu.VMEM((3, EARLY, BLK, BLK), f32),
            pltpu.VMEM((2 * rows, LANES), f32),
            pltpu.VMEM((tiles, LANES), f32),
            pltpu.VMEM((2 * rows, LANES), f32),
            pltpu.VMEM((tiles, LANES), f32),
            pltpu.VMEM((2 * rows, LANES), f32),
            pltpu.VMEM((3, rows, LANES), f32),
            pltpu.VMEM((2, PIECES, tiles // PIECES, LANES), f32),
            pltpu.VMEM((2, PIECES, DEV // 2, tiles // PIECES, LANES), f32),
            pltpu.VMEM((tiles + SUB, LANES), f32),
            pltpu.VMEM((4, tiles + SUB, LANES), f32),
            pltpu.VMEM((rows // LANES, LANES), f32),
            pltpu.VMEM((rows // LANES, LANES), f32),
            pltpu.SemaphoreType.DMA((2 * nblk + 5,)),
            pltpu.SemaphoreType.DMA((7, nblk)),
            pltpu.SemaphoreType.DMA((DEV, nblk)),
            pltpu.SemaphoreType.DMA((7, nblk)),
            pltpu.SemaphoreType.DMA((DEV, nblk)),
            pltpu.SemaphoreType.DMA((7,)),
            pltpu.SemaphoreType.DMA((DEV,)),
            pltpu.SemaphoreType.DMA((2, PIECES, 3)),
            pltpu.SemaphoreType.DMA((2, PIECES, DEV // 2)),
            pltpu.SemaphoreType.DMA((3,)),
            pltpu.SemaphoreType.DMA((3,)),
            pltpu.SemaphoreType.DMA((3, EARLY + 1)),
            pltpu.SemaphoreType.DMA((3, EARLY + 1)),
            pltpu.SemaphoreType.DMA((4,)),
            pltpu.SemaphoreType.DMA((4,)),
        ],
        compiler_params=pltpu.CompilerParams(collective_id=0, has_side_effects=True, vmem_limit_bytes=50 << 20),
        name="fgw",
    )(eps, *[pltpu.with_memory_space_constraint(x, pltpu.HBM) for x in (mass, q, src, tgt, plan, fsrc, ftgt)])


def solution(mesh):
    def local_fgw(cost_src, cost_tgt, plan_init, mass_src, mass_tgt, feat_src, feat_tgt, epsilon):
        return fgw(
            cost_src, cost_tgt, plan_init, mass_src.reshape(-1, LANES), mass_tgt.reshape(-1, LANES),
            feat_src, feat_tgt, epsilon.reshape(1))

    row_spec = P(('pairs', 'rows'), None)
    vec_spec = P(('pairs', 'rows'))
    in_specs = (row_spec, row_spec, row_spec, vec_spec, P('pairs'), row_spec, row_spec, P())
    return jax.shard_map(local_fgw, mesh=mesh, in_specs=in_specs, out_specs=row_spec, check_vma=False)
```

```python
import functools

import jax
import jax.numpy as jnp
from jax import lax
from jax.experimental import pallas as pl
from jax.experimental.pallas import tpu as pltpu
from jax.sharding import PartitionSpec as P

ALPHA = 0.5
OUTER_STEPS = 2
SWEEPS = 10
LANES = 128
SUB = 8
BLK = 256
DEV = 8
AHEAD = 2
LAG = 2
EARLY = 7
PIECES = 2


def tree_sum(vals):
    while len(vals) > 1:
        vals = [a + b for a, b in zip(vals[::2], vals[1::2])] + vals[len(vals) & ~1:]
    return vals[0]


def rows_of(owner):
    return pl.ds(pl.multiple_of(owner * BLK, BLK), BLK)


class Place:
    def __init__(self):
        self.me = lax.axis_index("rows")
        core = lax.rem(self.me, 2)
        x = lax.rem(self.me // 2, 2)
        y = self.me // 4
        self.core = core
        self.sib = self.me + 1 - 2 * core
        dx, dy = 2 - 4 * x, 4 - 8 * y
        self.x0, self.x1 = self.me + dx, self.sib + dx
        self.y0, self.y1 = self.me + dy, self.sib + dy
        self.d0, self.d1 = self.me + dx + dy, self.sib + dx + dy


def build_kernel(cost_ref, kern_ref, eps, half, rows, cols):
    tiles = cols // LANES
    inv_eps = 1.0 / jnp.full((SUB, LANES), eps, jnp.float32)

    def block(b, carry):
        row = pl.multiple_of(b * SUB, SUB)
        at_row = pl.ds(half * rows + row, SUB)
        vals = [cost_ref[at_row, t * LANES:(t + 1) * LANES] for t in range(tiles)]
        low = functools.reduce(jnp.minimum, vals)
        low = jnp.min(low, axis=1, keepdims=True)
        for t in range(tiles):
            kern_ref[half, pl.ds(row, SUB), t * LANES:(t + 1) * LANES] = jnp.exp((low - vals[t]) * inv_eps)
        return carry

    lax.fori_loop(0, rows // SUB, block, 0, unroll=16)


def spread(line, eye):
    wide = jnp.broadcast_to(line, (LANES, LANES))
    col = jnp.sum(jnp.where(eye, wide, 0.0), axis=1, keepdims=True)
    return jnp.broadcast_to(col, (LANES, LANES))


def sinkhorn(at, kern_ref, p_ref, q_ref, u_ref, v_ref, dots_ref, part_ref, gath_ref, send_sem, recv_sem):
    halves, rows, cols = kern_ref.shape
    tiles = cols // LANES
    span = tiles // PIECES
    blocks = [(h, b) for h in range(halves) for b in range(rows // SUB)]
    chip = at.me // 2
    peers = (at.x0, at.y0, at.d0)

    def copy(par, g, k, slot):
        return pltpu.make_async_remote_copy(
            src_ref=part_ref.at[par, g], dst_ref=gath_ref.at[par, g, slot],
            send_sem=send_sem.at[par, g, k], recv_sem=recv_sem.at[par, g, slot], device_id={"rows": peers[k]})

    def tile(h, b, t):
        return kern_ref[h, b * SUB:(b + 1) * SUB, t * LANES:(t + 1) * LANES]

    def at_row(h, b):
        return slice(h * rows + b * SUB, h * rows + (b + 1) * SUB)

    def dots_of(g):
        vrow = [jnp.broadcast_to(v_ref[t:t + 1, :], (SUB, LANES)) for t in range(g * span, (g + 1) * span)]
        for h, b in blocks:
            dots = tree_sum([tile(h, b, g * span + t) * vrow[t] for t in range(span)])
            if g > 0:
                dots = dots + dots_ref[at_row(h, b), :]
            if g < PIECES - 1:
                dots_ref[at_row(h, b), :] = dots
            else:
                u_ref[at_row(h, b), :] = p_ref[at_row(h, b), :] / jnp.sum(dots, axis=1, keepdims=True)

    def sums_of(par, g):
        acc = [None] * span
        for h, b in blocks:
            scale = u_ref[at_row(h, b), :]
            for t in range(span):
                term = tile(h, b, g * span + t) * scale
                acc[t] = term if acc[t] is None else acc[t] + term
        sums = jnp.concatenate([jnp.sum(a, axis=0, keepdims=True) for a in acc], axis=0)
        part_ref[par, g] = sums
        for k in (2, 0, 1):
            copy(par, g, k, chip).start()
        gath_ref[par, g, chip] = sums

    def scales_of(par, g):
        for k in range(3):
            copy(par, g, k, peers[k] // 2).wait_recv()
        total = gath_ref[par, g, 0]
        for d in range(1, DEV // 2):
            total = total + gath_ref[par, g, d]
        v_ref[g * span:(g + 1) * span, :] = q_ref[g * span:(g + 1) * span, :] / total

    def sent(par):
        for g in range(PIECES):
            for k in range(3):
                copy(par, g, k, chip).wait_send()

    v_ref[...] = jnp.ones_like(v_ref)

    def sweep(step, carry):
        par = lax.rem(step, 2)
        for g in range(PIECES):
            @pl.when(step > 0)
            def _():
                scales_of(1 - par, g)

            dots_of(g)

        @pl.when(step > 0)
        def _():
            sent(1 - par)

        for g in range(PIECES):
            sums_of(par, g)
        return carry

    lax.fori_loop(0, SWEEPS, sweep, 0)
    for g in range(PIECES):
        scales_of((SWEEPS - 1) % 2, g)
    sent((SWEEPS - 1) % 2)


def plan_block(kern, scale, v_ref, j):
    parts = []
    for h in range(BLK // LANES):
        vrow = v_ref[pl.ds(j * (BLK // LANES) + h, 1), :]
        parts.append(scale * kern(h) * vrow)
    return jnp.concatenate(parts, axis=1)


def gather_plan(at, chunks, plan_ref, send_sem, recv_sem, produce, column, form=None):
    def copy(owner, j, dest, kind):
        view = plan_ref.at[j, rows_of(owner), :]
        return pltpu.make_async_remote_copy(
            src_ref=view, dst_ref=view, send_sem=send_sem.at[kind, j],
            recv_sem=recv_sem.at[owner, j], device_id={"rows": dest})

    def over_links(j):
        return True if form is None else (at.core == 1) | (j >= EARLY)

    def when(cond):
        return (lambda f: f()) if cond is True else pl.when(cond)

    def send_own(j):
        @when(over_links(j))
        def _():
            copy(at.me, j, at.x0, 0).start()
            copy(at.me, j, at.y0, 1).start()

        copy(at.me, j, at.sib, 2).start()

    def begin():
        for j in range(AHEAD):
            produce(j)
            send_own(j)

    def turn(it, carry):
        @pl.when(it + AHEAD < chunks)
        def _():
            produce(it + AHEAD)
            send_own(it + AHEAD)

        @pl.when((it < chunks) & over_links(it))
        def _():
            copy(at.x0, it, at.x0, 0).wait_recv()
            copy(at.x0, it, at.sib, 3).start()

            @pl.when(lax.rem(it, 2) == 0)
            def _():
                copy(at.x0, it, at.y0, 6).start()

            copy(at.y0, it, at.y0, 0).wait_recv()
            copy(at.y0, it, at.sib, 4).start()

            @pl.when(lax.rem(it, 2) == 1)
            def _():
                copy(at.y0, it, at.x0, 6).start()

        if form is not None:
            @pl.when((it < chunks) & (at.core == 0) & (it < EARLY))
            def _():
                for k, owner in enumerate((at.x0, at.y0, at.d0)):
                    plan_ref[it, rows_of(owner), :] = form(k, it).astype(jnp.bfloat16)
                    copy(owner, it, at.sib, 3 + k).start()

        @pl.when((it >= LAG) & (it < LAG + chunks) & over_links(it - LAG))
        def _():
            copy(at.d0, it - LAG, at.d0, 0).wait_recv()
            copy(at.d0, it - LAG, at.sib, 5).start()

        @pl.when(it >= LAG + 1)
        def _():
            j = it - LAG - 1
            for owner in (at.sib, at.x1, at.y1, at.d1):
                copy(owner, j, at.sib, 0).wait_recv()
            column(j)

        return carry

    def drain(j, carry):
        for kind in (2, 3, 4, 5):
            copy(at.me, j, at.sib, kind).wait_send()

        @when(over_links(j))
        def _():
            for kind in (0, 1, 6):
                copy(at.me, j, at.sib, kind).wait_send()

        return carry

    def go_on():
        lax.fori_loop(0, chunks + LAG + 1, turn, 0)
        lax.fori_loop(0, chunks, drain, 0)

    return begin, go_on


def fgw_kernel(
    eps_ref, mass_hbm, q_hbm, src_hbm, tgt_hbm, plan_hbm, fsrc_hbm, ftgt_hbm, out_ref,
    stage_ref, stage2_ref, feat_ref, plan_ref, tgt_ref, src_ref, fsrc_ref, ftgt_ref, a_ref, cross_ref, cost_ref, kern_ref,
    early_ref, p_ref, q_ref, u_ref, v_ref, dots_ref, other_ref, part_ref, gath_ref, msg_ref, news_ref, mass_ref, mass2_ref,
    load_sem, plan_send, plan_recv, tgt_send, tgt_recv, feat_send, feat_recv, sum_send, sum_recv,
    swap_send, swap_recv, early_send, early_recv, msg_send, msg_recv,
):
    at = Place()
    me = at.me
    _, rows, cols = kern_ref.shape
    nblk = cols // BLK
    eps = eps_ref[0]

    def load_plan(j):
        return pltpu.make_async_copy(plan_hbm.at[:, pl.ds(pl.multiple_of(j * BLK, BLK), BLK)], stage_ref.at[j], load_sem.at[j])

    def load_tgt(j):
        return pltpu.make_async_copy(tgt_hbm.at[:, pl.ds(pl.multiple_of(j * BLK, BLK), BLK)], stage2_ref.at[j], load_sem.at[nblk + j])

    load_feat = pltpu.make_async_copy(ftgt_hbm, feat_ref.at[0], load_sem.at[2 * nblk])
    load_fsrc = pltpu.make_async_copy(fsrc_hbm, feat_ref.at[1], load_sem.at[2 * nblk + 1])
    load_src = pltpu.make_async_copy(src_hbm, cost_ref.at[:rows], load_sem.at[2 * nblk + 2])
    load_mass = pltpu.make_async_copy(mass_hbm, mass_ref, load_sem.at[2 * nblk + 3])
    load_q = pltpu.make_async_copy(q_hbm, q_ref, load_sem.at[2 * nblk + 4])

    barrier = pltpu.get_barrier_semaphore()
    for off in range(1, DEV):
        pl.semaphore_signal(barrier, inc=1, device_id={"rows": lax.rem(me + off, DEV)})

    order = (me, at.sib, at.y0, at.x0, at.y1, at.x1, at.d0, at.d1)
    for j in order:
        load_tgt(j).start()
    load_feat.start()
    load_mass.start()
    load_q.start()
    load_fsrc.start()
    for j in range(nblk):
        load_plan(j).start()
    load_src.start()

    def cast_tgt(j):
        load_tgt(j).wait()
        tgt_ref[j, rows_of(me), :] = stage2_ref[j].astype(jnp.bfloat16)

    cast_tgt(me)
    cast_tgt(at.sib)
    pl.semaphore_wait(barrier, DEV - 1)

    def tcopy(owner, col, dest, kind):
        view = tgt_ref.at[col, rows_of(owner), :]
        return pltpu.make_async_remote_copy(
            src_ref=view, dst_ref=view, send_sem=tgt_send.at[kind, col],
            recv_sem=tgt_recv.at[owner, col], device_id={"rows": dest})

    def fcopy(owner, dest, kind):
        view = ftgt_ref.at[rows_of(owner), :]
        return pltpu.make_async_remote_copy(
            src_ref=view, dst_ref=view, send_sem=feat_send.at[kind], recv_sem=feat_recv.at[owner], device_id={"rows": dest})

    out_x = (at.me, at.sib, at.y0, at.y1, at.d0)
    out_y = (at.me, at.sib, at.x0, at.x1, at.d1)
    in_x = (at.x0, at.x1, at.d0, at.d1, at.y0)
    in_y = (at.y0, at.y1, at.d0, at.d1, at.x1)

    def pair_send(wait):
        for core, dest in ((0, at.x0), (1, at.y0)):
            @pl.when(at.core == core)
            def _():
                copy = tcopy(me, at.sib, dest, core)
                copy.wait_send() if wait else copy.start()

    tcopy(me, me, at.x0, 0).start()
    tcopy(me, me, at.y0, 1).start()
    pair_send(False)
    for col in (me, at.sib):
        tcopy(me, col, at.sib, 2).start()
    load_feat.wait()
    ftgt_ref[rows_of(me), :] = feat_ref[0].astype(jnp.bfloat16)
    fcopy(me, at.x0, 0).start()
    fcopy(me, at.y0, 1).start()
    fcopy(me, at.sib, 2).start()
    for j in order[2:]:
        cast_tgt(j)
        tcopy(me, j, at.sib, 2).start()
    for k in range(2, 5):
        tcopy(me, out_x[k], at.x0, 0).start()
        tcopy(me, out_y[k], at.y0, 1).start()

    load_mass.wait()
    load_q.wait()
    swap = pltpu.make_async_remote_copy(
        src_ref=mass_ref, dst_ref=mass2_ref, send_sem=swap_send.at[0], recv_sem=swap_recv.at[0], device_id={"rows": at.sib})
    swap.start()
    load_fsrc.wait()
    fsrc_ref[:BLK] = feat_ref[1].astype(jnp.bfloat16)
    swap_feat = pltpu.make_async_remote_copy(
        src_ref=fsrc_ref.at[:BLK], dst_ref=fsrc_ref.at[BLK:], send_sem=swap_send.at[1], recv_sem=swap_recv.at[1],
        device_id={"rows": at.sib})
    swap_feat.start()
    load_src.wait()
    src_ref[:rows] = cost_ref[:rows, :].astype(jnp.bfloat16)
    swap_src = pltpu.make_async_remote_copy(
        src_ref=src_ref.at[:rows], dst_ref=src_ref.at[rows:], send_sem=swap_send.at[2], recv_sem=swap_recv.at[2],
        device_id={"rows": at.sib})
    swap_src.start()
    eye = lax.broadcasted_iota(jnp.int32, (LANES, LANES), 0) == lax.broadcasted_iota(jnp.int32, (LANES, LANES), 1)
    swap.wait()
    for r in range(rows // LANES):
        p_ref[r * LANES:(r + 1) * LANES, :] = spread(mass_ref[r:r + 1, :], eye)
        p_ref[rows + r * LANES:rows + (r + 1) * LANES, :] = spread(mass2_ref[r:r + 1, :], eye)

    def on_reach(f):
        @pl.when(at.core == 1)
        def _():
            f(2 * rows)

        @pl.when(at.core == 0)
        def _():
            f(rows)

    def add_column(j):
        def add(reach, base_ref):
            lhs = a_ref[:reach, pl.ds(pl.multiple_of(j * BLK, BLK), BLK)]
            for col in range(nblk):
                where = slice(col * BLK, (col + 1) * BLK)
                prod = jnp.dot(lhs, tgt_ref[col, rows_of(j), :], preferred_element_type=jnp.float32)
                cost_ref[:reach, where] = base_ref[:reach, where] - (2.0 * (1.0 - ALPHA)) * prod

        def go(reach):
            @pl.when(j == 0)
            def _():
                add(reach, cross_ref)

            @pl.when(j > 0)
            def _():
                add(reach, cost_ref)

        on_reach(go)

    def column(j):
        def go(reach):
            prod = jnp.dot(src_ref[:reach, :], plan_ref[j], preferred_element_type=jnp.float32)
            a_ref[:reach, pl.ds(pl.multiple_of(j * BLK, BLK), BLK)] = prod.astype(jnp.bfloat16)

        on_reach(go)
        add_column(j)

    def cast_plan(j):
        load_plan(j).wait()
        plan_ref[j, rows_of(me), :] = stage_ref[j].astype(jnp.bfloat16)

    begin, go_on = gather_plan(at, nblk, plan_ref, plan_send, plan_recv, cast_plan, column)

    def mirror(owner, col):
        tgt_ref[owner, rows_of(col), :] = tgt_ref[col, rows_of(owner), :].T

    base = me - at.core

    def mirror_row(owner):
        def body(t, carry):
            mirror(owner, lax.rem(base + 2 + t, DEV))
            return carry

        lax.fori_loop(0, DEV - 2, body, 0)

    def stream(k, s, other):
        core = lax.rem(at.core + other, 2)
        xb, yb, db = at.x0 - at.core, at.y0 - at.core, at.d0 - at.core
        near = xb + s * (yb - xb)
        far = yb + s * (xb - yb)
        which = k // 2
        chip = jnp.where(which == 0, near, jnp.where(which == 1, db, far))
        flip = jnp.where(which == 2, s, 0)
        return near + core, chip + lax.rem(core + k + flip, 2)

    def arrivals(k, carry):
        for s, fwd in ((0, 3), (1, 4)):
            @pl.when((k != 1) | (at.core == s))
            def _():
                owner, col = stream(k, s, 0)
                tcopy(owner, col, at.sib, 0).wait_recv()
                tcopy(owner, col, at.sib, fwd).start()

        @pl.when(k == 0)
        def _():
            tcopy(at.y0, at.y0, at.x0, 6).start()

        @pl.when((k == 1) & (at.core == 0))
        def _():
            tcopy(at.x0, at.x1, at.y0, 6).start()

        @pl.when(k == 1)
        def _():
            fcopy(at.x0, at.sib, 0).wait_recv()
            fcopy(at.x0, at.sib, 3).start()
            fcopy(at.y0, at.sib, 0).wait_recv()
            fcopy(at.y0, at.sib, 4).start()

            @pl.when(at.core == 0)
            def _():
                fcopy(at.x0, at.y0, 6).start()

            @pl.when(at.core == 1)
            def _():
                fcopy(at.y0, at.x0, 6).start()

            mirror_row(me)

        @pl.when(k == 2)
        def _():
            begin()

            def from_sib(j, c):
                tcopy(at.sib, j, at.sib, 0).wait_recv()
                return c

            lax.fori_loop(0, nblk, from_sib, 0)
            mirror_row(at.sib)

        def near(t, c):
            other = t // 2
            owner, col = stream(k, lax.rem(t, 2), other)

            @pl.when((k != 1) | (lax.rem(at.core + other, 2) == lax.rem(t, 2)))
            def _():
                @pl.when(t >= 2)
                def _():
                    tcopy(owner, col, at.sib, 0).wait_recv()

                @pl.when(k >= 1)
                def _():
                    mirror(owner, col)

            return c

        lax.fori_loop(0, 4, near, 0)
        return carry

    lax.fori_loop(0, 5, arrivals, 0)
    tcopy(at.d0, at.d0, at.d0, 0).wait_recv()
    tcopy(at.d0, at.d0, at.sib, 5).start()

    @pl.when(at.core == 0)
    def _():
        tcopy(at.d0, at.d1, at.d0, 0).wait_recv()
        tcopy(at.d0, at.d1, at.sib, 5).start()

    fcopy(at.d0, at.sib, 0).wait_recv()
    fcopy(at.d0, at.sib, 5).start()
    for owner in (at.sib, at.x1, at.y1, at.d1):
        fcopy(owner, at.sib, 0).wait_recv()
    swap_feat.wait()
    swap_src.wait()

    def crosses(reach):
        def cross(j, carry):
            prod = lax.dot_general(
                fsrc_ref[:reach, :], ftgt_ref[rows_of(j), :], (((1,), (1,)), ((), ())),
                preferred_element_type=jnp.float32)
            cross_ref[:reach, pl.ds(pl.multiple_of(j * BLK, BLK), BLK)] = (-2.0 * ALPHA) * prod
            return carry

        lax.fori_loop(0, nblk, cross, 0)

    on_reach(crosses)
    tcopy(at.d1, at.d1, at.sib, 0).wait_recv()

    @pl.when(at.core == 1)
    def _():
        tcopy(at.d1, at.d0, at.sib, 0).wait_recv()

    mirror(at.d0 - at.core, at.d0 - at.core + 1)

    go_on()

    for kind in range(7):
        fcopy(me, at.sib, kind).wait_send()
    pair_send(True)
    for k in (0, 2, 3, 4):
        tcopy(me, out_x[k], at.x0, 0).wait_send()
        tcopy(me, out_y[k], at.y0, 1).wait_send()
        tcopy(at.x0, in_x[k], at.sib, 3).wait_send()
        tcopy(at.y0, in_y[k], at.sib, 4).wait_send()
    tcopy(at.d0, at.d0, at.sib, 5).wait_send()
    tcopy(at.y0, at.y0, at.x0, 6).wait_send()

    @pl.when(at.core == 0)
    def _():
        tcopy(at.x0, at.x1, at.sib, 3).wait_send()
        tcopy(at.d0, at.d1, at.sib, 5).wait_send()
        tcopy(at.x0, at.x1, at.y0, 6).wait_send()

    @pl.when(at.core == 1)
    def _():
        tcopy(at.y0, at.y1, at.sib, 4).wait_send()

    def sib_done(j, carry):
        tcopy(me, j, at.sib, 2).wait_send()
        return carry

    lax.fori_loop(0, nblk, sib_done, 0)

    def early(src, j, slot, dest, kind):
        return pltpu.make_async_remote_copy(
            src_ref=src, dst_ref=early_ref.at[slot, j], send_sem=early_send.at[kind, j],
            recv_sem=early_recv.at[slot, j], device_id={"rows": dest})

    def early_half(i, dest):
        part = pl.ds(i * (BLK // 2), BLK // 2)
        return pltpu.make_async_remote_copy(
            src_ref=early_ref.at[i, EARLY - 1, part], dst_ref=early_ref.at[2, EARLY - 1, part],
            send_sem=early_send.at[2, EARLY - 1 + i], recv_sem=early_recv.at[2, EARLY - 1 + i], device_id={"rows": dest})

    def own_part(j):
        return kern_ref.at[0, :, pl.ds(pl.multiple_of(j * BLK, BLK), BLK)]

    def early_round():
        def send(j):
            early(own_part(j), j, 0, at.x0, 0).start()
            early(own_part(j), j, 1, at.y0, 1).start()

        for j in range(AHEAD):
            send(j)

        def turn(j, carry):
            @pl.when(j + AHEAD < EARLY)
            def _():
                send(j + AHEAD)

            early(own_part(j), j, 0, at.x0, 0).wait_recv()

            @pl.when((lax.rem(j, 2) == 0) & (j < EARLY - 1))
            def _():
                early(early_ref.at[0, j], j, 2, at.y0, 2).start()

            @pl.when(j == EARLY - 1)
            def _():
                early_half(0, at.y0).start()

            early(own_part(j), j, 1, at.y0, 1).wait_recv()

            @pl.when((lax.rem(j, 2) == 1) & (j < EARLY - 1))
            def _():
                early(early_ref.at[1, j], j, 2, at.x0, 2).start()

            @pl.when(j == EARLY - 1)
            def _():
                early_half(1, at.x0).start()

            return carry

        lax.fori_loop(0, EARLY, turn, 0)

        def done(j, carry):
            for kind in range(2):
                early(own_part(j), j, kind, at.x0, kind).wait_send()

            @pl.when(j < EARLY - 1)
            def _():
                early(own_part(j), j, 2, at.x0, 2).wait_recv()
                early(own_part(j), j, 2, at.x0, 2).wait_send()

            return carry

        lax.fori_loop(0, EARLY, done, 0)
        for i in range(2):
            early_half(i, at.x0).wait_recv()
            early_half(i, at.x0).wait_send()

    tiles = cols // LANES
    across = (at.sib, at.x1, at.y1, at.d1)

    def news(k):
        return pltpu.make_async_remote_copy(
            src_ref=msg_ref, dst_ref=news_ref.at[k], send_sem=msg_send.at[k], recv_sem=msg_recv.at[k],
            device_id={"rows": across[k]})

    def sweeps(first):
        reach = len(across) if first else 1
        build_kernel(cost_ref, kern_ref, eps, 0, rows, cols)

        @pl.when(at.core == 1)
        def _():
            build_kernel(cost_ref, kern_ref, eps, 1, rows, cols)
            sinkhorn(at, kern_ref, p_ref, q_ref, u_ref, v_ref, dots_ref, part_ref, gath_ref, sum_send, sum_recv)
            msg_ref[:tiles] = v_ref[...]
            msg_ref[tiles:] = jnp.zeros_like(msg_ref[tiles:])
            for r in range(rows // LANES):
                scale = u_ref[rows + r * LANES:rows + (r + 1) * LANES, :]
                msg_ref[tiles + r:tiles + r + 1] = jnp.sum(jnp.where(eye, scale, 0.0), axis=0, keepdims=True)
            for k in range(reach):
                news(k).start()

        @pl.when(at.core == 0)
        def _():
            if first:
                early_round()
            for k in range(reach):
                news(k).wait_recv()
            v_ref[...] = news_ref[0, :tiles]
            for r in range(rows // LANES):
                u_ref[r * LANES:(r + 1) * LANES, :] = spread(news_ref[0, tiles + r:tiles + r + 1], eye)
                for k in range(1, reach):
                    other_ref[k - 1, r * LANES:(r + 1) * LANES, :] = spread(news_ref[k, tiles + r:tiles + r + 1], eye)

    def news_done(reach):
        @pl.when(at.core == 1)
        def _():
            for k in range(reach):
                news(k).wait_send()

    def own_block(j):
        cols_at = pl.multiple_of(j * BLK, BLK)
        return plan_block(lambda h: kern_ref[0, :, pl.ds(cols_at + h * LANES, LANES)], u_ref[:rows, :], v_ref, j)

    sweeps(True)

    def next_plan(j):
        plan_ref[j, rows_of(me), :] = own_block(j).astype(jnp.bfloat16)

    def form(k, j):
        return plan_block(lambda h: early_ref[k, j, :, h * LANES:(h + 1) * LANES], other_ref[k], v_ref, j)

    begin, go_on = gather_plan(at, nblk, plan_ref, plan_send, plan_recv, next_plan, column, form)
    begin()
    go_on()
    news_done(len(across))
    sweeps(False)

    for j in range(nblk):
        out_ref[:, j * BLK:(j + 1) * BLK] = own_block(j)
    news_done(1)


def fgw(src, tgt, plan, mass, q, fsrc, ftgt, eps):
    rows, cols = plan.shape
    tiles = cols // LANES
    nblk = cols // BLK
    vmem = pl.BlockSpec(memory_space=pltpu.VMEM)
    hbm = pl.BlockSpec(memory_space=pltpu.HBM)
    f32, bf16 = jnp.float32, jnp.bfloat16
    return pl.pallas_call(
        fgw_kernel,
        out_shape=jax.ShapeDtypeStruct((rows, cols), f32),
        in_specs=[pl.BlockSpec(memory_space=pltpu.SMEM)] + [hbm] * 7,
        out_specs=vmem,
        scratch_shapes=[
            pltpu.VMEM((nblk, BLK, BLK), f32),
            pltpu.VMEM((nblk, BLK, BLK), f32),
            pltpu.VMEM((2, BLK, BLK), f32),
            pltpu.VMEM((nblk, DEV * BLK, BLK), bf16),
            pltpu.VMEM((nblk, DEV * BLK, BLK), bf16),
            pltpu.VMEM((2 * rows, cols), bf16),
            pltpu.VMEM((2 * BLK, BLK), bf16),
            pltpu.VMEM((DEV * BLK, BLK), bf16),
            pltpu.VMEM((2 * rows, cols), bf16),
            pltpu.VMEM((2 * rows, cols), f32),
            pltpu.VMEM((2 * rows, cols), f32),
            pltpu.VMEM((2, rows, cols), f32),
            pltpu.VMEM((3, EARLY, BLK, BLK), f32),
            pltpu.VMEM((2 * rows, LANES), f32),
            pltpu.VMEM((tiles, LANES), f32),
            pltpu.VMEM((2 * rows, LANES), f32),
            pltpu.VMEM((tiles, LANES), f32),
            pltpu.VMEM((2 * rows, LANES), f32),
            pltpu.VMEM((3, rows, LANES), f32),
            pltpu.VMEM((2, PIECES, tiles // PIECES, LANES), f32),
            pltpu.VMEM((2, PIECES, DEV // 2, tiles // PIECES, LANES), f32),
            pltpu.VMEM((tiles + SUB, LANES), f32),
            pltpu.VMEM((4, tiles + SUB, LANES), f32),
            pltpu.VMEM((rows // LANES, LANES), f32),
            pltpu.VMEM((rows // LANES, LANES), f32),
            pltpu.SemaphoreType.DMA((2 * nblk + 5,)),
            pltpu.SemaphoreType.DMA((7, nblk)),
            pltpu.SemaphoreType.DMA((DEV, nblk)),
            pltpu.SemaphoreType.DMA((7, nblk)),
            pltpu.SemaphoreType.DMA((DEV, nblk)),
            pltpu.SemaphoreType.DMA((7,)),
            pltpu.SemaphoreType.DMA((DEV,)),
            pltpu.SemaphoreType.DMA((2, PIECES, 3)),
            pltpu.SemaphoreType.DMA((2, PIECES, DEV // 2)),
            pltpu.SemaphoreType.DMA((3,)),
            pltpu.SemaphoreType.DMA((3,)),
            pltpu.SemaphoreType.DMA((3, EARLY + 1)),
            pltpu.SemaphoreType.DMA((3, EARLY + 1)),
            pltpu.SemaphoreType.DMA((4,)),
            pltpu.SemaphoreType.DMA((4,)),
        ],
        compiler_params=pltpu.CompilerParams(collective_id=0, has_side_effects=True, vmem_limit_bytes=50 << 20),
        name="fgw",
    )(eps, *[pltpu.with_memory_space_constraint(x, pltpu.HBM) for x in (mass, q, src, tgt, plan, fsrc, ftgt)])


def solution(mesh):
    def local_fgw(cost_src, cost_tgt, plan_init, mass_src, mass_tgt, feat_src, feat_tgt, epsilon):
        return fgw(
            cost_src, cost_tgt, plan_init, mass_src.reshape(-1, LANES), mass_tgt.reshape(-1, LANES),
            feat_src, feat_tgt, epsilon.reshape(1))

    row_spec = P(('pairs', 'rows'), None)
    vec_spec = P(('pairs', 'rows'))
    in_specs = (row_spec, row_spec, row_spec, vec_spec, P('pairs'), row_spec, row_spec, P())
    return jax.shard_map(local_fgw, mesh=mesh, in_specs=in_specs, out_specs=row_spec, check_vma=False)
```

```python
import functools

import jax
import jax.numpy as jnp
from jax import lax
from jax.experimental import pallas as pl
from jax.experimental.pallas import tpu as pltpu
from jax.sharding import PartitionSpec as P

ALPHA = 0.5
OUTER_STEPS = 2
SWEEPS = 10
LANES = 128
SUB = 8
BLK = 256
DEV = 8
AHEAD = 2
LAG = 2
EARLY = 7
PIECES = 2


def tree_sum(vals):
    while len(vals) > 1:
        vals = [a + b for a, b in zip(vals[::2], vals[1::2])] + vals[len(vals) & ~1:]
    return vals[0]


def rows_of(owner):
    return pl.ds(pl.multiple_of(owner * BLK, BLK), BLK)


class Place:
    def __init__(self):
        self.me = lax.axis_index("rows")
        core = lax.rem(self.me, 2)
        x = lax.rem(self.me // 2, 2)
        y = self.me // 4
        self.core = core
        self.sib = self.me + 1 - 2 * core
        dx, dy = 2 - 4 * x, 4 - 8 * y
        self.x0, self.x1 = self.me + dx, self.sib + dx
        self.y0, self.y1 = self.me + dy, self.sib + dy
        self.d0, self.d1 = self.me + dx + dy, self.sib + dx + dy


def build_kernel(cost_ref, kern_ref, eps, half, rows, cols):
    tiles = cols // LANES
    inv_eps = 1.0 / jnp.full((SUB, LANES), eps, jnp.float32)

    def block(b, carry):
        row = pl.multiple_of(b * SUB, SUB)
        at_row = pl.ds(pl.multiple_of(half * rows + row, SUB), SUB)
        vals = [cost_ref[at_row, t * LANES:(t + 1) * LANES] for t in range(tiles)]
        low = functools.reduce(jnp.minimum, vals)
        low = jnp.min(low, axis=1, keepdims=True)
        for t in range(tiles):
            kern_ref[half, pl.ds(row, SUB), t * LANES:(t + 1) * LANES] = jnp.exp((low - vals[t]) * inv_eps)
        return carry

    lax.fori_loop(0, rows // SUB, block, 0, unroll=16)


def spread(line, eye):
    wide = jnp.broadcast_to(line, (LANES, LANES))
    col = jnp.sum(jnp.where(eye, wide, 0.0), axis=1, keepdims=True)
    return jnp.broadcast_to(col, (LANES, LANES))


def sinkhorn(at, kern_ref, p_ref, q_ref, u_ref, v_ref, dots_ref, part_ref, gath_ref, send_sem, recv_sem):
    halves, rows, cols = kern_ref.shape
    tiles = cols // LANES
    span = tiles // PIECES
    blocks = [(h, b) for h in range(halves) for b in range(rows // SUB)]
    chip = at.me // 2
    peers = (at.x0, at.y0, at.d0)

    def copy(par, g, k, slot):
        return pltpu.make_async_remote_copy(
            src_ref=part_ref.at[par, g], dst_ref=gath_ref.at[par, g, slot],
            send_sem=send_sem.at[par, g, k], recv_sem=recv_sem.at[par, g, slot], device_id={"rows": peers[k]})

    def tile(h, b, t):
        return kern_ref[h, b * SUB:(b + 1) * SUB, t * LANES:(t + 1) * LANES]

    def at_row(h, b):
        return slice(h * rows + b * SUB, h * rows + (b + 1) * SUB)

    def dots_of(g):
        vrow = [jnp.broadcast_to(v_ref[t:t + 1, :], (SUB, LANES)) for t in range(g * span, (g + 1) * span)]
        for h, b in blocks:
            dots = tree_sum([tile(h, b, g * span + t) * vrow[t] for t in range(span)])
            if g > 0:
                dots = dots + dots_ref[at_row(h, b), :]
            if g < PIECES - 1:
                dots_ref[at_row(h, b), :] = dots
            else:
                u_ref[at_row(h, b), :] = p_ref[at_row(h, b), :] / jnp.sum(dots, axis=1, keepdims=True)

    def sums_of(par, g):
        acc = [None] * span
        for h, b in blocks:
            scale = u_ref[at_row(h, b), :]
            for t in range(span):
                term = tile(h, b, g * span + t) * scale
                acc[t] = term if acc[t] is None else acc[t] + term
        sums = jnp.concatenate([jnp.sum(a, axis=0, keepdims=True) for a in acc], axis=0)
        part_ref[par, g] = sums
        for k in (2, 0, 1):
            copy(par, g, k, chip).start()
        gath_ref[par, g, chip] = sums

    def scales_of(par, g):
        for k in range(3):
            copy(par, g, k, peers[k] // 2).wait_recv()
        total = gath_ref[par, g, 0]
        for d in range(1, DEV // 2):
            total = total + gath_ref[par, g, d]
        v_ref[g * span:(g + 1) * span, :] = q_ref[g * span:(g + 1) * span, :] / total

    def sent(par):
        for g in range(PIECES):
            for k in range(3):
                copy(par, g, k, chip).wait_send()

    v_ref[...] = jnp.ones_like(v_ref)

    def sweep(step, carry):
        par = lax.rem(step, 2)
        for g in range(PIECES):
            @pl.when(step > 0)
            def _():
                scales_of(1 - par, g)

            dots_of(g)

        @pl.when(step > 0)
        def _():
            sent(1 - par)

        for g in range(PIECES):
            sums_of(par, g)
        return carry

    lax.fori_loop(0, SWEEPS, sweep, 0)
    for g in range(PIECES):
        scales_of((SWEEPS - 1) % 2, g)
    sent((SWEEPS - 1) % 2)


def plan_block(kern, scale, v_ref, j):
    parts = []
    for h in range(BLK // LANES):
        vrow = v_ref[pl.ds(j * (BLK // LANES) + h, 1), :]
        parts.append(scale * kern(h) * vrow)
    return jnp.concatenate(parts, axis=1)


def gather_plan(at, chunks, plan_ref, send_sem, recv_sem, produce, column, form=None):
    def copy(owner, j, dest, kind):
        view = plan_ref.at[j, rows_of(owner), :]
        return pltpu.make_async_remote_copy(
            src_ref=view, dst_ref=view, send_sem=send_sem.at[kind, j],
            recv_sem=recv_sem.at[owner, j], device_id={"rows": dest})

    def over_links(j):
        return True if form is None else (at.core == 1) | (j >= EARLY)

    def when(cond):
        return (lambda f: f()) if cond is True else pl.when(cond)

    def send_own(j):
        @when(over_links(j))
        def _():
            copy(at.me, j, at.x0, 0).start()
            copy(at.me, j, at.y0, 1).start()

        copy(at.me, j, at.sib, 2).start()

    def begin():
        for j in range(AHEAD):
            produce(j)
            send_own(j)

    def turn(it, carry):
        @pl.when(it + AHEAD < chunks)
        def _():
            produce(it + AHEAD)
            send_own(it + AHEAD)

        @pl.when((it < chunks) & over_links(it))
        def _():
            copy(at.x0, it, at.x0, 0).wait_recv()
            copy(at.x0, it, at.sib, 3).start()

            @pl.when(lax.rem(it, 2) == 0)
            def _():
                copy(at.x0, it, at.y0, 6).start()

            copy(at.y0, it, at.y0, 0).wait_recv()
            copy(at.y0, it, at.sib, 4).start()

            @pl.when(lax.rem(it, 2) == 1)
            def _():
                copy(at.y0, it, at.x0, 6).start()

        if form is not None:
            @pl.when((it < chunks) & (at.core == 0) & (it < EARLY))
            def _():
                for k, owner in enumerate((at.x0, at.y0, at.d0)):
                    plan_ref[it, rows_of(owner), :] = form(k, it).astype(jnp.bfloat16)
                    copy(owner, it, at.sib, 3 + k).start()

        @pl.when((it >= LAG) & (it < LAG + chunks) & over_links(it - LAG))
        def _():
            copy(at.d0, it - LAG, at.d0, 0).wait_recv()
            copy(at.d0, it - LAG, at.sib, 5).start()

        @pl.when(it >= LAG + 1)
        def _():
            j = it - LAG - 1
            for owner in (at.sib, at.x1, at.y1, at.d1):
                copy(owner, j, at.sib, 0).wait_recv()
            column(j)

        return carry

    def drain(j, carry):
        for kind in (2, 3, 4, 5):
            copy(at.me, j, at.sib, kind).wait_send()

        @when(over_links(j))
        def _():
            for kind in (0, 1, 6):
                copy(at.me, j, at.sib, kind).wait_send()

        return carry

    def go_on():
        lax.fori_loop(0, chunks + LAG + 1, turn, 0)
        lax.fori_loop(0, chunks, drain, 0)

    return begin, go_on


def fgw_kernel(
    eps_ref, mass_hbm, q_hbm, src_hbm, tgt_hbm, plan_hbm, fsrc_hbm, ftgt_hbm, out_ref,
    stage_ref, stage2_ref, feat_ref, plan_ref, tgt_ref, src_ref, fsrc_ref, ftgt_ref, a_ref, cross_ref, cost_ref, kern_ref,
    early_ref, p_ref, q_ref, u_ref, v_ref, dots_ref, other_ref, part_ref, gath_ref, msg_ref, news_ref, mass_ref, mass2_ref,
    load_sem, plan_send, plan_recv, tgt_send, tgt_recv, feat_send, feat_recv, sum_send, sum_recv,
    swap_send, swap_recv, early_send, early_recv, msg_send, msg_recv,
):
    at = Place()
    me = at.me
    _, rows, cols = kern_ref.shape
    nblk = cols // BLK
    eps = eps_ref[0]

    def load_plan(j):
        return pltpu.make_async_copy(plan_hbm.at[:, pl.ds(pl.multiple_of(j * BLK, BLK), BLK)], stage_ref.at[j], load_sem.at[j])

    def load_tgt(j):
        return pltpu.make_async_copy(tgt_hbm.at[:, pl.ds(pl.multiple_of(j * BLK, BLK), BLK)], stage2_ref.at[j], load_sem.at[nblk + j])

    load_feat = pltpu.make_async_copy(ftgt_hbm, feat_ref.at[0], load_sem.at[2 * nblk])
    load_fsrc = pltpu.make_async_copy(fsrc_hbm, feat_ref.at[1], load_sem.at[2 * nblk + 1])
    load_src = pltpu.make_async_copy(src_hbm, cost_ref.at[:rows], load_sem.at[2 * nblk + 2])
    load_mass = pltpu.make_async_copy(mass_hbm, mass_ref, load_sem.at[2 * nblk + 3])
    load_q = pltpu.make_async_copy(q_hbm, q_ref, load_sem.at[2 * nblk + 4])

    barrier = pltpu.get_barrier_semaphore()
    for off in range(1, DEV):
        pl.semaphore_signal(barrier, inc=1, device_id={"rows": lax.rem(me + off, DEV)})

    order = (me, at.sib, at.y0, at.x0, at.y1, at.x1, at.d0, at.d1)
    for j in order:
        load_tgt(j).start()
    load_feat.start()
    load_mass.start()
    load_q.start()
    load_fsrc.start()
    for j in range(nblk):
        load_plan(j).start()
    load_src.start()

    def cast_tgt(j):
        load_tgt(j).wait()
        tgt_ref[j, rows_of(me), :] = stage2_ref[j].astype(jnp.bfloat16)

    cast_tgt(me)
    cast_tgt(at.sib)
    pl.semaphore_wait(barrier, DEV - 1)

    def tcopy(owner, col, dest, kind):
        view = tgt_ref.at[col, rows_of(owner), :]
        return pltpu.make_async_remote_copy(
            src_ref=view, dst_ref=view, send_sem=tgt_send.at[kind, col],
            recv_sem=tgt_recv.at[owner, col], device_id={"rows": dest})

    def fcopy(owner, dest, kind):
        view = ftgt_ref.at[rows_of(owner), :]
        return pltpu.make_async_remote_copy(
            src_ref=view, dst_ref=view, send_sem=feat_send.at[kind], recv_sem=feat_recv.at[owner], device_id={"rows": dest})

    out_x = (at.me, at.sib, at.y0, at.y1, at.d0)
    out_y = (at.me, at.sib, at.x0, at.x1, at.d1)
    in_x = (at.x0, at.x1, at.d0, at.d1, at.y0)
    in_y = (at.y0, at.y1, at.d0, at.d1, at.x1)

    def pair_send(wait):
        for core, dest in ((0, at.x0), (1, at.y0)):
            @pl.when(at.core == core)
            def _():
                copy = tcopy(me, at.sib, dest, core)
                copy.wait_send() if wait else copy.start()

    tcopy(me, me, at.x0, 0).start()
    tcopy(me, me, at.y0, 1).start()
    pair_send(False)
    for col in (me, at.sib):
        tcopy(me, col, at.sib, 2).start()
    load_feat.wait()
    ftgt_ref[rows_of(me), :] = feat_ref[0].astype(jnp.bfloat16)
    fcopy(me, at.x0, 0).start()
    fcopy(me, at.y0, 1).start()
    fcopy(me, at.sib, 2).start()
    for j in order[2:]:
        cast_tgt(j)
        tcopy(me, j, at.sib, 2).start()
    for k in range(2, 5):
        tcopy(me, out_x[k], at.x0, 0).start()
        tcopy(me, out_y[k], at.y0, 1).start()

    load_mass.wait()
    load_q.wait()
    swap = pltpu.make_async_remote_copy(
        src_ref=mass_ref, dst_ref=mass2_ref, send_sem=swap_send.at[0], recv_sem=swap_recv.at[0], device_id={"rows": at.sib})
    swap.start()
    load_fsrc.wait()
    fsrc_ref[:BLK] = feat_ref[1].astype(jnp.bfloat16)
    swap_feat = pltpu.make_async_remote_copy(
        src_ref=fsrc_ref.at[:BLK], dst_ref=fsrc_ref.at[BLK:], send_sem=swap_send.at[1], recv_sem=swap_recv.at[1],
        device_id={"rows": at.sib})
    swap_feat.start()
    load_src.wait()
    src_ref[:rows] = cost_ref[:rows, :].astype(jnp.bfloat16)
    swap_src = pltpu.make_async_remote_copy(
        src_ref=src_ref.at[:rows], dst_ref=src_ref.at[rows:], send_sem=swap_send.at[2], recv_sem=swap_recv.at[2],
        device_id={"rows": at.sib})
    swap_src.start()
    eye = lax.broadcasted_iota(jnp.int32, (LANES, LANES), 0) == lax.broadcasted_iota(jnp.int32, (LANES, LANES), 1)
    swap.wait()
    for r in range(rows // LANES):
        p_ref[r * LANES:(r + 1) * LANES, :] = spread(mass_ref[r:r + 1, :], eye)
        p_ref[rows + r * LANES:rows + (r + 1) * LANES, :] = spread(mass2_ref[r:r + 1, :], eye)

    def on_reach(f):
        @pl.when(at.core == 1)
        def _():
            f(2 * rows)

        @pl.when(at.core == 0)
        def _():
            f(rows)

    def add_column(j):
        def add(reach, base_ref):
            lhs = a_ref[:reach, pl.ds(pl.multiple_of(j * BLK, BLK), BLK)]
            for col in range(nblk):
                where = slice(col * BLK, (col + 1) * BLK)
                prod = jnp.dot(lhs, tgt_ref[col, rows_of(j), :], preferred_element_type=jnp.float32)
                cost_ref[:reach, where] = base_ref[:reach, where] - (2.0 * (1.0 - ALPHA)) * prod

        def go(reach):
            @pl.when(j == 0)
            def _():
                add(reach, cross_ref)

            @pl.when(j > 0)
            def _():
                add(reach, cost_ref)

        on_reach(go)

    def column(j):
        def go(reach):
            prod = jnp.dot(src_ref[:reach, :], plan_ref[j], preferred_element_type=jnp.float32)
            a_ref[:reach, pl.ds(pl.multiple_of(j * BLK, BLK), BLK)] = prod.astype(jnp.bfloat16)

        on_reach(go)
        add_column(j)

    def cast_plan(j):
        load_plan(j).wait()
        plan_ref[j, rows_of(me), :] = stage_ref[j].astype(jnp.bfloat16)

    begin, go_on = gather_plan(at, nblk, plan_ref, plan_send, plan_recv, cast_plan, column)

    def mirror(owner, col):
        tgt_ref[owner, rows_of(col), :] = tgt_ref[col, rows_of(owner), :].T

    base = me - at.core

    def mirror_row(owner):
        def body(t, carry):
            mirror(owner, lax.rem(base + 2 + t, DEV))
            return carry

        lax.fori_loop(0, DEV - 2, body, 0)

    def stream(k, s, other):
        core = lax.rem(at.core + other, 2)
        xb, yb, db = at.x0 - at.core, at.y0 - at.core, at.d0 - at.core
        near = xb + s * (yb - xb)
        far = yb + s * (xb - yb)
        which = k // 2
        chip = jnp.where(which == 0, near, jnp.where(which == 1, db, far))
        flip = jnp.where(which == 2, s, 0)
        return near + core, chip + lax.rem(core + k + flip, 2)

    def arrivals(k, carry):
        for s, fwd in ((0, 3), (1, 4)):
            @pl.when((k != 1) | (at.core == s))
            def _():
                owner, col = stream(k, s, 0)
                tcopy(owner, col, at.sib, 0).wait_recv()
                tcopy(owner, col, at.sib, fwd).start()

        @pl.when(k == 0)
        def _():
            tcopy(at.y0, at.y0, at.x0, 6).start()

        @pl.when((k == 1) & (at.core == 0))
        def _():
            tcopy(at.x0, at.x1, at.y0, 6).start()

        @pl.when(k == 1)
        def _():
            fcopy(at.x0, at.sib, 0).wait_recv()
            fcopy(at.x0, at.sib, 3).start()
            fcopy(at.y0, at.sib, 0).wait_recv()
            fcopy(at.y0, at.sib, 4).start()

            @pl.when(at.core == 0)
            def _():
                fcopy(at.x0, at.y0, 6).start()

            @pl.when(at.core == 1)
            def _():
                fcopy(at.y0, at.x0, 6).start()

            mirror_row(me)

        @pl.when(k == 2)
        def _():
            begin()

            def from_sib(j, c):
                tcopy(at.sib, j, at.sib, 0).wait_recv()
                return c

            lax.fori_loop(0, nblk, from_sib, 0)
            mirror_row(at.sib)

        def near(t, c):
            other = t // 2
            owner, col = stream(k, lax.rem(t, 2), other)

            @pl.when((k != 1) | (lax.rem(at.core + other, 2) == lax.rem(t, 2)))
            def _():
                @pl.when(t >= 2)
                def _():
                    tcopy(owner, col, at.sib, 0).wait_recv()

                @pl.when(k >= 1)
                def _():
                    mirror(owner, col)

            return c

        lax.fori_loop(0, 4, near, 0)
        return carry

    lax.fori_loop(0, 5, arrivals, 0)
    tcopy(at.d0, at.d0, at.d0, 0).wait_recv()
    tcopy(at.d0, at.d0, at.sib, 5).start()

    @pl.when(at.core == 0)
    def _():
        tcopy(at.d0, at.d1, at.d0, 0).wait_recv()
        tcopy(at.d0, at.d1, at.sib, 5).start()

    fcopy(at.d0, at.sib, 0).wait_recv()
    fcopy(at.d0, at.sib, 5).start()
    for owner in (at.sib, at.x1, at.y1, at.d1):
        fcopy(owner, at.sib, 0).wait_recv()
    swap_feat.wait()
    swap_src.wait()

    def crosses(reach):
        def cross(j, carry):
            prod = lax.dot_general(
                fsrc_ref[:reach, :], ftgt_ref[rows_of(j), :], (((1,), (1,)), ((), ())),
                preferred_element_type=jnp.float32)
            cross_ref[:reach, pl.ds(pl.multiple_of(j * BLK, BLK), BLK)] = (-2.0 * ALPHA) * prod
            return carry

        lax.fori_loop(0, nblk, cross, 0)

    on_reach(crosses)
    tcopy(at.d1, at.d1, at.sib, 0).wait_recv()

    @pl.when(at.core == 1)
    def _():
        tcopy(at.d1, at.d0, at.sib, 0).wait_recv()

    mirror(at.d0 - at.core, at.d0 - at.core + 1)

    go_on()

    for kind in range(7):
        fcopy(me, at.sib, kind).wait_send()
    pair_send(True)
    for k in (0, 2, 3, 4):
        tcopy(me, out_x[k], at.x0, 0).wait_send()
        tcopy(me, out_y[k], at.y0, 1).wait_send()
        tcopy(at.x0, in_x[k], at.sib, 3).wait_send()
        tcopy(at.y0, in_y[k], at.sib, 4).wait_send()
    tcopy(at.d0, at.d0, at.sib, 5).wait_send()
    tcopy(at.y0, at.y0, at.x0, 6).wait_send()

    @pl.when(at.core == 0)
    def _():
        tcopy(at.x0, at.x1, at.sib, 3).wait_send()
        tcopy(at.d0, at.d1, at.sib, 5).wait_send()
        tcopy(at.x0, at.x1, at.y0, 6).wait_send()

    @pl.when(at.core == 1)
    def _():
        tcopy(at.y0, at.y1, at.sib, 4).wait_send()

    def sib_done(j, carry):
        tcopy(me, j, at.sib, 2).wait_send()
        return carry

    lax.fori_loop(0, nblk, sib_done, 0)

    def early(src, j, slot, dest, kind):
        return pltpu.make_async_remote_copy(
            src_ref=src, dst_ref=early_ref.at[slot, j], send_sem=early_send.at[kind, j],
            recv_sem=early_recv.at[slot, j], device_id={"rows": dest})

    def early_half(i, dest):
        part = pl.ds(i * (BLK // 2), BLK // 2)
        return pltpu.make_async_remote_copy(
            src_ref=early_ref.at[i, EARLY - 1, part], dst_ref=early_ref.at[2, EARLY - 1, part],
            send_sem=early_send.at[2, EARLY - 1 + i], recv_sem=early_recv.at[2, EARLY - 1 + i], device_id={"rows": dest})

    def own_part(j):
        return kern_ref.at[0, :, pl.ds(pl.multiple_of(j * BLK, BLK), BLK)]

    def early_round():
        def send(j):
            early(own_part(j), j, 0, at.x0, 0).start()
            early(own_part(j), j, 1, at.y0, 1).start()

        for j in range(AHEAD):
            send(j)

        def turn(j, carry):
            @pl.when(j + AHEAD < EARLY)
            def _():
                send(j + AHEAD)

            early(own_part(j), j, 0, at.x0, 0).wait_recv()

            @pl.when((lax.rem(j, 2) == 0) & (j < EARLY - 1))
            def _():
                early(early_ref.at[0, j], j, 2, at.y0, 2).start()

            @pl.when(j == EARLY - 1)
            def _():
                early_half(0, at.y0).start()

            early(own_part(j), j, 1, at.y0, 1).wait_recv()

            @pl.when((lax.rem(j, 2) == 1) & (j < EARLY - 1))
            def _():
                early(early_ref.at[1, j], j, 2, at.x0, 2).start()

            @pl.when(j == EARLY - 1)
            def _():
                early_half(1, at.x0).start()

            return carry

        lax.fori_loop(0, EARLY, turn, 0)

        def done(j, carry):
            for kind in range(2):
                early(own_part(j), j, kind, at.x0, kind).wait_send()

            @pl.when(j < EARLY - 1)
            def _():
                early(own_part(j), j, 2, at.x0, 2).wait_recv()
                early(own_part(j), j, 2, at.x0, 2).wait_send()

            return carry

        lax.fori_loop(0, EARLY, done, 0)
        for i in range(2):
            early_half(i, at.x0).wait_recv()
            early_half(i, at.x0).wait_send()

    tiles = cols // LANES
    across = (at.sib, at.x1, at.y1, at.d1)

    def news(k):
        return pltpu.make_async_remote_copy(
            src_ref=msg_ref, dst_ref=news_ref.at[k], send_sem=msg_send.at[k], recv_sem=msg_recv.at[k],
            device_id={"rows": across[k]})

    def sweeps(first):
        reach = len(across) if first else 1
        def build(half, carry):
            build_kernel(cost_ref, kern_ref, eps, half, rows, cols)
            return carry

        lax.fori_loop(0, 1 + at.core, build, 0)

        @pl.when(at.core == 1)
        def _():
            sinkhorn(at, kern_ref, p_ref, q_ref, u_ref, v_ref, dots_ref, part_ref, gath_ref, sum_send, sum_recv)
            msg_ref[:tiles] = v_ref[...]
            msg_ref[tiles:] = jnp.zeros_like(msg_ref[tiles:])
            for r in range(rows // LANES):
                scale = u_ref[rows + r * LANES:rows + (r + 1) * LANES, :]
                msg_ref[tiles + r:tiles + r + 1] = jnp.sum(jnp.where(eye, scale, 0.0), axis=0, keepdims=True)
            for k in range(reach):
                news(k).start()

        @pl.when(at.core == 0)
        def _():
            if first:
                early_round()
            for k in range(reach):
                news(k).wait_recv()
            v_ref[...] = news_ref[0, :tiles]
            for r in range(rows // LANES):
                u_ref[r * LANES:(r + 1) * LANES, :] = spread(news_ref[0, tiles + r:tiles + r + 1], eye)
                for k in range(1, reach):
                    other_ref[k - 1, r * LANES:(r + 1) * LANES, :] = spread(news_ref[k, tiles + r:tiles + r + 1], eye)

    def news_done(reach):
        @pl.when(at.core == 1)
        def _():
            for k in range(reach):
                news(k).wait_send()

    def own_block(j):
        cols_at = pl.multiple_of(j * BLK, BLK)
        return plan_block(lambda h: kern_ref[0, :, pl.ds(cols_at + h * LANES, LANES)], u_ref[:rows, :], v_ref, j)

    sweeps(True)

    def next_plan(j):
        plan_ref[j, rows_of(me), :] = own_block(j).astype(jnp.bfloat16)

    def form(k, j):
        return plan_block(lambda h: early_ref[k, j, :, h * LANES:(h + 1) * LANES], other_ref[k], v_ref, j)

    begin, go_on = gather_plan(at, nblk, plan_ref, plan_send, plan_recv, next_plan, column, form)
    begin()
    go_on()
    news_done(len(across))
    sweeps(False)

    for j in range(nblk):
        out_ref[:, j * BLK:(j + 1) * BLK] = own_block(j)
    news_done(1)


def fgw(src, tgt, plan, mass, q, fsrc, ftgt, eps):
    rows, cols = plan.shape
    tiles = cols // LANES
    nblk = cols // BLK
    vmem = pl.BlockSpec(memory_space=pltpu.VMEM)
    hbm = pl.BlockSpec(memory_space=pltpu.HBM)
    f32, bf16 = jnp.float32, jnp.bfloat16
    return pl.pallas_call(
        fgw_kernel,
        out_shape=jax.ShapeDtypeStruct((rows, cols), f32),
        in_specs=[pl.BlockSpec(memory_space=pltpu.SMEM)] + [hbm] * 7,
        out_specs=vmem,
        scratch_shapes=[
            pltpu.VMEM((nblk, BLK, BLK), f32),
            pltpu.VMEM((nblk, BLK, BLK), f32),
            pltpu.VMEM((2, BLK, BLK), f32),
            pltpu.VMEM((nblk, DEV * BLK, BLK), bf16),
            pltpu.VMEM((nblk, DEV * BLK, BLK), bf16),
            pltpu.VMEM((2 * rows, cols), bf16),
            pltpu.VMEM((2 * BLK, BLK), bf16),
            pltpu.VMEM((DEV * BLK, BLK), bf16),
            pltpu.VMEM((2 * rows, cols), bf16),
            pltpu.VMEM((2 * rows, cols), f32),
            pltpu.VMEM((2 * rows, cols), f32),
            pltpu.VMEM((2, rows, cols), f32),
            pltpu.VMEM((3, EARLY, BLK, BLK), f32),
            pltpu.VMEM((2 * rows, LANES), f32),
            pltpu.VMEM((tiles, LANES), f32),
            pltpu.VMEM((2 * rows, LANES), f32),
            pltpu.VMEM((tiles, LANES), f32),
            pltpu.VMEM((2 * rows, LANES), f32),
            pltpu.VMEM((3, rows, LANES), f32),
            pltpu.VMEM((2, PIECES, tiles // PIECES, LANES), f32),
            pltpu.VMEM((2, PIECES, DEV // 2, tiles // PIECES, LANES), f32),
            pltpu.VMEM((tiles + SUB, LANES), f32),
            pltpu.VMEM((4, tiles + SUB, LANES), f32),
            pltpu.VMEM((rows // LANES, LANES), f32),
            pltpu.VMEM((rows // LANES, LANES), f32),
            pltpu.SemaphoreType.DMA((2 * nblk + 5,)),
            pltpu.SemaphoreType.DMA((7, nblk)),
            pltpu.SemaphoreType.DMA((DEV, nblk)),
            pltpu.SemaphoreType.DMA((7, nblk)),
            pltpu.SemaphoreType.DMA((DEV, nblk)),
            pltpu.SemaphoreType.DMA((7,)),
            pltpu.SemaphoreType.DMA((DEV,)),
            pltpu.SemaphoreType.DMA((2, PIECES, 3)),
            pltpu.SemaphoreType.DMA((2, PIECES, DEV // 2)),
            pltpu.SemaphoreType.DMA((3,)),
            pltpu.SemaphoreType.DMA((3,)),
            pltpu.SemaphoreType.DMA((3, EARLY + 1)),
            pltpu.SemaphoreType.DMA((3, EARLY + 1)),
            pltpu.SemaphoreType.DMA((4,)),
            pltpu.SemaphoreType.DMA((4,)),
        ],
        compiler_params=pltpu.CompilerParams(collective_id=0, has_side_effects=True, vmem_limit_bytes=50 << 20),
        name="fgw",
    )(eps, *[pltpu.with_memory_space_constraint(x, pltpu.HBM) for x in (mass, q, src, tgt, plan, fsrc, ftgt)])


def solution(mesh):
    def local_fgw(cost_src, cost_tgt, plan_init, mass_src, mass_tgt, feat_src, feat_tgt, epsilon):
        return fgw(
            cost_src, cost_tgt, plan_init, mass_src.reshape(-1, LANES), mass_tgt.reshape(-1, LANES),
            feat_src, feat_tgt, epsilon.reshape(1))

    row_spec = P(('pairs', 'rows'), None)
    vec_spec = P(('pairs', 'rows'))
    in_specs = (row_spec, row_spec, row_spec, vec_spec, P('pairs'), row_spec, row_spec, P())
    return jax.shard_map(local_fgw, mesh=mesh, in_specs=in_specs, out_specs=row_spec, check_vma=False)
```
